32 devices in a mesh: seq: 16 (over z, y, x), head: 2 (over core).
Axes of the slice: x: 2, y: 2, z: 4, core: 2. Of those that a mesh axis runs over, the one named last changes fastest.
Arguments:
- query_vectors: bfloat16 [4096, 2560], P(('seq', 'head')), may hold values from -6 to 6
- address_vectors: bfloat16 [4096, 2560], P(('seq', 'head')), may hold values from -0.75 to 0.75
- payload_vectors: bfloat16 [4096, 2560], P(('seq', 'head')), may hold values from -6 to 6
- forget_logarithms: bfloat16 [4096, 2560], P(('seq', 'head')), may hold values from -1.5 to 0
- pre_sigmoid_filter: bfloat16 [4096, 2560], P(('seq', 'head')), may hold values from -6 to 6
- current_reward_table: float32 [40, 64], replicated, may hold values from -0.5 to 1.5
- cluster_standardize_weight: float32 [2560], replicated, may hold values from 0.25 to 1.75
- cluster_standardize_offset: float32 [2560], replicated, may hold values from -1.5 to 1.5
Outputs:
- mixed: bfloat16 [4096, 2560], P('seq', 'head')
The draws below stay inside these ranges and needn't reach their ends.
All inputs are finite; a program needn't handle non-finite values.
Results may differ from the reference program's by a relative error of at most 0.001.
Values may be sent and summed in bfloat16 or wider, within the bound.
No kernel may reach another device: no remote copies, remote signals or barrier semaphores. Data moves between devices by JAX's collectives and lax.ppermute only.
A program may use at most 192 MiB of HBM per device.

```python
import math
import jax
import jax.numpy as jnp
from jax import lax

D = 2560
HOSTED_ATTENDERS = 40
CHANNEL_COUNT = 64
TOK_DEV = 128
TEXT_LENGTH = 4096


def draw_forget_logarithms(key, part):
    address_block = jax.random.split(jax.random.fold_in(key, 17), 7)
    fast_share = 0.5
    element = jax.random.uniform(address_block[3], (TEXT_LENGTH, D), jnp.float32, 0.5, 1.5)
    fast = jax.random.uniform(address_block[0], (HOSTED_ATTENDERS,), jnp.float32) < fast_share
    slow_rate = jnp.exp(jax.random.uniform(address_block[1], (HOSTED_ATTENDERS, CHANNEL_COUNT), jnp.float32, math.log(0.2), math.log(0.8))) / TEXT_LENGTH
    fast_rate = jnp.exp(jax.random.uniform(address_block[2], (HOSTED_ATTENDERS, CHANNEL_COUNT), jnp.float32, math.log(1.0 / 50.0), math.log(1.0 / 25.0)))
    forget_speed = jnp.where(fast[:, None], fast_rate, slow_rate).reshape(D)
    slabs = TEXT_LENGTH // TOK_DEV
    slab_factor = jax.random.uniform(address_block[4], (slabs, 1, 1), jnp.float32, 0.6, 1.5)
    forget_weighting = (element.reshape(slabs, TOK_DEV, D) * slab_factor).reshape(TEXT_LENGTH, D)
    block_offsets = jax.random.randint(address_block[5], (3,), 0, TEXT_LENGTH)
    forget_shrinkage = jax.random.uniform(address_block[6], (3,), jnp.float32, 0.2, 0.35)
    word_spans = jnp.zeros((TEXT_LENGTH,), jnp.float32).at[block_offsets].add(-jnp.log(1.0 - forget_shrinkage))
    return (-(forget_speed[None, :] * forget_weighting) - word_spans[:, None]).astype(jnp.bfloat16)


def steps_of(key, extent, cuts, low, top_value):
    loudness, own = 1.0, jax.random.fold_in(key, 6)
    for axis_at, shards_of in cuts:
        heights = jnp.exp(jax.random.uniform(jax.random.fold_in(own, axis_at), (shards_of,), jnp.float32, low / len(cuts), top_value / len(cuts)))
        loudness = loudness * jnp.repeat(heights, extent[axis_at] // shards_of).reshape([-1 if axis == axis_at else 1 for axis in range(len(extent))])
    return loudness


def centred(key, shape, width, bound, cuts=(), dtype=jnp.bfloat16):
    entries = jax.random.normal(key, shape, jnp.float32) * width
    if len(cuts) > 0:
        entries = steps_of(key, shape, cuts, -0.22, 0.18) * entries
    return jnp.clip(entries, min=-bound, max=bound).astype(dtype)


def setup_inputs(seed: int = 0) -> dict:
    streams_of = jax.random.split(jax.random.key(seed), 9)
    query_vectors = centred(streams_of[0], (TEXT_LENGTH, D), 1.0, 6.0, ((0, 32),))
    address_vectors = centred(streams_of[1], (TEXT_LENGTH, D), 0.125, 0.75, ((0, 32),))
    payload_vectors = centred(streams_of[2], (TEXT_LENGTH, D), 1.0, 6.0, ((0, 32),))
    forget_logarithms = draw_forget_logarithms(jax.random.fold_in(streams_of[8], 71), 0)
    pre_sigmoid_filter = centred(streams_of[4], (TEXT_LENGTH, D), 1.0, 6.0, ((0, 32),))
    current_reward_table = jnp.clip(jax.random.uniform(streams_of[5], (HOSTED_ATTENDERS, CHANNEL_COUNT), jnp.float32, -0.5, 1.5), -0.5, 1.5)
    cluster_standardize_weight = jnp.clip(1.0 + 0.15 * jax.random.normal(streams_of[6], (D,), jnp.float32), 0.25, 1.75)
    cluster_standardize_offset = centred(streams_of[7], (D,), 0.3, 1.5, (), jnp.float32)
    return dict(query_vectors=query_vectors, address_vectors=address_vectors, payload_vectors=payload_vectors, forget_logarithms=forget_logarithms, pre_sigmoid_filter=pre_sigmoid_filter, current_reward_table=current_reward_table, cluster_standardize_weight=cluster_standardize_weight, cluster_standardize_offset=cluster_standardize_offset)


def reference(query_vectors, address_vectors, payload_vectors, forget_logarithms, pre_sigmoid_filter, current_reward_table, cluster_standardize_weight, cluster_standardize_offset):
    highest = lax.Precision.HIGHEST
    blocks = TEXT_LENGTH // TOK_DEV

    def prepare(array):
        return array.astype(jnp.float32).reshape(blocks, TOK_DEV, HOSTED_ATTENDERS, CHANNEL_COUNT)
    later = lax.broadcasted_iota(jnp.int32, (TOK_DEV, TOK_DEV), 0)
    earlier = lax.broadcasted_iota(jnp.int32, (TOK_DEV, TOK_DEV), 1)
    strict = later > earlier

    def advance(state, pieces):
        incoming_memory, address_block, payload_block, forget_multiplier = pieces
        cumul = jnp.cumsum(forget_multiplier, axis=0)
        before = cumul - forget_multiplier
        final = cumul[-1]
        scaled_receptance = incoming_memory * jnp.exp(before)
        scaled_k = address_block * jnp.exp(-cumul)
        end_keys = address_block * jnp.exp(final[None] - cumul)
        scores = jnp.einsum('thc,shc->hts', scaled_receptance, scaled_k, precision=highest)
        scores = jnp.where(strict[None], scores, jnp.float32(0.0))
        diagonal_piece = lax.optimization_barrier(jnp.sum(incoming_memory * current_reward_table[None] * address_block, axis=2))
        mixed_output = jnp.einsum('hts,shj->thj', scores, payload_block, precision=highest)
        mixed_output = mixed_output + jnp.einsum('thc,hcj->thj', scaled_receptance, state, precision=highest)
        mixed_output = mixed_output + diagonal_piece[:, :, None] * payload_block
        state = jnp.exp(final)[:, :, None] * state + jnp.einsum('shc,shj->hcj', end_keys, payload_block, precision=highest)
        return (state, mixed_output)
    start_state = jnp.zeros((HOSTED_ATTENDERS, CHANNEL_COUNT, CHANNEL_COUNT), jnp.float32)
    _, outputs = lax.scan(advance, start_state, (prepare(query_vectors), prepare(address_vectors), prepare(payload_vectors), prepare(forget_logarithms)))
    outputs = outputs.reshape(TEXT_LENGTH, HOSTED_ATTENDERS, CHANNEL_COUNT)
    center = outputs - lax.optimization_barrier(jnp.mean(outputs, axis=2, keepdims=True))
    spread = lax.optimization_barrier(jnp.mean(center * center, axis=2, keepdims=True))
    normed = (center * lax.rsqrt(spread + 1e-05)).reshape(TEXT_LENGTH, D)
    gate = pre_sigmoid_filter.astype(jnp.float32)
    return ((normed * cluster_standardize_weight[None] + cluster_standardize_offset[None]) * gate * jax.nn.sigmoid(gate)).astype(jnp.bfloat16)
```

```python
import functools

import jax
import jax.numpy as jnp
from jax import lax
from jax.experimental import pallas as pl
from jax.experimental.pallas import tpu as pltpu
from jax.sharding import PartitionSpec as P

CHANNELS = 64
LANES = 256
HEADS = LANES // CHANNELS
BLOCK = 64
PLANE = 4
F32 = jnp.float32
BF16 = jnp.bfloat16


def split(value):
    high = value.astype(BF16)
    return high, (value - high.astype(F32)).astype(BF16)


def dot(left, right):
    return lax.dot_general(left, right, (((1,), (0,)), ((), ())), preferred_element_type=F32)


def dot_nt(left, right):
    return lax.dot_general(left, right, (((1,), (1,)), ((), ())), preferred_element_type=F32)


def same_head(value):
    rows = lax.broadcasted_iota(jnp.int32, (LANES, LANES), 0) // CHANNELS
    columns = lax.broadcasted_iota(jnp.int32, (LANES, LANES), 1) // CHANNELS
    return jnp.where(rows == columns, F32(value), F32(0.0)).astype(BF16)


def head_of_lane(rows):
    return lax.broadcasted_iota(jnp.int32, (rows, LANES), 1) // CHANNELS


def own_blocks(stacked, rows):
    lane_head = head_of_lane(rows)
    picked = stacked[:rows]
    for head in range(1, HEADS):
        picked = jnp.where(lane_head == head, stacked[head * rows : (head + 1) * rows], picked)
    return picked


def cumulate(decay):
    length = decay.shape[0]
    rows = lax.broadcasted_iota(jnp.int32, (length, length), 0)
    columns = lax.broadcasted_iota(jnp.int32, (length, length), 1)
    lower = jnp.where(rows >= columns, F32(1.0), F32(0.0)).astype(BF16)
    return dot(lower, decay)


def ends_of(key, value, decay, out_ref):
    length = decay.shape[0]
    cumul = cumulate(decay)
    final = cumul[length - 1 : length]
    high, low = split(key.astype(F32) * jnp.exp(final - cumul))
    turned = value.astype(F32).T.astype(BF16)
    out_ref[0, :CHANNELS, :] = own_blocks(dot(turned, high) + dot(turned, low), CHANNELS)
    out_ref[0, CHANNELS:, :] = jnp.broadcast_to(jnp.exp(final), (8, LANES))


def ends_kernel(core_ref, km, vm, wm, kt, vt, wt, mine_ref, theirs_ref):
    ends_of(kt[...], vt[...], wt[...], theirs_ref)
    ends_of(km[...], vm[...], wm[...], mine_ref)


def within_kernel(core_ref, r_ref, k_ref, v_ref, w_ref, bonus_ref, out_ref):
    r, k, v, w = r_ref[...].astype(F32), k_ref[...].astype(F32), v_ref[...], w_ref[...]
    length = w.shape[0]
    cumul = cumulate(w)
    before = cumul - w.astype(F32)
    lane_head = head_of_lane(BLOCK)
    diagonal_high, diagonal_low = split(r * bonus_ref[...] * k)
    ones = same_head(1.0)
    diagonal = dot(diagonal_high, ones) + dot(diagonal_low, ones)
    pieces = []
    for start in range(0, length, BLOCK):
        stop = start + BLOCK
        middle = start + BLOCK // 2 - 1
        reference = cumul[middle : middle + 1]
        receptance = r[start:stop] * jnp.exp(before[start:stop] - reference)
        stacked = jnp.concatenate(
            [jnp.where(lane_head == head, receptance, F32(0.0)) for head in range(HEADS)], axis=0
        )
        r_high, r_low = split(stacked)
        k_high, k_low = split(k[:stop] * jnp.exp(reference - cumul[:stop]))
        scores = dot_nt(r_high, k_high) + dot_nt(r_low, k_high) + dot_nt(r_high, k_low)
        later = lax.broadcasted_iota(jnp.int32, scores.shape, 0) % BLOCK + start
        earlier = lax.broadcasted_iota(jnp.int32, scores.shape, 1)
        s_high, s_low = split(jnp.where(later > earlier, scores, F32(0.0)))
        pieces.append(own_blocks(dot(s_high, v[:stop]) + dot(s_low, v[:stop]), BLOCK))
    mixed = jnp.concatenate(pieces, axis=0) + diagonal * v.astype(F32)
    m_high, m_low = split(mixed)
    share = same_head(1.0 / CHANNELS)
    out_ref[0] = mixed - (dot(m_high, share) + dot(m_low, share))
    out_ref[1] = r * jnp.exp(before)


def finish_kernel(
    place_ref, p0, p1, p2, p3, ends_mine, ends_other, in_mine, in_other, g_mine, g_other,
    gain_ref, bias_ref, out_ref, state_ref,
):
    core, place = place_ref[0], place_ref[1]
    rows = CHANNELS // PLANE
    for step, piece in enumerate((p0, p1, p2, p3)):
        at = pl.multiple_of(lax.bitwise_xor(place, step) * rows, rows)
        state_ref[pl.ds(at, rows), :] = piece[...]
    length = in_mine.shape[1]
    first = core == 0
    share = same_head(1.0 / CHANNELS)
    mask_rows = lax.broadcasted_iota(jnp.int32, (LANES, LANES), 0) // CHANNELS
    mask = mask_rows == head_of_lane(LANES)
    early = jnp.where(first, ends_mine[0], ends_other[0])
    state = state_ref[...]
    for half in range(2):
        local = core == half
        if half == 1:
            state = early[CHANNELS : CHANNELS + 1] * state + early[:CHANNELS]
        centred = state - jnp.mean(state, axis=0, keepdims=True)
        wide = jnp.where(mask, jnp.concatenate([centred] * HEADS, axis=0), F32(0.0))
        s_high, s_low = split(wide)
        r_high, r_low = split(jnp.where(local, in_mine[1], in_other[1]))
        mixed = jnp.where(local, in_mine[0], in_other[0])
        mixed = mixed + (dot_nt(r_high, s_high) + dot_nt(r_low, s_high) + dot_nt(r_high, s_low))
        q_high, q_low = split(mixed * mixed)
        spread = dot(q_high, share) + dot(q_low, share)
        normed = mixed * lax.rsqrt(spread + 1e-5)
        gate = jnp.where(local, g_mine[...].astype(F32), g_other[...].astype(F32))
        gated = (normed * gain_ref[...] + bias_ref[...]) * gate / (1.0 + jnp.exp(-gate))
        out_ref[half * length : (half + 1) * length, :] = gated.astype(BF16)


def body(r, k, v, w, gate, bonus, gain, bias):
    length, width = r.shape
    cores, count = lax.axis_size("head"), lax.axis_size("seq")
    assert cores == 2 and count % PLANE == 0
    half = width // cores
    groups = half // LANES
    core, position = lax.axis_index("head"), lax.axis_index("seq")
    place = position % PLANE
    where = jnp.stack([core, place]).astype(jnp.int32)
    swap = [(0, 1), (1, 0)]

    def lanes(side):
        def index(g, ref):
            c = ref[0] if side == 0 else 1 - ref[0]
            return (0, c * groups + g)
        return index

    token = lambda side: pl.BlockSpec((length, LANES), lanes(side))
    row = lambda side: pl.BlockSpec((1, LANES), lanes(side))
    ends_spec = pl.BlockSpec((1, CHANNELS + 8, LANES), lambda g, ref: (g, 0, 0))
    ends_shape = jax.ShapeDtypeStruct((groups, CHANNELS + 8, LANES), F32)
    mine, theirs = pl.pallas_call(
        ends_kernel,
        out_shape=[ends_shape, ends_shape],
        grid_spec=pltpu.PrefetchScalarGridSpec(
            num_scalar_prefetch=1,
            grid=(groups,),
            in_specs=[token(0)] * 3 + [token(1)] * 3,
            out_specs=[ends_spec, ends_spec],
        ),
        name="ends",
    )(where, k, v, w, k, v, w)
    other = lax.ppermute(theirs, "head", swap)

    pair_spec = pl.BlockSpec((2, length, LANES), lambda g, ref: (0, 0, g))

    def within(side):
        return pl.pallas_call(
            within_kernel,
            out_shape=jax.ShapeDtypeStruct((2, length, half), F32),
            grid_spec=pltpu.PrefetchScalarGridSpec(
                num_scalar_prefetch=1,
                grid=(groups,),
                in_specs=[token(side)] * 4 + [row(side)],
                out_specs=pair_spec,
            ),
            name="within_other" if side else "within_mine",
        )(where, r, k, v, w, bonus.reshape(1, width))

    in_other = lax.ppermute(within(1), "head", swap)
    in_mine = within(0)
    gate_other = lax.ppermute(gate, "head", swap)

    first = jnp.where(core == 0, mine, other)
    second = jnp.where(core == 0, other, mine)
    chip = first[:, :CHANNELS] * second[:, CHANNELS : CHANNELS + 1] + second[:, :CHANNELS]
    chip_decay = first[:, CHANNELS] * second[:, CHANNELS]
    rows = CHANNELS // PLANE
    quarters = chip.reshape(groups, PLANE, rows, LANES)
    packed_rows = groups * rows

    def pack(state, decay):
        pad = jnp.zeros((-groups % 8, LANES), F32)
        return jnp.concatenate([state.reshape(packed_rows, LANES), decay, pad], axis=0)

    def unpack(packed):
        state = packed[:packed_rows].reshape(groups, rows, LANES)
        return state, packed[packed_rows : packed_rows + groups]

    def to_place(step):
        return [(i, i ^ step) for i in range(count)]

    def quarter(step):
        return pack(
            lax.dynamic_index_in_dim(quarters, place ^ step, 1, keepdims=False), chip_decay
        )

    got = [quarter(0)] + [
        lax.ppermute(quarter(step), "seq", to_place(step)) for step in range(1, PLANE)
    ]

    def choose(options, at):
        picked = options[0]
        for index in range(1, PLANE):
            picked = jnp.where(at == index, options[index], picked)
        return picked

    def join(earlier, later):
        return (later[1][:, None, :] * earlier[0] + later[0], earlier[1] * later[1])

    slabs = [unpack(choose(got, place ^ slab)) for slab in range(PLANE)]
    prefixes = [(jnp.zeros_like(slabs[0][0]), jnp.ones_like(slabs[0][1]))]
    for slab in slabs:
        prefixes.append(join(prefixes[-1], slab))
    window = prefixes.pop()
    before = None
    distance = 1
    while distance < count // PLANE:
        hop = distance * PLANE
        got = unpack(
            lax.ppermute(pack(*window), "seq", [(i, i + hop) for i in range(count - hop)])
        )
        before = got if before is None else join(got, before)
        window = join(got, window)
        distance *= 2
    if before is not None:
        finals = [join(before, prefix)[0] for prefix in prefixes]
    else:
        finals = [prefix[0] for prefix in prefixes]
    finals = [final.reshape(packed_rows, LANES) for final in finals]
    states = [choose(finals, place)] + [
        lax.ppermute(choose(finals, place ^ step), "seq", to_place(step))
        for step in range(1, PLANE)
    ]
    piece_spec = pl.BlockSpec((rows, LANES), lambda g, ref: (g, 0))
    return pl.pallas_call(
        finish_kernel,
        out_shape=jax.ShapeDtypeStruct((cores * length, half), BF16),
        grid_spec=pltpu.PrefetchScalarGridSpec(
            num_scalar_prefetch=1,
            grid=(groups,),
            in_specs=[piece_spec] * PLANE
            + [ends_spec] * 2
            + [pair_spec] * 2
            + [token(0)] * 2
            + [row(0)] * 2,
            out_specs=pl.BlockSpec((cores * length, LANES), lambda g, ref: (0, g)),
            scratch_shapes=[pltpu.VMEM((CHANNELS, LANES), F32)],
        ),
        name="finish",
    )(where, *states, mine, other, in_mine, in_other, gate, gate_other,
      gain.reshape(1, width), bias.reshape(1, width))


def solution(mesh):
    tokens = P(("seq", "head"), None)
    return jax.shard_map(
        body,
        mesh=mesh,
        in_specs=(tokens,) * 5 + (P(), P(), P()),
        out_specs=P("seq", "head"),
        check_vma=False,
    )
```

```python
import functools

import jax
import jax.numpy as jnp
from jax import lax
from jax.experimental import pallas as pl
from jax.experimental.pallas import tpu as pltpu
from jax.sharding import PartitionSpec as P

CHANNELS = 64
LANES = 256
HEADS = LANES // CHANNELS
BLOCK = 64
PLANE = 4
VMEM_LIMIT = 16 * 2**20
F32 = jnp.float32
BF16 = jnp.bfloat16


def split(value):
    high = value.astype(BF16)
    return high, (value - high.astype(F32)).astype(BF16)


def dot(left, right):
    return lax.dot_general(left, right, (((1,), (0,)), ((), ())), preferred_element_type=F32)


def dot_nt(left, right):
    return lax.dot_general(left, right, (((1,), (1,)), ((), ())), preferred_element_type=F32)


def same_head(value):
    rows = lax.broadcasted_iota(jnp.int32, (LANES, LANES), 0) // CHANNELS
    columns = lax.broadcasted_iota(jnp.int32, (LANES, LANES), 1) // CHANNELS
    return jnp.where(rows == columns, F32(value), F32(0.0)).astype(BF16)


def head_of_lane(rows):
    return lax.broadcasted_iota(jnp.int32, (rows, LANES), 1) // CHANNELS


def own_blocks(stacked, rows):
    lane_head = head_of_lane(rows)
    picked = stacked[:rows]
    for head in range(1, HEADS):
        picked = jnp.where(lane_head == head, stacked[head * rows : (head + 1) * rows], picked)
    return picked


def cumulate(decay):
    length = decay.shape[0]
    rows = lax.broadcasted_iota(jnp.int32, (length, length), 0)
    columns = lax.broadcasted_iota(jnp.int32, (length, length), 1)
    lower = jnp.where(rows >= columns, F32(1.0), F32(0.0)).astype(BF16)
    return dot(lower, decay)


def ends_of(key, value, decay):
    length = decay.shape[0]
    cumul = cumulate(decay)
    final = cumul[length - 1 : length]
    high, low = split(key.astype(F32) * jnp.exp(final - cumul))
    turned = value.astype(F32).T.astype(BF16)
    wide = dot(
        jnp.concatenate([turned, turned], axis=1), jnp.concatenate([high, low], axis=0)
    )
    return own_blocks(wide, CHANNELS), jnp.broadcast_to(jnp.exp(final), (8, LANES))


def ends_kernel(k_ref, v_ref, w_ref, mine_ref, theirs_ref):
    groups = mine_ref.shape[0]
    for side, out_ref in ((1, theirs_ref), (0, mine_ref)):
        for group in range(groups):
            at = lanes_at(side, group, groups)
            state, decay = ends_of(k_ref[:, at], v_ref[:, at], w_ref[:, at])
            out_ref[group, :CHANNELS, :] = state
            out_ref[group, CHANNELS:, :] = decay


def lanes_at(side, group, groups):
    core = lax.axis_index("head")
    core = core if side == 0 else 1 - core
    return pl.ds(pl.multiple_of((core * groups + group) * LANES, LANES), LANES)


def within_kernel(side, r_ref, k_ref, v_ref, w_ref, table_ref, out_ref):
    groups = out_ref.shape[2] // LANES
    length = w_ref.shape[0]
    lane_head = head_of_lane(BLOCK)
    ones = same_head(1.0)
    share = same_head(1.0 / CHANNELS)
    shape = (HEADS * length, length)
    row = lax.broadcasted_iota(jnp.int32, shape, 0)
    later = row // (HEADS * BLOCK) * BLOCK + row % BLOCK
    strict = later > lax.broadcasted_iota(jnp.int32, shape, 1)
    for group in range(groups):
        at = lanes_at(side, group, groups)
        out = pl.ds(group * LANES, LANES)
        r, k, v, w = r_ref[:, at].astype(F32), k_ref[:, at].astype(F32), v_ref[:, at], w_ref[:, at]
        cumul = cumulate(w)
        before = cumul - w.astype(F32)
        out_ref[1, :, out] = r * jnp.exp(before)
        diagonal_high, diagonal_low = split(r * table_ref[0:1, at] * k)
        diagonal = dot(diagonal_high, ones) + dot(diagonal_low, ones)
        pieces = []
        for start in range(0, length, BLOCK):
            stop = start + BLOCK
            middle = start + BLOCK // 2 - 1
            reference = cumul[middle : middle + 1]
            receptance = r[start:stop] * jnp.exp(before[start:stop] - reference)
            stacked = jnp.concatenate(
                [jnp.where(lane_head == head, receptance, F32(0.0)) for head in range(HEADS)],
                axis=0,
            )
            keys = k[:stop] * jnp.exp(reference - cumul[:stop])
            if stop < length:
                keys = jnp.concatenate([keys, jnp.zeros((length - stop, LANES), F32)], axis=0)
            r_high, r_low = split(stacked)
            k_high, k_low = split(keys)
            pieces.append(dot_nt(r_high, k_high) + dot_nt(r_low, k_high) + dot_nt(r_high, k_low))
        s_high, s_low = split(jnp.where(strict, jnp.concatenate(pieces, axis=0), F32(0.0)))
        wide = dot(jnp.concatenate([s_high, s_low], axis=1), jnp.concatenate([v, v], axis=0))
        step = HEADS * BLOCK
        mixed = jnp.concatenate(
            [own_blocks(wide[i * step : (i + 1) * step], BLOCK) for i in range(length // BLOCK)],
            axis=0,
        )
        mixed = mixed + diagonal * v.astype(F32)
        m_high, m_low = split(mixed)
        out_ref[0, :, out] = mixed - (dot(m_high, share) + dot(m_low, share))


def finish_kernel(
    p0, p1, p2, p3, ends_mine, ends_other, in_mine, in_other, g_mine, g_other, table_ref,
    out_ref, state_ref,
):
    core = lax.axis_index("head")
    place = lax.axis_index("seq") % PLANE
    groups = ends_mine.shape[0]
    rows = CHANNELS // PLANE
    length = in_mine.shape[1]
    first = core == 0
    share = same_head(1.0 / CHANNELS)
    mask = lax.broadcasted_iota(jnp.int32, (LANES, LANES), 0) // CHANNELS == head_of_lane(LANES)
    for step, piece in enumerate((p0, p1, p2, p3)):
        source = lax.bitwise_xor(place, step) * rows
        for group in range(groups):
            at = pl.multiple_of(source + group * CHANNELS, rows)
            state_ref[pl.ds(at, rows), :] = piece[group * rows : (group + 1) * rows, :]
    for group in range(groups):
        at = lanes_at(0, group, groups)
        out = pl.ds(group * LANES, LANES)
        early = jnp.where(first, ends_mine[group], ends_other[group])
        state = state_ref[group * CHANNELS : (group + 1) * CHANNELS, :]
        for half in range(2):
            local = core == half
            if half == 1:
                state = early[CHANNELS : CHANNELS + 1] * state + early[:CHANNELS]
            centred = state - jnp.mean(state, axis=0, keepdims=True)
            wide = jnp.where(mask, jnp.concatenate([centred] * HEADS, axis=0), F32(0.0))
            s_high, s_low = split(wide)
            r_high, r_low = split(jnp.where(local, in_mine[1, :, out], in_other[1, :, out]))
            mixed = jnp.where(local, in_mine[0, :, out], in_other[0, :, out])
            mixed = mixed + (
                dot_nt(r_high, s_high) + dot_nt(r_low, s_high) + dot_nt(r_high, s_low)
            )
            q_high, q_low = split(mixed * mixed)
            spread = dot(q_high, share) + dot(q_low, share)
            normed = mixed * lax.rsqrt(spread + 1e-5)
            gate = jnp.where(local, g_mine[:, at].astype(F32), g_other[:, at].astype(F32))
            gated = (normed * table_ref[1:2, at] + table_ref[2:3, at]) * gate
            gated = gated / (1.0 + jnp.exp(-gate))
            out_ref[half * length : (half + 1) * length, out] = gated.astype(BF16)


def body(r, k, v, w, gate, bonus, gain, bias):
    length, width = r.shape
    cores, count = lax.axis_size("head"), lax.axis_size("seq")
    assert cores == 2 and count % PLANE == 0
    half = width // cores
    groups = half // LANES
    core, position = lax.axis_index("head"), lax.axis_index("seq")
    place = position % PLANE
    swap = [(0, 1), (1, 0)]
    params = pltpu.CompilerParams(vmem_limit_bytes=VMEM_LIMIT)
    table = jnp.stack([bonus.reshape(width), gain, bias])

    ends_shape = jax.ShapeDtypeStruct((groups, CHANNELS + 8, LANES), F32)
    mine, theirs = pl.pallas_call(
        ends_kernel, out_shape=[ends_shape, ends_shape], compiler_params=params, name="ends"
    )(k, v, w)
    other = lax.ppermute(theirs, "head", swap)

    def within(side):
        return pl.pallas_call(
            functools.partial(within_kernel, side),
            out_shape=jax.ShapeDtypeStruct((2, length, half), F32),
            compiler_params=params,
            name="within_other" if side else "within_mine",
        )(r, k, v, w, table)

    in_other = lax.ppermute(within(1), "head", swap)
    in_mine = within(0)
    gate_other = lax.ppermute(gate, "head", swap)

    first = jnp.where(core == 0, mine, other)
    second = jnp.where(core == 0, other, mine)
    chip = first[:, :CHANNELS] * second[:, CHANNELS : CHANNELS + 1] + second[:, :CHANNELS]
    chip_decay = first[:, CHANNELS] * second[:, CHANNELS]
    rows = CHANNELS // PLANE
    quarters = chip.reshape(groups, PLANE, rows, LANES)
    packed_rows = groups * rows

    def pack(state, decay):
        pad = jnp.zeros((-groups % 8, LANES), F32)
        return jnp.concatenate([state.reshape(packed_rows, LANES), decay, pad], axis=0)

    def unpack(packed):
        state = packed[:packed_rows].reshape(groups, rows, LANES)
        return state, packed[packed_rows : packed_rows + groups]

    def to_place(step):
        return [(i, i ^ step) for i in range(count)]

    def quarter(step):
        return pack(
            lax.dynamic_index_in_dim(quarters, place ^ step, 1, keepdims=False), chip_decay
        )

    got = [quarter(0)] + [
        lax.ppermute(quarter(step), "seq", to_place(step)) for step in range(1, PLANE)
    ]

    def choose(options, at):
        picked = options[0]
        for index in range(1, PLANE):
            picked = jnp.where(at == index, options[index], picked)
        return picked

    def join(earlier, later):
        return (later[1][:, None, :] * earlier[0] + later[0], earlier[1] * later[1])

    slabs = [unpack(choose(got, place ^ slab)) for slab in range(PLANE)]
    prefixes = [(jnp.zeros_like(slabs[0][0]), jnp.ones_like(slabs[0][1]))]
    for slab in slabs:
        prefixes.append(join(prefixes[-1], slab))
    window = prefixes.pop()
    before = None
    distance = 1
    while distance < count // PLANE:
        hop = distance * PLANE
        got = unpack(
            lax.ppermute(pack(*window), "seq", [(i, i + hop) for i in range(count - hop)])
        )
        before = got if before is None else join(got, before)
        window = join(got, window)
        distance *= 2
    if before is not None:
        finals = [join(before, prefix)[0] for prefix in prefixes]
    else:
        finals = [prefix[0] for prefix in prefixes]
    finals = [final.reshape(packed_rows, LANES) for final in finals]
    states = [choose(finals, place)] + [
        lax.ppermute(choose(finals, place ^ step), "seq", to_place(step))
        for step in range(1, PLANE)
    ]
    return pl.pallas_call(
        finish_kernel,
        out_shape=jax.ShapeDtypeStruct((cores * length, half), BF16),
        scratch_shapes=[pltpu.VMEM((groups * CHANNELS, LANES), F32)],
        compiler_params=params,
        name="finish",
    )(*states, mine, other, in_mine, in_other, gate, gate_other, table)


def solution(mesh):
    tokens = P(("seq", "head"), None)
    return jax.shard_map(
        body,
        mesh=mesh,
        in_specs=(tokens,) * 5 + (P(), P(), P()),
        out_specs=P("seq", "head"),
        check_vma=False,
    )
```

```python
import functools

import jax
import jax.numpy as jnp
from jax import lax
from jax.experimental import pallas as pl
from jax.experimental.pallas import tpu as pltpu
from jax.sharding import PartitionSpec as P


CHANNELS = 64
TILE = 128
LANES = 256
HEADS = LANES // CHANNELS
BLOCK = 64
PLANE = 4
ROWS = CHANNELS // PLANE
VMEM_LIMIT = 12 * 2**20
F32 = jnp.float32
BF16 = jnp.bfloat16


def split(value):
    high = value.astype(BF16)
    return high, (value - high.astype(F32)).astype(BF16)


def dot(left, right):
    return lax.dot_general(left, right, (((1,), (0,)), ((), ())), preferred_element_type=F32)


def dot_nt(left, right):
    return lax.dot_general(left, right, (((1,), (1,)), ((), ())), preferred_element_type=F32)


def same_head(value):
    rows = lax.broadcasted_iota(jnp.int32, (LANES, LANES), 0) // CHANNELS
    columns = lax.broadcasted_iota(jnp.int32, (LANES, LANES), 1) // CHANNELS
    return jnp.where(rows == columns, F32(value), F32(0.0)).astype(BF16)


def half_masks(rows):
    left = lax.broadcasted_iota(jnp.int32, (rows, TILE), 1) < CHANNELS
    one, zero = F32(1.0), F32(0.0)
    return jnp.where(left, one, zero).astype(BF16), jnp.where(left, zero, one).astype(BF16)


def spread_heads(value, masks):
    zero = jnp.zeros((value.shape[0], TILE), value.dtype)
    pieces = []
    for head in range(HEADS):
        tile = head // 2
        kept = value[:, tile * TILE : (tile + 1) * TILE] * masks[head % 2]
        pieces.append(
            jnp.concatenate([kept if i == tile else zero for i in range(LANES // TILE)], axis=1)
        )
    return jnp.concatenate(pieces, axis=0)


def own_blocks(stacked, rows):
    left = lax.broadcasted_iota(jnp.int32, (rows, TILE), 1) < CHANNELS
    pieces = []
    for tile in range(LANES // TILE):
        part = stacked[:, tile * TILE : (tile + 1) * TILE]
        head = 2 * tile
        pieces.append(
            jnp.where(
                left,
                part[head * rows : (head + 1) * rows],
                part[(head + 1) * rows : (head + 2) * rows],
            )
        )
    return jnp.concatenate(pieces, axis=1)


def cumulate(decay):
    length = decay.shape[0]
    rows = lax.broadcasted_iota(jnp.int32, (length, length), 0)
    columns = lax.broadcasted_iota(jnp.int32, (length, length), 1)
    lower = jnp.where(rows >= columns, F32(1.0), F32(0.0)).astype(BF16)
    return dot(lower, decay)


def lanes_at(side, group, groups):
    core = lax.axis_index("head")
    core = core if side == 0 else 1 - core
    return pl.ds(pl.multiple_of((core * groups + group) * LANES, LANES), LANES)


def half_at(side, half):
    core = lax.axis_index("head")
    core = core if side == 0 else 1 - core
    return pl.ds(pl.multiple_of(core * half, LANES), half)


def ends_of(key, value, decay):
    length = decay.shape[0]
    cumul = cumulate(decay)
    final = cumul[length - 1 : length]
    high, low = split(key.astype(F32) * jnp.exp(final - cumul))
    turned = value.astype(F32).T.astype(BF16)
    wide = dot(
        jnp.concatenate([turned, turned], axis=1), jnp.concatenate([high, low], axis=0)
    )
    return own_blocks(wide, CHANNELS), jnp.broadcast_to(jnp.exp(final), (8, LANES))


def ends_kernel(k_ref, v_ref, w_ref, mine_ref, theirs_ref, k_buf, v_buf, w_buf, sems):
    groups = mine_ref.shape[0]
    half = groups * LANES
    copies = {}
    for side in (1, 0):
        at = half_at(side, half)
        for index, (ref, buf) in enumerate(((w_ref, w_buf), (k_ref, k_buf), (v_ref, v_buf))):
            copies[side, index] = pltpu.make_async_copy(
                ref.at[:, at], buf.at[side], sems.at[side, index]
            )
            copies[side, index].start()
    for side, out_ref in ((1, theirs_ref), (0, mine_ref)):
        for index in range(3):
            copies[side, index].wait()
        for group in range(groups):
            at = pl.ds(group * LANES, LANES)
            state, decay = ends_of(k_buf[side, :, at], v_buf[side, :, at], w_buf[side, :, at])
            out_ref[group, :CHANNELS, :] = state
            out_ref[group, CHANNELS:, :] = decay


def combine_kernel(mine_ref, other_ref, q0, q1, q2, q3, state_ref):
    core = lax.axis_index("head")
    place = lax.axis_index("seq") % PLANE
    groups = mine_ref.shape[0]
    first = core == 0
    outs = (q0, q1, q2, q3)
    for out in outs:
        out[...] = jnp.zeros_like(out)
    for group in range(groups):
        mine, other = mine_ref[group], other_ref[group]
        early, late = jnp.where(first, mine, other), jnp.where(first, other, mine)
        decay = late[CHANNELS : CHANNELS + 1]
        state_ref[...] = early[:CHANNELS] * decay + late[:CHANNELS]
        both = early[CHANNELS : CHANNELS + 1] * decay
        for step, out in enumerate(outs):
            at = pl.multiple_of(lax.bitwise_xor(place, step) * ROWS, ROWS)
            out[group * ROWS : (group + 1) * ROWS, :] = state_ref[pl.ds(at, ROWS), :]
            at = groups * ROWS + group
            out[at : at + 1, :] = both


def plane_kernel(q0, q1, q2, q3, total_ref, prefix_ref, slab_ref):
    place = lax.axis_index("seq") % PLANE
    groups = total_ref.shape[0] // ROWS
    for step, piece in enumerate((q0, q1, q2, q3)):
        slab_ref[lax.bitwise_xor(place, step)] = piece[...]
    total_ref[...] = jnp.zeros_like(total_ref)
    for group in range(groups):
        rows = slice(group * ROWS, (group + 1) * ROWS)
        at = groups * ROWS + group
        row = slice(at, at + 1)
        state = jnp.zeros((ROWS, LANES), F32)
        decay = jnp.ones((1, LANES), F32)
        for slab in range(PLANE):
            prefix_ref[slab, rows, :] = state
            prefix_ref[slab, row, :] = decay
            step = slab_ref[slab, row, :]
            state = step * state + slab_ref[slab, rows, :]
            decay = step * decay
        total_ref[rows, :] = state
        total_ref[row, :] = decay


def round_kernel(bit, first_round, total_ref, got_ref, before_ref, total_out, before_out):
    plane = lax.axis_index("seq") // PLANE
    upper = lax.bitwise_and(plane, bit) != 0
    groups = total_ref.shape[0] // ROWS
    total_out[...] = jnp.zeros_like(total_out)
    before_out[...] = jnp.zeros_like(before_out)
    for group in range(groups):
        rows = slice(group * ROWS, (group + 1) * ROWS)
        at = groups * ROWS + group
        row = slice(at, at + 1)
        total, got = total_ref[rows, :], got_ref[rows, :]
        total_decay, got_decay = total_ref[row, :], got_ref[row, :]
        low, high = jnp.where(upper, got, total), jnp.where(upper, total, got)
        total_out[rows, :] = jnp.where(upper, total_decay, got_decay) * low + high
        total_out[row, :] = total_decay * got_decay
        if first_round:
            before = jnp.where(upper, got, F32(0.0))
            before_decay = jnp.where(upper, got_decay, F32(1.0))
        else:
            decay = before_ref[row, :]
            before = before_ref[rows, :]
            before = jnp.where(upper, decay * got + before, before)
            before_decay = jnp.where(upper, got_decay * decay, decay)
        before_out[rows, :] = before
        before_out[row, :] = before_decay


def back_kernel(bit, prefix_ref, before_ref, got_ref, p0, p1, p2, p3):
    seq = lax.axis_index("seq")
    place = seq % PLANE
    upper = lax.bitwise_and(seq // PLANE, bit) != 0
    groups = p0.shape[0] // ROWS
    for group in range(groups):
        rows = slice(group * ROWS, (group + 1) * ROWS)
        at = groups * ROWS + group
        row = slice(at, at + 1)
        before = before_ref[rows, :]
        before = jnp.where(upper, before_ref[row, :] * got_ref[rows, :] + before, before)
        for step, out in enumerate((p0, p1, p2, p3)):
            to = lax.bitwise_xor(place, step)
            out[rows, :] = prefix_ref[to, row, :] * before + prefix_ref[to, rows, :]


def within_kernel(side, r_ref, k_ref, v_ref, w_ref, g_ref, table_ref, out_ref):
    groups = out_ref.shape[2] // LANES
    length = w_ref.shape[0]
    ones = same_head(1.0)
    share = same_head(1.0 / CHANNELS)
    masks = half_masks(BLOCK)
    shape = (HEADS * length, length)
    row = lax.broadcasted_iota(jnp.int32, shape, 0)
    later = row // (HEADS * BLOCK) * BLOCK + row % BLOCK
    strict = later > lax.broadcasted_iota(jnp.int32, shape, 1)
    for group in range(groups):
        at = lanes_at(side, group, groups)
        out = pl.ds(group * LANES, LANES)
        r, k, v, w = r_ref[:, at].astype(F32), k_ref[:, at].astype(F32), v_ref[:, at], w_ref[:, at]
        gate = g_ref[:, at].astype(F32)
        out_ref[2, :, out] = gate / (1.0 + jnp.exp(-gate))
        cumul = cumulate(w)
        before = cumul - w.astype(F32)
        out_ref[1, :, out] = r * jnp.exp(before)
        diagonal_high, diagonal_low = split(r * table_ref[0:1, at] * k)
        diagonal = dot(diagonal_high, ones) + dot(diagonal_low, ones)
        pieces = []
        for start in range(0, length, BLOCK):
            stop = start + BLOCK
            middle = start + BLOCK // 2 - 1
            reference = cumul[middle : middle + 1]
            r_high, r_low = split(r[start:stop] * jnp.exp(before[start:stop] - reference))
            k_high, k_low = split(k[:stop] * jnp.exp(reference - cumul[:stop]))
            if stop < length:
                rest = jnp.zeros((length - stop, LANES), BF16)
                k_high = jnp.concatenate([k_high, rest], axis=0)
                k_low = jnp.concatenate([k_low, rest], axis=0)
            r_high, r_low = spread_heads(r_high, masks), spread_heads(r_low, masks)
            pieces.append(dot_nt(r_high, k_high) + dot_nt(r_low, k_high) + dot_nt(r_high, k_low))
        s_high, s_low = split(jnp.where(strict, jnp.concatenate(pieces, axis=0), F32(0.0)))
        wide = dot(jnp.concatenate([s_high, s_low], axis=1), jnp.concatenate([v, v], axis=0))
        step = HEADS * BLOCK
        mixed = jnp.concatenate(
            [own_blocks(wide[i * step : (i + 1) * step], BLOCK) for i in range(length // BLOCK)],
            axis=0,
        )
        mixed = mixed + diagonal * v.astype(F32)
        m_high, m_low = split(mixed)
        out_ref[0, :, out] = mixed - (dot(m_high, share) + dot(m_low, share))


def finish_kernel(
    p0, p1, p2, p3, ends_mine, ends_other, in_mine, in_other, table_ref, out_ref,
    state_ref, buf, sems,
):
    core = lax.axis_index("head")
    place = lax.axis_index("seq") % PLANE
    groups = ends_mine.shape[0]
    length = in_mine.shape[1]
    first = core == 0
    share = same_head(1.0 / CHANNELS)
    masks = half_masks(CHANNELS)
    for step, piece in enumerate((p0, p1, p2, p3)):
        source = lax.bitwise_xor(place, step) * ROWS
        for group in range(groups):
            at = pl.multiple_of(source + group * CHANNELS, ROWS)
            state_ref[pl.ds(at, ROWS), :] = piece[group * ROWS : (group + 1) * ROWS, :]
    copies = []
    for group in range(groups):
        at = lanes_at(0, group, groups)
        out = pl.ds(group * LANES, LANES)
        early = jnp.where(first, ends_mine[group], ends_other[group])
        state = state_ref[group * CHANNELS : (group + 1) * CHANNELS, :]
        for half in range(2):
            local = core == half
            if half == 1:
                state = early[CHANNELS : CHANNELS + 1] * state + early[:CHANNELS]
            s_high, s_low = split(state - jnp.mean(state, axis=0, keepdims=True))
            s_high, s_low = spread_heads(s_high, masks), spread_heads(s_low, masks)
            r_high, r_low = split(jnp.where(local, in_mine[1, :, out], in_other[1, :, out]))
            mixed = jnp.where(local, in_mine[0, :, out], in_other[0, :, out])
            mixed = mixed + (
                dot_nt(r_high, s_high) + dot_nt(r_low, s_high) + dot_nt(r_high, s_low)
            )
            q_high, q_low = split(mixed * mixed)
            spread = dot(q_high, share) + dot(q_low, share)
            normed = mixed * lax.rsqrt(spread + 1e-5)
            gate = jnp.where(local, in_mine[2, :, out], in_other[2, :, out])
            gated = (normed * table_ref[1:2, at] + table_ref[2:3, at]) * gate
            buf[half * length : (half + 1) * length, out] = gated.astype(BF16)
        copies.append(
            pltpu.make_async_copy(buf.at[:, out], out_ref.at[:, out], sems.at[group])
        )
        copies[-1].start()
    for copy in copies:
        copy.wait()


def program(r, k, v, w, gate, bonus, gain, bias):
    length, width = r.shape
    cores, count = lax.axis_size("head"), lax.axis_size("seq")
    planes = count // PLANE
    assert cores == 2 and count == planes * PLANE
    assert planes > 1 and planes & (planes - 1) == 0
    half = width // cores
    groups = half // LANES
    swap = [(0, 1), (1, 0)]
    hbm = pl.BlockSpec(memory_space=pltpu.HBM)
    table = jnp.stack([bonus.reshape(width), gain, bias])

    def call(kernel, outs, **options):
        return pl.pallas_call(
            kernel,
            out_shape=outs,
            compiler_params=pltpu.CompilerParams(vmem_limit_bytes=VMEM_LIMIT),
            **options,
        )

    ends_shape = jax.ShapeDtypeStruct((groups, CHANNELS + 8, LANES), F32)
    packed = jax.ShapeDtypeStruct((groups * ROWS + -(-groups // 8) * 8, LANES), F32)
    piece = jax.ShapeDtypeStruct((groups * ROWS, LANES), F32)
    half_buffer = pltpu.VMEM((cores, length, half), BF16)
    mine, theirs = call(
        ends_kernel,
        [ends_shape] * 2,
        in_specs=[hbm] * 3,
        scratch_shapes=[half_buffer] * 3 + [pltpu.SemaphoreType.DMA((cores, 3))],
    )(*(pltpu.with_memory_space_constraint(x, pltpu.HBM) for x in (k, v, w)))
    other = lax.ppermute(theirs, "head", swap)

    def within(side):
        return call(
            functools.partial(within_kernel, side), jax.ShapeDtypeStruct((3, length, half), F32)
        )(r, k, v, w, gate, table)

    def to_places(pieces):
        return [pieces[0]] + [
            lax.ppermute(pieces[step], "seq", [(i, i ^ step) for i in range(count)])
            for step in range(1, PLANE)
        ]

    def mirror(value, bit):
        flip = (2 * bit - 1) * PLANE
        return lax.ppermute(value, "seq", [(i, i ^ flip) for i in range(count)])

    quarters = call(
        combine_kernel, [packed] * PLANE, scratch_shapes=[pltpu.VMEM((CHANNELS, LANES), F32)]
    )(mine, other)
    in_other = lax.ppermute(within(1), "head", swap)
    total, prefix = call(
        plane_kernel,
        [packed, jax.ShapeDtypeStruct((PLANE,) + packed.shape, F32)],
        scratch_shapes=[pltpu.VMEM((PLANE,) + packed.shape, F32)],
    )(*to_places(quarters))
    in_mine = within(0)
    before = total
    bit = 1
    while 2 * bit < planes:
        total, before = call(
            functools.partial(round_kernel, bit, bit == 1), [packed] * 2
        )(total, mirror(total, bit), before)
        bit *= 2
    states = call(functools.partial(back_kernel, bit), [piece] * PLANE)(
        prefix, before, mirror(total, bit)
    )
    return call(
        finish_kernel,
        jax.ShapeDtypeStruct((cores * length, half), BF16),
        out_specs=hbm,
        scratch_shapes=[
            pltpu.VMEM((groups * CHANNELS, LANES), F32),
            pltpu.VMEM((cores * length, half), BF16),
            pltpu.SemaphoreType.DMA((groups,)),
        ],
    )(*to_places(states), mine, other, in_mine, in_other, table)


def solution(mesh):
    tokens = P(("seq", "head"), None)
    return jax.shard_map(
        program,
        mesh=mesh,
        in_specs=(tokens,) * 5 + (P(), P(), P()),
        out_specs=P("seq", "head"),
        check_vma=False,
    )
```

```python
import functools

import jax
import jax.numpy as jnp
from jax import lax
from jax.experimental import pallas as pl
from jax.experimental.pallas import tpu as pltpu
from jax.sharding import PartitionSpec as P


CHANNELS = 64
TILE = 128
LANES = 256
HEADS = LANES // CHANNELS
BLOCK = 64
PLANE = 4
ROWS = CHANNELS // PLANE
STATE_STEP = 0.75 * 6.0
VMEM_LIMIT = 12 * 2**20
F32 = jnp.float32
BF16 = jnp.bfloat16


def split(value):
    high = value.astype(BF16)
    return high, (value - high.astype(F32)).astype(BF16)


def dot(left, right):
    return lax.dot_general(left, right, (((1,), (0,)), ((), ())), preferred_element_type=F32)


def dot_nt(left, right):
    return lax.dot_general(left, right, (((1,), (1,)), ((), ())), preferred_element_type=F32)


def same_head(value):
    rows = lax.broadcasted_iota(jnp.int32, (LANES, LANES), 0) // CHANNELS
    columns = lax.broadcasted_iota(jnp.int32, (LANES, LANES), 1) // CHANNELS
    return jnp.where(rows == columns, F32(value), F32(0.0)).astype(BF16)


def half_masks(rows):
    left = lax.broadcasted_iota(jnp.int32, (rows, TILE), 1) < CHANNELS
    one, zero = F32(1.0), F32(0.0)
    return jnp.where(left, one, zero).astype(BF16), jnp.where(left, zero, one).astype(BF16)


def spread_heads(value, masks):
    zero = jnp.zeros((value.shape[0], TILE), value.dtype)
    pieces = []
    for head in range(HEADS):
        tile = head // 2
        kept = value[:, tile * TILE : (tile + 1) * TILE] * masks[head % 2]
        pieces.append(
            jnp.concatenate([kept if i == tile else zero for i in range(LANES // TILE)], axis=1)
        )
    return jnp.concatenate(pieces, axis=0)


def own_blocks(stacked, rows):
    left = lax.broadcasted_iota(jnp.int32, (rows, TILE), 1) < CHANNELS
    pieces = []
    for tile in range(LANES // TILE):
        part = stacked[:, tile * TILE : (tile + 1) * TILE]
        head = 2 * tile
        pieces.append(
            jnp.where(
                left,
                part[head * rows : (head + 1) * rows],
                part[(head + 1) * rows : (head + 2) * rows],
            )
        )
    return jnp.concatenate(pieces, axis=1)


def cumulate(decay):
    length = decay.shape[0]
    rows = lax.broadcasted_iota(jnp.int32, (length, length), 0)
    columns = lax.broadcasted_iota(jnp.int32, (length, length), 1)
    lower = jnp.where(rows >= columns, F32(1.0), F32(0.0)).astype(BF16)
    return dot(lower, decay)


def lanes_at(side, group, groups):
    core = lax.axis_index("head")
    core = core if side == 0 else 1 - core
    return pl.ds(pl.multiple_of((core * groups + group) * LANES, LANES), LANES)


def half_at(side, half):
    core = lax.axis_index("head")
    core = core if side == 0 else 1 - core
    return pl.ds(pl.multiple_of(core * half, LANES), half)


def ends_of(key, value, decay):
    length = decay.shape[0]
    cumul = cumulate(decay)
    final = cumul[length - 1 : length]
    high, low = split(key.astype(F32) * jnp.exp(final - cumul))
    turned = value.astype(F32).T.astype(BF16)
    wide = dot(
        jnp.concatenate([turned, turned], axis=1), jnp.concatenate([high, low], axis=0)
    )
    return own_blocks(wide, CHANNELS), jnp.broadcast_to(final, (8, LANES))


def ends_kernel(side, k_ref, v_ref, w_ref, out_ref, k_buf, v_buf, w_buf, sems):
    groups = out_ref.shape[0]
    copies = []
    for index, (ref, buf) in enumerate(((w_ref, w_buf), (k_ref, k_buf), (v_ref, v_buf))):
        at = half_at(side, groups * LANES)
        copies.append(pltpu.make_async_copy(ref.at[:, at], buf, sems.at[index]))
        copies[-1].start()
    for copy in copies:
        copy.wait()
    for group in range(groups):
        at = pl.ds(group * LANES, LANES)
        state, decay = ends_of(k_buf[:, at], v_buf[:, at], w_buf[:, at])
        out_ref[group, :CHANNELS, :] = state
        out_ref[group, CHANNELS:, :] = decay


def log_rows(groups, group):
    at = groups * ROWS + group
    return slice(at, at + 1), slice(at + groups, at + groups + 1)


def put_log(ref, groups, group, value):
    high, low = log_rows(groups, group)
    rounded = value.astype(BF16).astype(F32)
    ref[high, :] = rounded
    ref[low, :] = value - rounded


def get_log(ref, groups, group):
    high, low = log_rows(groups, group)
    return ref[high, :] + ref[low, :]


def combine_kernel(scale, mine_ref, other_ref, q0, q1, q2, q3, state_ref):
    core = lax.axis_index("head")
    place = lax.axis_index("seq") % PLANE
    groups = mine_ref.shape[0]
    first = core == 0
    outs = (q0, q1, q2, q3)
    for out in outs:
        out[groups * ROWS :, :] = jnp.zeros((out.shape[0] - groups * ROWS, LANES), F32)
    for group in range(groups):
        mine, other = mine_ref[group], other_ref[group]
        early, late = jnp.where(first, mine, other), jnp.where(first, other, mine)
        late_log = late[CHANNELS : CHANNELS + 1]
        state = early[:CHANNELS] * jnp.exp(late_log) + late[:CHANNELS]
        state_ref[...] = state if scale == 1.0 else state * F32(scale)
        both = early[CHANNELS : CHANNELS + 1] + late_log
        for step, out in enumerate(outs):
            at = pl.multiple_of(lax.bitwise_xor(place, step) * ROWS, ROWS)
            out[group * ROWS : (group + 1) * ROWS, :] = state_ref[pl.ds(at, ROWS), :]
            put_log(out, groups, group, both)


def plane_kernel(groups, q0, q1, q2, q3, total_ref, prefix_ref, slab_ref):
    place = lax.axis_index("seq") % PLANE
    for step, piece in enumerate((q0, q1, q2, q3)):
        slab_ref[lax.bitwise_xor(place, step)] = piece[...]
    total_ref[groups * ROWS :, :] = jnp.zeros((total_ref.shape[0] - groups * ROWS, LANES), F32)
    for group in range(groups):
        rows = slice(group * ROWS, (group + 1) * ROWS)
        row, _ = log_rows(groups, group)
        state = jnp.zeros((ROWS, LANES), F32)
        log = jnp.zeros((1, LANES), F32)
        for slab in range(PLANE):
            prefix_ref[slab, rows, :] = state
            prefix_ref[slab, row, :] = jnp.exp(log)
            step = get_log(slab_ref.at[slab], groups, group)
            state = jnp.exp(step) * state + slab_ref[slab, rows, :]
            log = log + step
        total_ref[rows, :] = state
        put_log(total_ref, groups, group, log)


def round_kernel(groups, bit, first_round, total_ref, got_ref, before_ref, total_out, before_out):
    plane = lax.axis_index("seq") // PLANE
    upper = lax.bitwise_and(plane, bit) != 0
    total_out[groups * ROWS :, :] = jnp.zeros((total_out.shape[0] - groups * ROWS, LANES), F32)
    for group in range(groups):
        rows = slice(group * ROWS, (group + 1) * ROWS)
        row, _ = log_rows(groups, group)
        total, got = total_ref[rows, :], got_ref[rows, :]
        total_log, got_log = get_log(total_ref, groups, group), get_log(got_ref, groups, group)
        low, high = jnp.where(upper, got, total), jnp.where(upper, total, got)
        total_out[rows, :] = jnp.exp(jnp.where(upper, total_log, got_log)) * low + high
        put_log(total_out, groups, group, total_log + got_log)
        if first_round:
            before = jnp.where(upper, got, F32(0.0))
            before_decay = jnp.where(upper, jnp.exp(got_log), F32(1.0))
        else:
            decay = before_ref[row, :]
            before = before_ref[rows, :]
            before = jnp.where(upper, decay * got + before, before)
            before_decay = jnp.where(upper, jnp.exp(got_log) * decay, decay)
        before_out[rows, :] = before
        before_out[row, :] = before_decay


def back_kernel(bit, prefix_ref, before_ref, got_ref, p0, p1, p2, p3):
    seq = lax.axis_index("seq")
    place = seq % PLANE
    upper = lax.bitwise_and(seq // PLANE, bit) != 0
    groups = p0.shape[0] // ROWS
    for group in range(groups):
        rows = slice(group * ROWS, (group + 1) * ROWS)
        row, _ = log_rows(groups, group)
        before = before_ref[rows, :]
        before = jnp.where(upper, before_ref[row, :] * got_ref[rows, :] + before, before)
        for step, out in enumerate((p0, p1, p2, p3)):
            to = lax.bitwise_xor(place, step)
            out[rows, :] = prefix_ref[to, row, :] * before + prefix_ref[to, rows, :]


def within_kernel(side, r_ref, k_ref, v_ref, w_ref, g_ref, table_ref, out_ref):
    groups = out_ref.shape[2] // LANES
    length = w_ref.shape[0]
    ones = same_head(1.0)
    share = same_head(1.0 / CHANNELS)
    masks = half_masks(BLOCK)
    shape = (HEADS * length, length)
    row = lax.broadcasted_iota(jnp.int32, shape, 0)
    later = row // (HEADS * BLOCK) * BLOCK + row % BLOCK
    strict = later > lax.broadcasted_iota(jnp.int32, shape, 1)
    for group in range(groups):
        at = lanes_at(side, group, groups)
        out = pl.ds(group * LANES, LANES)
        r, k, v, w = r_ref[:, at].astype(F32), k_ref[:, at].astype(F32), v_ref[:, at], w_ref[:, at]
        gate = g_ref[:, at].astype(F32)
        out_ref[2, :, out] = gate / (1.0 + jnp.exp(-gate))
        cumul = cumulate(w)
        before = cumul - w.astype(F32)
        out_ref[1, :, out] = r * jnp.exp(before)
        diagonal_high, diagonal_low = split(r * table_ref[0:1, at] * k)
        diagonal = dot(diagonal_high, ones) + dot(diagonal_low, ones)
        pieces = []
        for start in range(0, length, BLOCK):
            stop = start + BLOCK
            middle = start + BLOCK // 2 - 1
            reference = cumul[middle : middle + 1]
            r_high, r_low = split(r[start:stop] * jnp.exp(before[start:stop] - reference))
            k_high, k_low = split(k[:stop] * jnp.exp(reference - cumul[:stop]))
            if stop < length:
                rest = jnp.zeros((length - stop, LANES), BF16)
                k_high = jnp.concatenate([k_high, rest], axis=0)
                k_low = jnp.concatenate([k_low, rest], axis=0)
            r_high, r_low = spread_heads(r_high, masks), spread_heads(r_low, masks)
            pieces.append(dot_nt(r_high, k_high) + dot_nt(r_low, k_high) + dot_nt(r_high, k_low))
        s_high, s_low = split(jnp.where(strict, jnp.concatenate(pieces, axis=0), F32(0.0)))
        wide = dot(jnp.concatenate([s_high, s_low], axis=1), jnp.concatenate([v, v], axis=0))
        step = HEADS * BLOCK
        mixed = jnp.concatenate(
            [own_blocks(wide[i * step : (i + 1) * step], BLOCK) for i in range(length // BLOCK)],
            axis=0,
        )
        mixed = mixed + diagonal * v.astype(F32)
        m_high, m_low = split(mixed)
        out_ref[0, :, out] = mixed - (dot(m_high, share) + dot(m_low, share))


def finish_kernel(
    scale, p0, p1, p2, p3, ends_mine, ends_other, in_mine, in_other, table_ref, out_ref,
    state_ref, buf, sems,
):
    core = lax.axis_index("head")
    place = lax.axis_index("seq") % PLANE
    groups = ends_mine.shape[0]
    length = in_mine.shape[1]
    first = core == 0
    share = same_head(1.0 / CHANNELS)
    masks = half_masks(CHANNELS)
    for step, piece in enumerate((p0, p1, p2, p3)):
        source = lax.bitwise_xor(place, step) * ROWS
        for group in range(groups):
            at = pl.multiple_of(source + group * CHANNELS, ROWS)
            state_ref[pl.ds(at, ROWS), :] = piece[group * ROWS : (group + 1) * ROWS, :] * F32(1.0 / scale)
    copies = []
    for group in range(groups):
        at = lanes_at(0, group, groups)
        out = pl.ds(group * LANES, LANES)
        early = jnp.where(first, ends_mine[group], ends_other[group])
        state = state_ref[group * CHANNELS : (group + 1) * CHANNELS, :]
        for half in range(2):
            local = core == half
            if half == 1:
                state = jnp.exp(early[CHANNELS : CHANNELS + 1]) * state + early[:CHANNELS]
            s_high, s_low = split(state - jnp.mean(state, axis=0, keepdims=True))
            s_high, s_low = spread_heads(s_high, masks), spread_heads(s_low, masks)
            r_high, r_low = split(jnp.where(local, in_mine[1, :, out], in_other[1, :, out]))
            mixed = jnp.where(local, in_mine[0, :, out], in_other[0, :, out])
            mixed = mixed + (
                dot_nt(r_high, s_high) + dot_nt(r_low, s_high) + dot_nt(r_high, s_low)
            )
            q_high, q_low = split(mixed * mixed)
            spread = dot(q_high, share) + dot(q_low, share)
            normed = mixed * lax.rsqrt(spread + 1e-5)
            gate = jnp.where(local, in_mine[2, :, out], in_other[2, :, out])
            gated = (normed * table_ref[1:2, at] + table_ref[2:3, at]) * gate
            buf[half * length : (half + 1) * length, out] = gated.astype(BF16)
        copies.append(
            pltpu.make_async_copy(buf.at[:, out], out_ref.at[:, out], sems.at[group])
        )
        copies[-1].start()
    for copy in copies:
        copy.wait()


def program(r, k, v, w, gate, bonus, gain, bias):
    length, width = r.shape
    cores, count = lax.axis_size("head"), lax.axis_size("seq")
    planes = count // PLANE
    assert cores == 2 and count == planes * PLANE
    assert planes > 1 and planes & (planes - 1) == 0
    half = width // cores
    groups = half // LANES
    swap = [(0, 1), (1, 0)]
    hbm = pl.BlockSpec(memory_space=pltpu.HBM)
    table = jnp.stack([bonus.reshape(width), gain, bias])

    def call(kernel, outs, **options):
        return pl.pallas_call(
            kernel,
            out_shape=outs,
            compiler_params=pltpu.CompilerParams(vmem_limit_bytes=VMEM_LIMIT),
            **options,
        )

    ends_shape = jax.ShapeDtypeStruct((groups, CHANNELS + 8, LANES), F32)
    packed_rows = -(-groups * (ROWS + 2) // 16) * 16
    packed = jax.ShapeDtypeStruct((packed_rows, LANES), F32)
    piece = jax.ShapeDtypeStruct((groups * ROWS, LANES), F32)
    scale = 1.0
    while STATE_STEP * length * cores * count * scale > 2.0**15:
        scale *= 0.5

    def ends(side):
        return call(
            functools.partial(ends_kernel, side),
            ends_shape,
            in_specs=[hbm] * 3,
            scratch_shapes=[pltpu.VMEM((length, half), BF16)] * 3
            + [pltpu.SemaphoreType.DMA((3,))],
        )(*(pltpu.with_memory_space_constraint(x, pltpu.HBM) for x in (k, v, w)))

    other = lax.ppermute(ends(1), "head", swap)
    mine = ends(0)

    def within(side):
        return call(
            functools.partial(within_kernel, side), jax.ShapeDtypeStruct((3, length, half), F32)
        )(r, k, v, w, gate, table)

    def over_seq(value, flip):
        pairs = [(i, i ^ flip) for i in range(count)]
        return lax.ppermute(value.astype(jnp.float16), "seq", pairs).astype(F32)

    def to_places(pieces):
        return [pieces[0]] + [over_seq(pieces[step], step) for step in range(1, PLANE)]

    def mirror(value, bit):
        return over_seq(value, (2 * bit - 1) * PLANE)

    quarters = call(
        functools.partial(combine_kernel, scale),
        [packed] * PLANE,
        scratch_shapes=[pltpu.VMEM((CHANNELS, LANES), F32)],
    )(mine, other)
    in_other = lax.ppermute(within(1), "head", swap)
    total, prefix = call(
        functools.partial(plane_kernel, groups),
        [packed, jax.ShapeDtypeStruct((PLANE,) + packed.shape, F32)],
        scratch_shapes=[pltpu.VMEM((PLANE,) + packed.shape, F32)],
    )(*to_places(quarters))
    in_mine = within(0)
    before = total
    bit = 1
    while 2 * bit < planes:
        total, before = call(
            functools.partial(round_kernel, groups, bit, bit == 1), [packed] * 2
        )(total, mirror(total, bit), before)
        bit *= 2
    states = call(functools.partial(back_kernel, bit), [piece] * PLANE)(
        prefix, before, mirror(total, bit)
    )
    return call(
        functools.partial(finish_kernel, scale),
        jax.ShapeDtypeStruct((cores * length, half), BF16),
        out_specs=hbm,
        scratch_shapes=[
            pltpu.VMEM((groups * CHANNELS, LANES), F32),
            pltpu.VMEM((cores * length, half), BF16),
            pltpu.SemaphoreType.DMA((groups,)),
        ],
    )(*to_places(states), mine, other, in_mine, in_other, table)


def solution(mesh):
    tokens = P(("seq", "head"), None)
    return jax.shard_map(
        program,
        mesh=mesh,
        in_specs=(tokens,) * 5 + (P(), P(), P()),
        out_specs=P("seq", "head"),
        check_vma=False,
    )
```

```python
import functools

import jax
import jax.numpy as jnp
from jax import lax
from jax.experimental import pallas as pl
from jax.experimental.pallas import tpu as pltpu
from jax.sharding import PartitionSpec as P


CHANNELS = 64
TILE = 128
LANES = 256
HEADS = LANES // CHANNELS
BLOCK = 64
PLANE = 4
ROWS = CHANNELS // PLANE
STATE_STEP = 0.75 * 6.0
VMEM_LIMIT = 12 * 2**20
F32 = jnp.float32
BF16 = jnp.bfloat16


def split(value):
    high = value.astype(BF16)
    return high, (value - high.astype(F32)).astype(BF16)


def dot(left, right):
    return lax.dot_general(left, right, (((1,), (0,)), ((), ())), preferred_element_type=F32)


def dot_nt(left, right):
    return lax.dot_general(left, right, (((1,), (1,)), ((), ())), preferred_element_type=F32)


def same_head(value):
    rows = lax.broadcasted_iota(jnp.int32, (LANES, LANES), 0) // CHANNELS
    columns = lax.broadcasted_iota(jnp.int32, (LANES, LANES), 1) // CHANNELS
    return jnp.where(rows == columns, F32(value), F32(0.0)).astype(BF16)


def half_masks(rows):
    left = lax.broadcasted_iota(jnp.int32, (rows, TILE), 1) < CHANNELS
    one, zero = F32(1.0), F32(0.0)
    return jnp.where(left, one, zero).astype(BF16), jnp.where(left, zero, one).astype(BF16)


def spread_heads(value, masks):
    zero = jnp.zeros((value.shape[0], TILE), value.dtype)
    pieces = []
    for head in range(HEADS):
        tile = head // 2
        kept = value[:, tile * TILE : (tile + 1) * TILE] * masks[head % 2]
        pieces.append(
            jnp.concatenate([kept if i == tile else zero for i in range(LANES // TILE)], axis=1)
        )
    return jnp.concatenate(pieces, axis=0)


def own_blocks(stacked, rows):
    left = lax.broadcasted_iota(jnp.int32, (rows, TILE), 1) < CHANNELS
    pieces = []
    for tile in range(LANES // TILE):
        part = stacked[:, tile * TILE : (tile + 1) * TILE]
        head = 2 * tile
        pieces.append(
            jnp.where(
                left,
                part[head * rows : (head + 1) * rows],
                part[(head + 1) * rows : (head + 2) * rows],
            )
        )
    return jnp.concatenate(pieces, axis=1)


def cumulate(decay):
    length = decay.shape[0]
    rows = lax.broadcasted_iota(jnp.int32, (length, length), 0)
    columns = lax.broadcasted_iota(jnp.int32, (length, length), 1)
    lower = jnp.where(rows >= columns, F32(1.0), F32(0.0)).astype(BF16)
    return dot(lower, decay)


def lanes_at(side, group, groups):
    core = lax.axis_index("head")
    core = core if side == 0 else 1 - core
    return pl.ds(pl.multiple_of((core * groups + group) * LANES, LANES), LANES)


def half_at(side, half):
    core = lax.axis_index("head")
    core = core if side == 0 else 1 - core
    return pl.ds(pl.multiple_of(core * half, LANES), half)


def ends_of(key, value, decay):
    length = decay.shape[0]
    cumul = cumulate(decay)
    final = cumul[length - 1 : length]
    high, low = split(key.astype(F32) * jnp.exp(final - cumul))
    turned = value.astype(F32).T.astype(BF16)
    wide = dot(
        jnp.concatenate([turned, turned], axis=1), jnp.concatenate([high, low], axis=0)
    )
    return own_blocks(wide, CHANNELS), jnp.broadcast_to(final, (8, LANES))


def ends_kernel(k_ref, v_ref, w_ref, mine_ref, theirs_ref, k_buf, v_buf, w_buf, sems):
    groups = mine_ref.shape[0]
    half = groups * LANES
    copies = {}
    for side in (1, 0):
        at = half_at(side, half)
        for index, (ref, buf) in enumerate(((w_ref, w_buf), (k_ref, k_buf), (v_ref, v_buf))):
            copies[side, index] = pltpu.make_async_copy(
                ref.at[:, at], buf.at[side], sems.at[side, index]
            )
            copies[side, index].start()
    for side, out_ref in ((1, theirs_ref), (0, mine_ref)):
        for index in range(3):
            copies[side, index].wait()
        for group in range(groups):
            at = pl.ds(group * LANES, LANES)
            state, decay = ends_of(k_buf[side, :, at], v_buf[side, :, at], w_buf[side, :, at])
            out_ref[group, :CHANNELS, :] = state
            out_ref[group, CHANNELS:, :] = decay


def log_rows(groups, group):
    at = groups * ROWS + group
    return slice(at, at + 1), slice(at + groups, at + groups + 1)


def put_log(ref, groups, group, value):
    high, low = log_rows(groups, group)
    rounded = value.astype(BF16).astype(F32)
    ref[high, :] = rounded
    ref[low, :] = value - rounded


def get_log(ref, groups, group):
    high, low = log_rows(groups, group)
    return ref[high, :] + ref[low, :]


def combine_kernel(scale, mine_ref, other_ref, q0, q1, q2, q3, state_ref):
    core = lax.axis_index("head")
    place = lax.axis_index("seq") % PLANE
    groups = mine_ref.shape[0]
    first = core == 0
    outs = (q0, q1, q2, q3)
    for out in outs:
        out[groups * ROWS :, :] = jnp.zeros((out.shape[0] - groups * ROWS, LANES), F32)
    for group in range(groups):
        mine, other = mine_ref[group], other_ref[group]
        early, late = jnp.where(first, mine, other), jnp.where(first, other, mine)
        late_log = late[CHANNELS : CHANNELS + 1]
        state = early[:CHANNELS] * jnp.exp(late_log) + late[:CHANNELS]
        state_ref[...] = state if scale == 1.0 else state * F32(scale)
        both = early[CHANNELS : CHANNELS + 1] + late_log
        for step, out in enumerate(outs):
            at = pl.multiple_of(lax.bitwise_xor(place, step) * ROWS, ROWS)
            out[group * ROWS : (group + 1) * ROWS, :] = state_ref[pl.ds(at, ROWS), :]
            put_log(out, groups, group, both)


def plane_kernel(groups, q0, q1, q2, q3, total_ref, prefix_ref, slab_ref):
    place = lax.axis_index("seq") % PLANE
    for step, piece in enumerate((q0, q1, q2, q3)):
        slab_ref[lax.bitwise_xor(place, step)] = piece[...]
    total_ref[groups * ROWS :, :] = jnp.zeros((total_ref.shape[0] - groups * ROWS, LANES), F32)
    for group in range(groups):
        rows = slice(group * ROWS, (group + 1) * ROWS)
        row, _ = log_rows(groups, group)
        state = jnp.zeros((ROWS, LANES), F32)
        log = jnp.zeros((1, LANES), F32)
        for slab in range(PLANE):
            prefix_ref[slab, rows, :] = state
            prefix_ref[slab, row, :] = jnp.exp(log)
            step = get_log(slab_ref.at[slab], groups, group)
            state = jnp.exp(step) * state + slab_ref[slab, rows, :]
            log = log + step
        total_ref[rows, :] = state
        put_log(total_ref, groups, group, log)


def round_kernel(groups, bit, first_round, total_ref, got_ref, before_ref, total_out, before_out):
    plane = lax.axis_index("seq") // PLANE
    upper = lax.bitwise_and(plane, bit) != 0
    total_out[groups * ROWS :, :] = jnp.zeros((total_out.shape[0] - groups * ROWS, LANES), F32)
    for group in range(groups):
        rows = slice(group * ROWS, (group + 1) * ROWS)
        row, _ = log_rows(groups, group)
        total, got = total_ref[rows, :], got_ref[rows, :]
        total_log, got_log = get_log(total_ref, groups, group), get_log(got_ref, groups, group)
        low, high = jnp.where(upper, got, total), jnp.where(upper, total, got)
        total_out[rows, :] = jnp.exp(jnp.where(upper, total_log, got_log)) * low + high
        put_log(total_out, groups, group, total_log + got_log)
        if first_round:
            before = jnp.where(upper, got, F32(0.0))
            before_decay = jnp.where(upper, jnp.exp(got_log), F32(1.0))
        else:
            decay = before_ref[row, :]
            before = before_ref[rows, :]
            before = jnp.where(upper, decay * got + before, before)
            before_decay = jnp.where(upper, jnp.exp(got_log) * decay, decay)
        before_out[rows, :] = before
        before_out[row, :] = before_decay


def back_kernel(bit, prefix_ref, before_ref, got_ref, p0, p1, p2, p3):
    seq = lax.axis_index("seq")
    place = seq % PLANE
    upper = lax.bitwise_and(seq // PLANE, bit) != 0
    groups = p0.shape[0] // ROWS
    for group in range(groups):
        rows = slice(group * ROWS, (group + 1) * ROWS)
        row, _ = log_rows(groups, group)
        before = before_ref[rows, :]
        before = jnp.where(upper, before_ref[row, :] * got_ref[rows, :] + before, before)
        for step, out in enumerate((p0, p1, p2, p3)):
            to = lax.bitwise_xor(place, step)
            out[rows, :] = prefix_ref[to, row, :] * before + prefix_ref[to, rows, :]


def within_kernel(side, r_ref, k_ref, v_ref, w_ref, g_ref, table_ref, out_ref):
    groups = out_ref.shape[2] // LANES
    length = w_ref.shape[0]
    ones = same_head(1.0)
    share = same_head(1.0 / CHANNELS)
    masks = half_masks(BLOCK)
    shape = (HEADS * length, length)
    row = lax.broadcasted_iota(jnp.int32, shape, 0)
    later = row // (HEADS * BLOCK) * BLOCK + row % BLOCK
    strict = later > lax.broadcasted_iota(jnp.int32, shape, 1)
    span = range(groups)
    at = [lanes_at(side, group, groups) for group in span]
    out = [pl.ds(group * LANES, LANES) for group in span]
    cumuls = [cumulate(w_ref[:, at[group]]) for group in span]
    for group in span:
        gate = g_ref[:, at[group]].astype(F32)
        out_ref[2, :, out[group]] = gate / (1.0 + jnp.exp(-gate))
    scores = []
    for group in span:
        r, k = r_ref[:, at[group]].astype(F32), k_ref[:, at[group]].astype(F32)
        cumul = cumuls[group]
        before = cumul - w_ref[:, at[group]].astype(F32)
        out_ref[1, :, out[group]] = r * jnp.exp(before)
        pieces = []
        for start in range(0, length, BLOCK):
            stop = start + BLOCK
            middle = start + BLOCK // 2 - 1
            reference = cumul[middle : middle + 1]
            r_high, r_low = split(r[start:stop] * jnp.exp(before[start:stop] - reference))
            k_high, k_low = split(k[:stop] * jnp.exp(reference - cumul[:stop]))
            if stop < length:
                rest = jnp.zeros((length - stop, LANES), BF16)
                k_high = jnp.concatenate([k_high, rest], axis=0)
                k_low = jnp.concatenate([k_low, rest], axis=0)
            r_high, r_low = spread_heads(r_high, masks), spread_heads(r_low, masks)
            pieces.append(dot_nt(r_high, k_high) + dot_nt(r_low, k_high) + dot_nt(r_high, k_low))
        scores.append(split(jnp.where(strict, jnp.concatenate(pieces, axis=0), F32(0.0))))
    mixes = []
    for group in span:
        v = v_ref[:, at[group]]
        wide = dot(jnp.concatenate(scores[group], axis=1), jnp.concatenate([v, v], axis=0))
        step = HEADS * BLOCK
        mixed = jnp.concatenate(
            [own_blocks(wide[i * step : (i + 1) * step], BLOCK) for i in range(length // BLOCK)],
            axis=0,
        )
        r, k = r_ref[:, at[group]].astype(F32), k_ref[:, at[group]].astype(F32)
        diagonal_high, diagonal_low = split(r * table_ref[0:1, at[group]] * k)
        diagonal = dot(diagonal_high, ones) + dot(diagonal_low, ones)
        mixes.append(mixed + diagonal * v.astype(F32))
    for group in span:
        m_high, m_low = split(mixes[group])
        out_ref[0, :, out[group]] = mixes[group] - (dot(m_high, share) + dot(m_low, share))


def finish_kernel(
    scale, p0, p1, p2, p3, ends_mine, ends_other, in_mine, in_other, table_ref, out_ref,
    state_ref, buf, sems,
):
    core = lax.axis_index("head")
    place = lax.axis_index("seq") % PLANE
    groups = ends_mine.shape[0]
    length = in_mine.shape[1]
    first = core == 0
    share = same_head(1.0 / CHANNELS)
    masks = half_masks(CHANNELS)
    for step, piece in enumerate((p0, p1, p2, p3)):
        source = lax.bitwise_xor(place, step) * ROWS
        for group in range(groups):
            at = pl.multiple_of(source + group * CHANNELS, ROWS)
            state_ref[pl.ds(at, ROWS), :] = piece[group * ROWS : (group + 1) * ROWS, :] * F32(1.0 / scale)
    states = {}
    for group in range(groups):
        early = jnp.where(first, ends_mine[group], ends_other[group])
        near = state_ref[group * CHANNELS : (group + 1) * CHANNELS, :]
        far = jnp.exp(early[CHANNELS : CHANNELS + 1]) * near + early[:CHANNELS]
        near = split(near - jnp.mean(near, axis=0, keepdims=True))
        far = split(far - jnp.mean(far, axis=0, keepdims=True))
        for side in range(2):
            pick = first if side == 0 else jnp.logical_not(first)
            states[side, group] = [
                spread_heads(jnp.where(pick, one, two), masks) for one, two in zip(near, far)
            ]
    copies = []
    for side, local in enumerate((in_mine, in_other)):
        mixes, spreads = {}, {}
        for group in range(groups):
            out = pl.ds(group * LANES, LANES)
            s_high, s_low = states[side, group]
            r_high, r_low = split(local[1, :, out])
            mixes[group] = local[0, :, out] + (
                dot_nt(r_high, s_high) + dot_nt(r_low, s_high) + dot_nt(r_high, s_low)
            )
        for group in range(groups):
            q_high, q_low = split(mixes[group] * mixes[group])
            spreads[group] = dot(q_high, share) + dot(q_low, share)
        for group in range(groups):
            at = lanes_at(0, group, groups)
            out = pl.ds(group * LANES, LANES)
            normed = mixes[group] * lax.rsqrt(spreads[group] + 1e-5)
            gated = (normed * table_ref[1:2, at] + table_ref[2:3, at]) * local[2, :, out]
            buf[side, :, out] = gated.astype(BF16)
        rows = pl.ds(pl.multiple_of((core if side == 0 else 1 - core) * length, length), length)
        copies.append(pltpu.make_async_copy(buf.at[side], out_ref.at[rows, :], sems.at[side]))
        copies[-1].start()
    for copy in copies:
        copy.wait()


def program(r, k, v, w, gate, bonus, gain, bias):
    length, width = r.shape
    cores, count = lax.axis_size("head"), lax.axis_size("seq")
    planes = count // PLANE
    assert cores == 2 and count == planes * PLANE
    assert planes > 1 and planes & (planes - 1) == 0
    half = width // cores
    groups = half // LANES
    swap = [(0, 1), (1, 0)]
    hbm = pl.BlockSpec(memory_space=pltpu.HBM)
    table = jnp.stack([bonus.reshape(width), gain, bias])

    def call(kernel, outs, **options):
        return pl.pallas_call(
            kernel,
            out_shape=outs,
            compiler_params=pltpu.CompilerParams(vmem_limit_bytes=VMEM_LIMIT),
            **options,
        )

    ends_shape = jax.ShapeDtypeStruct((groups, CHANNELS + 8, LANES), F32)
    packed_rows = -(-groups * (ROWS + 2) // 16) * 16
    packed = jax.ShapeDtypeStruct((packed_rows, LANES), F32)
    piece = jax.ShapeDtypeStruct((groups * ROWS, LANES), F32)
    scale = 1.0
    while STATE_STEP * length * cores * count * scale > 2.0**15:
        scale *= 0.5

    mine, theirs = call(
        ends_kernel,
        [ends_shape] * 2,
        in_specs=[hbm] * 3,
        scratch_shapes=[pltpu.VMEM((cores, length, half), BF16)] * 3
        + [pltpu.SemaphoreType.DMA((cores, 3))],
    )(*(pltpu.with_memory_space_constraint(x, pltpu.HBM) for x in (k, v, w)))
    other = lax.ppermute(theirs, "head", swap)

    def within(side):
        return call(
            functools.partial(within_kernel, side), jax.ShapeDtypeStruct((3, length, half), F32)
        )(r, k, v, w, gate, table)

    def over_seq(value, flip):
        pairs = [(i, i ^ flip) for i in range(count)]
        return lax.ppermute(value.astype(jnp.float16), "seq", pairs).astype(F32)

    def to_places(pieces):
        return [pieces[0]] + [over_seq(pieces[step], step) for step in range(1, PLANE)]

    def mirror(value, bit):
        return over_seq(value, (2 * bit - 1) * PLANE)

    quarters = call(
        functools.partial(combine_kernel, scale),
        [packed] * PLANE,
        scratch_shapes=[pltpu.VMEM((CHANNELS, LANES), F32)],
    )(mine, other)
    in_other = lax.ppermute(within(1), "head", swap)
    total, prefix = call(
        functools.partial(plane_kernel, groups),
        [packed, jax.ShapeDtypeStruct((PLANE,) + packed.shape, F32)],
        scratch_shapes=[pltpu.VMEM((PLANE,) + packed.shape, F32)],
    )(*to_places(quarters))
    in_mine = within(0)
    before = total
    bit = 1
    while 2 * bit < planes:
        total, before = call(
            functools.partial(round_kernel, groups, bit, bit == 1), [packed] * 2
        )(total, mirror(total, bit), before)
        bit *= 2
    states = call(functools.partial(back_kernel, bit), [piece] * PLANE)(
        prefix, before, mirror(total, bit)
    )
    return call(
        functools.partial(finish_kernel, scale),
        jax.ShapeDtypeStruct((cores * length, half), BF16),
        out_specs=hbm,
        scratch_shapes=[
            pltpu.VMEM((groups * CHANNELS, LANES), F32),
            pltpu.VMEM((cores, length, half), BF16),
            pltpu.SemaphoreType.DMA((cores,)),
        ],
    )(*to_places(states), mine, other, in_mine, in_other, table)


def solution(mesh):
    tokens = P(("seq", "head"), None)
    return jax.shard_map(
        program,
        mesh=mesh,
        in_specs=(tokens,) * 5 + (P(), P(), P()),
        out_specs=P("seq", "head"),
        check_vma=False,
    )
```

```python
import functools

import jax
import jax.numpy as jnp
from jax import lax
from jax.experimental import pallas as pl
from jax.experimental.pallas import tpu as pltpu
from jax.sharding import PartitionSpec as P


CHANNELS = 64
TILE = 128
LANES = 256
HEADS = LANES // CHANNELS
BLOCK = 64
PLANE = 4
ROWS = CHANNELS // PLANE
VMEM_LIMIT = 12 * 2**20
F32 = jnp.float32
BF16 = jnp.bfloat16


def split(value):
    high = value.astype(BF16)
    return high, (value - high.astype(F32)).astype(BF16)


def dot(left, right):
    return lax.dot_general(left, right, (((1,), (0,)), ((), ())), preferred_element_type=F32)


def dot_nt(left, right):
    return lax.dot_general(left, right, (((1,), (1,)), ((), ())), preferred_element_type=F32)


def same_head(value):
    rows = lax.broadcasted_iota(jnp.int32, (LANES, LANES), 0) // CHANNELS
    columns = lax.broadcasted_iota(jnp.int32, (LANES, LANES), 1) // CHANNELS
    return jnp.where(rows == columns, F32(value), F32(0.0)).astype(BF16)


def half_masks(rows):
    left = lax.broadcasted_iota(jnp.int32, (rows, TILE), 1) < CHANNELS
    one, zero = F32(1.0), F32(0.0)
    return jnp.where(left, one, zero).astype(BF16), jnp.where(left, zero, one).astype(BF16)


def spread_heads(value, masks):
    zero = jnp.zeros((value.shape[0], TILE), value.dtype)
    pieces = []
    for head in range(HEADS):
        tile = head // 2
        kept = value[:, tile * TILE : (tile + 1) * TILE] * masks[head % 2]
        pieces.append(
            jnp.concatenate([kept if i == tile else zero for i in range(LANES // TILE)], axis=1)
        )
    return jnp.concatenate(pieces, axis=0)


def own_blocks(stacked, rows):
    left = lax.broadcasted_iota(jnp.int32, (rows, TILE), 1) < CHANNELS
    pieces = []
    for tile in range(LANES // TILE):
        part = stacked[:, tile * TILE : (tile + 1) * TILE]
        head = 2 * tile
        pieces.append(
            jnp.where(
                left,
                part[head * rows : (head + 1) * rows],
                part[(head + 1) * rows : (head + 2) * rows],
            )
        )
    return jnp.concatenate(pieces, axis=1)


def cumulate(decay):
    length = decay.shape[0]
    rows = lax.broadcasted_iota(jnp.int32, (length, length), 0)
    columns = lax.broadcasted_iota(jnp.int32, (length, length), 1)
    lower = jnp.where(rows >= columns, F32(1.0), F32(0.0)).astype(BF16)
    return dot(lower, decay)


def lanes_at(side, group, groups):
    core = lax.axis_index("head")
    core = core if side == 0 else 1 - core
    return pl.ds(pl.multiple_of((core * groups + group) * LANES, LANES), LANES)


def bonus_row(ref, side, group, groups):
    core = lax.axis_index("head")
    core = core if side == 0 else 1 - core
    first = (core * groups + group) * HEADS
    return jnp.concatenate([ref[pl.ds(first + head, 1), :] for head in range(HEADS)], axis=1)


def tile_row(ref, group, groups):
    tiles = LANES // TILE
    first = (lax.axis_index("head") * groups + group) * tiles
    return jnp.concatenate([ref[pl.ds(first + tile, 1), :] for tile in range(tiles)], axis=1)


def half_at(side, half):
    core = lax.axis_index("head")
    core = core if side == 0 else 1 - core
    return pl.ds(pl.multiple_of(core * half, LANES), half)


def ends_of(key, value, decay):
    length = decay.shape[0]
    cumul = cumulate(decay)
    final = cumul[length - 1 : length]
    high, low = split(key.astype(F32) * jnp.exp(final - cumul))
    turned = value.astype(F32).T.astype(BF16)
    wide = dot(
        jnp.concatenate([turned, turned], axis=1), jnp.concatenate([high, low], axis=0)
    )
    return own_blocks(wide, CHANNELS), jnp.broadcast_to(final, (8, LANES))


def ends_kernel(k_ref, v_ref, w_ref, mine_ref, theirs_ref, k_buf, v_buf, w_buf, sems):
    groups = mine_ref.shape[0]
    half = groups * LANES
    copies = {}
    for side in (1, 0):
        at = half_at(side, half)
        for index, (ref, buf) in enumerate(((w_ref, w_buf), (k_ref, k_buf), (v_ref, v_buf))):
            copies[side, index] = pltpu.make_async_copy(
                ref.at[:, at], buf.at[:, pl.ds(side * half, half)], sems.at[side, index]
            )
            copies[side, index].start()
    for side, out_ref in ((1, theirs_ref), (0, mine_ref)):
        for index in range(3):
            copies[side, index].wait()
        for group in range(groups):
            at = pl.ds(side * half + group * LANES, LANES)
            state, decay = ends_of(k_buf[:, at], v_buf[:, at], w_buf[:, at])
            out_ref[group, :CHANNELS, :] = state
            out_ref[group, CHANNELS:, :] = decay


def log_row(groups, group):
    return slice(groups * ROWS + group, groups * ROWS + group + 1)


def combine_kernel(mine_ref, other_ref, q0, q1, q2, q3, state_ref):
    core = lax.axis_index("head")
    place = lax.axis_index("seq") % PLANE
    groups = mine_ref.shape[0]
    first = core == 0
    outs = (q0, q1, q2, q3)
    for out in outs:
        out[groups * ROWS :, :] = jnp.zeros((out.shape[0] - groups * ROWS, LANES), F32)
    for group in range(groups):
        mine, other = mine_ref[group], other_ref[group]
        early, late = jnp.where(first, mine, other), jnp.where(first, other, mine)
        late_log = late[CHANNELS : CHANNELS + 1]
        state_ref[...] = early[:CHANNELS] * jnp.exp(late_log) + late[:CHANNELS]
        both = early[CHANNELS : CHANNELS + 1] + late_log
        for step, out in enumerate(outs):
            at = pl.multiple_of(lax.bitwise_xor(place, step) * ROWS, ROWS)
            out[group * ROWS : (group + 1) * ROWS, :] = state_ref[pl.ds(at, ROWS), :]
            out[log_row(groups, group), :] = both


def plane_kernel(groups, q0, q1, q2, q3, total_ref, prefix_ref, slab_ref):
    place = lax.axis_index("seq") % PLANE
    for step, piece in enumerate((q0, q1, q2, q3)):
        slab_ref[lax.bitwise_xor(place, step)] = piece[...]
    total_ref[groups * ROWS :, :] = jnp.zeros((total_ref.shape[0] - groups * ROWS, LANES), F32)
    for group in range(groups):
        rows = slice(group * ROWS, (group + 1) * ROWS)
        row = log_row(groups, group)
        state = jnp.zeros((ROWS, LANES), F32)
        log = jnp.zeros((1, LANES), F32)
        for slab in range(PLANE):
            prefix_ref[slab, rows, :] = state
            prefix_ref[slab, row, :] = jnp.exp(log)
            step = slab_ref[slab, row, :]
            state = jnp.exp(step) * state + slab_ref[slab, rows, :]
            log = log + step
        total_ref[rows, :] = state
        total_ref[row, :] = log


def round_kernel(groups, bit, first_round, total_ref, got_ref, before_ref, total_out, before_out):
    plane = lax.axis_index("seq") // PLANE
    upper = lax.bitwise_and(plane, bit) != 0
    total_out[groups * ROWS :, :] = jnp.zeros((total_out.shape[0] - groups * ROWS, LANES), F32)
    for group in range(groups):
        rows = slice(group * ROWS, (group + 1) * ROWS)
        row = log_row(groups, group)
        total, got = total_ref[rows, :], got_ref[rows, :]
        total_log, got_log = total_ref[row, :], got_ref[row, :]
        low, high = jnp.where(upper, got, total), jnp.where(upper, total, got)
        total_out[rows, :] = jnp.exp(jnp.where(upper, total_log, got_log)) * low + high
        total_out[row, :] = total_log + got_log
        if first_round:
            before = jnp.where(upper, got, F32(0.0))
            before_decay = jnp.where(upper, jnp.exp(got_log), F32(1.0))
        else:
            decay = before_ref[row, :]
            before = before_ref[rows, :]
            before = jnp.where(upper, decay * got + before, before)
            before_decay = jnp.where(upper, jnp.exp(got_log) * decay, decay)
        before_out[rows, :] = before
        before_out[row, :] = before_decay


def back_kernel(bit, prefix_ref, before_ref, got_ref, p0, p1, p2, p3):
    seq = lax.axis_index("seq")
    place = seq % PLANE
    upper = lax.bitwise_and(seq // PLANE, bit) != 0
    groups = p0.shape[0] // ROWS
    for group in range(groups):
        rows = slice(group * ROWS, (group + 1) * ROWS)
        row = log_row(groups, group)
        before = before_ref[rows, :]
        before = jnp.where(upper, before_ref[row, :] * got_ref[rows, :] + before, before)
        for step, out in enumerate((p0, p1, p2, p3)):
            to = lax.bitwise_xor(place, step)
            out[rows, :] = prefix_ref[to, row, :] * before + prefix_ref[to, rows, :]


def within_kernel(side, r_ref, k_ref, v_ref, w_ref, g_ref, bonus_ref, out_ref):
    groups = out_ref.shape[2] // LANES
    length = w_ref.shape[0]
    ones = same_head(1.0)
    share = same_head(1.0 / CHANNELS)
    masks = half_masks(BLOCK)
    shape = (HEADS * length, length)
    row = lax.broadcasted_iota(jnp.int32, shape, 0)
    later = row // (HEADS * BLOCK) * BLOCK + row % BLOCK
    strict = later > lax.broadcasted_iota(jnp.int32, shape, 1)
    span = range(groups)
    at = [lanes_at(side, group, groups) for group in span]
    out = [pl.ds(group * LANES, LANES) for group in span]
    held = [pl.ds((side * groups + group) * LANES, LANES) for group in span]
    cumuls = [cumulate(w_ref[:, held[group]]) for group in span]
    for group in span:
        gate = g_ref[:, at[group]].astype(F32)
        out_ref[2, :, out[group]] = gate / (1.0 + jnp.exp(-gate))
    scores = []
    for group in span:
        r, k = r_ref[:, at[group]].astype(F32), k_ref[:, held[group]].astype(F32)
        cumul = cumuls[group]
        before = cumul - w_ref[:, held[group]].astype(F32)
        out_ref[1, :, out[group]] = r * jnp.exp(before)
        pieces = []
        for start in range(0, length, BLOCK):
            stop = start + BLOCK
            middle = start + BLOCK // 2 - 1
            reference = cumul[middle : middle + 1]
            r_high, r_low = split(r[start:stop] * jnp.exp(before[start:stop] - reference))
            k_high, k_low = split(k[:stop] * jnp.exp(reference - cumul[:stop]))
            if stop < length:
                rest = jnp.zeros((length - stop, LANES), BF16)
                k_high = jnp.concatenate([k_high, rest], axis=0)
                k_low = jnp.concatenate([k_low, rest], axis=0)
            r_high, r_low = spread_heads(r_high, masks), spread_heads(r_low, masks)
            pieces.append(dot_nt(r_high, k_high) + dot_nt(r_low, k_high) + dot_nt(r_high, k_low))
        scores.append(split(jnp.where(strict, jnp.concatenate(pieces, axis=0), F32(0.0))))
    mixes = []
    for group in span:
        v = v_ref[:, held[group]]
        wide = dot(jnp.concatenate(scores[group], axis=1), jnp.concatenate([v, v], axis=0))
        step = HEADS * BLOCK
        mixed = jnp.concatenate(
            [own_blocks(wide[i * step : (i + 1) * step], BLOCK) for i in range(length // BLOCK)],
            axis=0,
        )
        r, k = r_ref[:, at[group]].astype(F32), k_ref[:, held[group]].astype(F32)
        diagonal_high, diagonal_low = split(r * bonus_row(bonus_ref, side, group, groups) * k)
        diagonal = dot(diagonal_high, ones) + dot(diagonal_low, ones)
        mixes.append(mixed + diagonal * v.astype(F32))
    for group in span:
        m_high, m_low = split(mixes[group])
        out_ref[0, :, out[group]] = mixes[group] - (dot(m_high, share) + dot(m_low, share))


def finish_kernel(
    p0, p1, p2, p3, ends_mine, ends_other, in_mine, in_other, gain_ref, bias_ref, out_ref,
    state_ref, buf, sems,
):
    core = lax.axis_index("head")
    place = lax.axis_index("seq") % PLANE
    groups = ends_mine.shape[0]
    length = in_mine.shape[1]
    first = core == 0
    share = same_head(1.0 / CHANNELS)
    masks = half_masks(CHANNELS)
    for step, piece in enumerate((p0, p1, p2, p3)):
        source = lax.bitwise_xor(place, step) * ROWS
        for group in range(groups):
            at = pl.multiple_of(source + group * CHANNELS, ROWS)
            state_ref[pl.ds(at, ROWS), :] = piece[group * ROWS : (group + 1) * ROWS, :]
    states = {}
    for group in range(groups):
        early = jnp.where(first, ends_mine[group], ends_other[group])
        near = state_ref[group * CHANNELS : (group + 1) * CHANNELS, :]
        far = jnp.exp(early[CHANNELS : CHANNELS + 1]) * near + early[:CHANNELS]
        near = split(near - jnp.mean(near, axis=0, keepdims=True))
        far = split(far - jnp.mean(far, axis=0, keepdims=True))
        for side in range(2):
            pick = first if side == 0 else jnp.logical_not(first)
            states[side, group] = [
                spread_heads(jnp.where(pick, one, two), masks) for one, two in zip(near, far)
            ]
    copies = []
    for side, local in enumerate((in_mine, in_other)):
        mixes, spreads = {}, {}
        for group in range(groups):
            out = pl.ds(group * LANES, LANES)
            s_high, s_low = states[side, group]
            r_high, r_low = split(local[1, :, out])
            mixes[group] = local[0, :, out] + (
                dot_nt(r_high, s_high) + dot_nt(r_low, s_high) + dot_nt(r_high, s_low)
            )
        for group in range(groups):
            q_high, q_low = split(mixes[group] * mixes[group])
            spreads[group] = dot(q_high, share) + dot(q_low, share)
        for group in range(groups):
            gain, bias = tile_row(gain_ref, group, groups), tile_row(bias_ref, group, groups)
            out = pl.ds(group * LANES, LANES)
            normed = mixes[group] * lax.rsqrt(spreads[group] + 1e-5)
            gated = (normed * gain + bias) * local[2, :, out]
            buf[side, :, out] = gated.astype(BF16)
        rows = pl.ds(pl.multiple_of((core if side == 0 else 1 - core) * length, length), length)
        copies.append(pltpu.make_async_copy(buf.at[side], out_ref.at[rows, :], sems.at[side]))
        copies[-1].start()
    for copy in copies:
        copy.wait()


def program(r, k, v, w, gate, bonus, gain, bias):
    length, width = r.shape
    cores, count = lax.axis_size("head"), lax.axis_size("seq")
    planes = count // PLANE
    assert cores == 2 and count == planes * PLANE
    assert planes > 1 and planes & (planes - 1) == 0
    half = width // cores
    groups = half // LANES
    swap = [(0, 1), (1, 0)]
    hbm = pl.BlockSpec(memory_space=pltpu.HBM)
    gain, bias = gain.reshape(-1, TILE), bias.reshape(-1, TILE)

    def call(kernel, outs, **options):
        return pl.pallas_call(
            kernel,
            out_shape=outs,
            compiler_params=pltpu.CompilerParams(vmem_limit_bytes=VMEM_LIMIT),
            **options,
        )

    ends_shape = jax.ShapeDtypeStruct((groups, CHANNELS + 8, LANES), F32)
    packed_rows = -(-groups * (ROWS + 1) // 8) * 8
    packed = jax.ShapeDtypeStruct((packed_rows, LANES), F32)
    piece = jax.ShapeDtypeStruct((groups * ROWS, LANES), F32)

    held = pltpu.VMEM((length, width), BF16)
    mine, theirs, k, v, w = call(
        ends_kernel,
        [pltpu.VMEM(ends_shape.shape, F32)] * 2 + [held] * 3,
        in_specs=[hbm] * 3,
        scratch_shapes=[pltpu.SemaphoreType.DMA((cores, 3))],
    )(*(pltpu.with_memory_space_constraint(x, pltpu.HBM) for x in (k, v, w)))
    other = lax.ppermute(theirs, "head", swap)

    def within(side):
        return call(
            functools.partial(within_kernel, side), jax.ShapeDtypeStruct((3, length, half), F32)
        )(r, k, v, w, gate, bonus)

    def over_seq(value, flip):
        pairs = [(i, i ^ flip) for i in range(count)]
        return lax.ppermute(value, "seq", pairs)

    def to_places(pieces):
        return [pieces[0]] + [over_seq(pieces[step], step) for step in range(1, PLANE)]

    def mirror(value, bit):
        return over_seq(value, (2 * bit - 1) * PLANE)

    quarters = call(
        combine_kernel, [packed] * PLANE, scratch_shapes=[pltpu.VMEM((CHANNELS, LANES), F32)]
    )(mine, other)
    in_other = lax.ppermute(within(1), "head", swap)
    total, prefix = call(
        functools.partial(plane_kernel, groups),
        [packed, jax.ShapeDtypeStruct((PLANE,) + packed.shape, F32)],
        scratch_shapes=[pltpu.VMEM((PLANE,) + packed.shape, F32)],
    )(*to_places(quarters))
    in_mine = within(0)
    before = total
    bit = 1
    while 2 * bit < planes:
        total, before = call(
            functools.partial(round_kernel, groups, bit, bit == 1), [packed] * 2
        )(total, mirror(total, bit), before)
        bit *= 2
    states = call(functools.partial(back_kernel, bit), [piece] * PLANE)(
        prefix, before, mirror(total, bit)
    )
    return call(
        finish_kernel,
        jax.ShapeDtypeStruct((cores * length, half), BF16),
        out_specs=hbm,
        scratch_shapes=[
            pltpu.VMEM((groups * CHANNELS, LANES), F32),
            pltpu.VMEM((cores, length, half), BF16),
            pltpu.SemaphoreType.DMA((cores,)),
        ],
    )(*to_places(states), mine, other, in_mine, in_other, gain, bias)


def solution(mesh):
    tokens = P(("seq", "head"), None)
    return jax.shard_map(
        program,
        mesh=mesh,
        in_specs=(tokens,) * 5 + (P(), P(), P()),
        out_specs=P("seq", "head"),
        check_vma=False,
    )
```

```python
import functools

import jax
import jax.numpy as jnp
from jax import lax
from jax.experimental import pallas as pl
from jax.experimental.pallas import tpu as pltpu
from jax.sharding import PartitionSpec as P


CHANNELS = 64
TILE = 128
LANES = 256
HEADS = LANES // CHANNELS
BLOCK = 64
PLANE = 4
ROWS = CHANNELS // PLANE
STATE_STEP = 0.75 * 6.0
SCALE_FLOOR = 2.0**-10
CODE_SPAN = 29.5
CODE_LOW = 14.0
VMEM_LIMIT = 12 * 2**20
F32 = jnp.float32
BF16 = jnp.bfloat16


def split(value):
    high = value.astype(BF16)
    return high, (value - high.astype(F32)).astype(BF16)


def dot(left, right):
    return lax.dot_general(left, right, (((1,), (0,)), ((), ())), preferred_element_type=F32)


def dot_nt(left, right):
    return lax.dot_general(left, right, (((1,), (1,)), ((), ())), preferred_element_type=F32)


def same_head(value):
    rows = lax.broadcasted_iota(jnp.int32, (LANES, LANES), 0) // CHANNELS
    columns = lax.broadcasted_iota(jnp.int32, (LANES, LANES), 1) // CHANNELS
    return jnp.where(rows == columns, F32(value), F32(0.0)).astype(BF16)


def half_masks(rows):
    left = lax.broadcasted_iota(jnp.int32, (rows, TILE), 1) < CHANNELS
    one, zero = F32(1.0), F32(0.0)
    return jnp.where(left, one, zero).astype(BF16), jnp.where(left, zero, one).astype(BF16)


def spread_heads(value, masks):
    zero = jnp.zeros((value.shape[0], TILE), value.dtype)
    pieces = []
    for head in range(HEADS):
        tile = head // 2
        kept = value[:, tile * TILE : (tile + 1) * TILE] * masks[head % 2]
        pieces.append(
            jnp.concatenate([kept if i == tile else zero for i in range(LANES // TILE)], axis=1)
        )
    return jnp.concatenate(pieces, axis=0)


def own_blocks(stacked, rows):
    left = lax.broadcasted_iota(jnp.int32, (rows, TILE), 1) < CHANNELS
    pieces = []
    for tile in range(LANES // TILE):
        part = stacked[:, tile * TILE : (tile + 1) * TILE]
        head = 2 * tile
        pieces.append(
            jnp.where(
                left,
                part[head * rows : (head + 1) * rows],
                part[(head + 1) * rows : (head + 2) * rows],
            )
        )
    return jnp.concatenate(pieces, axis=1)


def cumulate(decay):
    length = decay.shape[0]
    rows = lax.broadcasted_iota(jnp.int32, (length, length), 0)
    columns = lax.broadcasted_iota(jnp.int32, (length, length), 1)
    lower = jnp.where(rows >= columns, F32(1.0), F32(0.0)).astype(BF16)
    return dot(lower, decay)


def lanes_at(side, group, groups):
    core = lax.axis_index("head")
    core = core if side == 0 else 1 - core
    return pl.ds(pl.multiple_of((core * groups + group) * LANES, LANES), LANES)


def bonus_row(ref, side, group, groups):
    core = lax.axis_index("head")
    core = core if side == 0 else 1 - core
    first = (core * groups + group) * HEADS
    return jnp.concatenate([ref[pl.ds(first + head, 1), :] for head in range(HEADS)], axis=1)


def tile_row(ref, group, groups):
    tiles = LANES // TILE
    first = (lax.axis_index("head") * groups + group) * tiles
    return jnp.concatenate([ref[pl.ds(first + tile, 1), :] for tile in range(tiles)], axis=1)


def half_at(side, half):
    core = lax.axis_index("head")
    core = core if side == 0 else 1 - core
    return pl.ds(pl.multiple_of(core * half, LANES), half)


def ends_of(key, value, decay):
    length = decay.shape[0]
    cumul = cumulate(decay)
    final = cumul[length - 1 : length]
    high, low = split(key.astype(F32) * jnp.exp(final - cumul))
    turned = value.astype(F32).T.astype(BF16)
    wide = dot(
        jnp.concatenate([turned, turned], axis=1), jnp.concatenate([high, low], axis=0)
    )
    return own_blocks(wide, CHANNELS), jnp.broadcast_to(final, (8, LANES))


def ends_kernel(k_ref, v_ref, w_ref, mine_ref, theirs_ref, k_buf, v_buf, w_buf, sems):
    groups = mine_ref.shape[0]
    half = groups * LANES
    copies = {}
    for side in (1, 0):
        at = half_at(side, half)
        for index, (ref, buf) in enumerate(((w_ref, w_buf), (k_ref, k_buf), (v_ref, v_buf))):
            copies[side, index] = pltpu.make_async_copy(
                ref.at[:, at], buf.at[:, pl.ds(side * half, half)], sems.at[side, index]
            )
            copies[side, index].start()
    for side, out_ref in ((1, theirs_ref), (0, mine_ref)):
        for index in range(3):
            copies[side, index].wait()
        for group in range(groups):
            at = pl.ds(side * half + group * LANES, LANES)
            state, decay = ends_of(k_buf[:, at], v_buf[:, at], w_buf[:, at])
            out_ref[group, :CHANNELS, :] = state
            out_ref[group, CHANNELS:, :] = decay


def log_row(groups, group):
    return slice(groups * ROWS + group, groups * ROWS + group + 1)


def wire_rows(groups):
    return -(-groups * (ROWS + 3) // 16) * 16


def put_wire(ref, shrink, group, state, log=None):
    groups = ref.shape[0] // (ROWS + 3)
    top = jnp.max(jnp.abs(state), axis=0, keepdims=True)
    scale = (top * 1.01 + SCALE_FLOOR).astype(BF16).astype(F32)
    code = jnp.exp2(jnp.abs(state) * (CODE_SPAN / scale) - CODE_LOW)
    ref[group * ROWS : (group + 1) * ROWS, :] = jnp.where(state < 0.0, -code, code)
    row = groups * ROWS + group
    ref[row : row + 1, :] = scale * F32(shrink)
    high = jnp.zeros((1, LANES), F32) if log is None else log.astype(BF16).astype(F32)
    ref[row + groups : row + groups + 1, :] = high
    low = high if log is None else log - high
    ref[row + 2 * groups : row + 2 * groups + 1, :] = low


def clear_rest(ref):
    groups = ref.shape[0] // (ROWS + 3)
    rest = ref.shape[0] - groups * (ROWS + 3)
    if rest:
        ref[groups * (ROWS + 3) :, :] = jnp.zeros((rest, LANES), F32)


def get_wire(ref, shrink, group):
    groups = ref.shape[0] // (ROWS + 3)
    row = groups * ROWS + group
    scale = ref[row : row + 1, :] * F32(1.0 / (shrink * CODE_SPAN))
    code = ref[group * ROWS : (group + 1) * ROWS, :]
    size = (jnp.log2(jnp.abs(code)) + CODE_LOW) * scale
    log = ref[row + groups : row + groups + 1, :] + ref[row + 2 * groups : row + 2 * groups + 1, :]
    return jnp.where(code < 0.0, -size, size), log


def combine_kernel(shrink, mine_ref, other_ref, q0, q1, q2, q3, state_ref):
    core = lax.axis_index("head")
    place = lax.axis_index("seq") % PLANE
    groups = mine_ref.shape[0]
    first = core == 0
    for out in (q1, q2, q3):
        clear_rest(out)
    for group in range(groups):
        mine, other = mine_ref[group], other_ref[group]
        early, late = jnp.where(first, mine, other), jnp.where(first, other, mine)
        late_log = late[CHANNELS : CHANNELS + 1]
        state_ref[group] = early[:CHANNELS] * jnp.exp(late_log) + late[:CHANNELS]
        both = early[CHANNELS : CHANNELS + 1] + late_log
        for step, out in enumerate((q0, q1, q2, q3)):
            at = pl.multiple_of(lax.bitwise_xor(place, step) * ROWS, ROWS)
            state = state_ref[group, pl.ds(at, ROWS), :]
            if step:
                put_wire(out, shrink, group, state, both)
            else:
                out[group * ROWS : (group + 1) * ROWS, :] = state
                out[log_row(groups, group), :] = both


def plane_kernel(groups, shrink, q0, q1, q2, q3, total_ref, wire_ref, prefix_ref, slab_ref):
    place = lax.axis_index("seq") % PLANE
    clear_rest(wire_ref)
    for group in range(groups):
        rows = slice(group * ROWS, (group + 1) * ROWS)
        row = log_row(groups, group)
        slab_ref[place, rows, :] = q0[rows, :]
        slab_ref[place, row, :] = q0[row, :]
        for step, piece in ((1, q1), (2, q2), (3, q3)):
            to = lax.bitwise_xor(place, step)
            state, log = get_wire(piece, shrink, group)
            slab_ref[to, rows, :] = state
            slab_ref[to, row, :] = log
    for group in range(groups):
        rows = slice(group * ROWS, (group + 1) * ROWS)
        row = log_row(groups, group)
        state = jnp.zeros((ROWS, LANES), F32)
        log = jnp.zeros((1, LANES), F32)
        for slab in range(PLANE):
            prefix_ref[slab, rows, :] = state
            prefix_ref[slab, row, :] = jnp.exp(log)
            step = slab_ref[slab, row, :]
            state = jnp.exp(step) * state + slab_ref[slab, rows, :]
            log = log + step
        total_ref[rows, :] = state
        total_ref[row, :] = log
        put_wire(wire_ref, shrink, group, state, log)


def round_kernel(
    groups, shrink, bit, first_round, total_ref, got_ref, before_ref, total_out, wire_out, before_out
):
    plane = lax.axis_index("seq") // PLANE
    upper = lax.bitwise_and(plane, bit) != 0
    clear_rest(wire_out)
    for group in range(groups):
        rows = slice(group * ROWS, (group + 1) * ROWS)
        row = log_row(groups, group)
        total, total_log = total_ref[rows, :], total_ref[row, :]
        got, got_log = get_wire(got_ref, shrink, group)
        low, high = jnp.where(upper, got, total), jnp.where(upper, total, got)
        both = jnp.exp(jnp.where(upper, total_log, got_log)) * low + high
        total_out[rows, :] = both
        total_out[row, :] = total_log + got_log
        put_wire(wire_out, shrink, group, both, total_log + got_log)
        if first_round:
            before = jnp.where(upper, got, F32(0.0))
            before_decay = jnp.where(upper, jnp.exp(got_log), F32(1.0))
        else:
            decay = before_ref[row, :]
            before = before_ref[rows, :]
            before = jnp.where(upper, decay * got + before, before)
            before_decay = jnp.where(upper, jnp.exp(got_log) * decay, decay)
        before_out[rows, :] = before
        before_out[row, :] = before_decay


def back_kernel(groups, shrink, bit, prefix_ref, before_ref, got_ref, p0, p1, p2, p3):
    seq = lax.axis_index("seq")
    place = seq % PLANE
    upper = lax.bitwise_and(seq // PLANE, bit) != 0
    for out in (p1, p2, p3):
        clear_rest(out)
    for group in range(groups):
        rows = slice(group * ROWS, (group + 1) * ROWS)
        row = log_row(groups, group)
        before = before_ref[rows, :]
        got, _ = get_wire(got_ref, shrink, group)
        before = jnp.where(upper, before_ref[row, :] * got + before, before)
        for step, out in enumerate((p0, p1, p2, p3)):
            to = lax.bitwise_xor(place, step)
            state = prefix_ref[to, row, :] * before + prefix_ref[to, rows, :]
            if step:
                put_wire(out, shrink, group, state)
            else:
                out[rows, :] = state


def within_kernel(side, r_ref, k_ref, v_ref, w_ref, g_ref, bonus_ref, out_ref):
    groups = out_ref.shape[2] // LANES
    length = w_ref.shape[0]
    ones = same_head(1.0)
    share = same_head(1.0 / CHANNELS)
    masks = half_masks(BLOCK)
    shape = (HEADS * length, length)
    row = lax.broadcasted_iota(jnp.int32, shape, 0)
    later = row // (HEADS * BLOCK) * BLOCK + row % BLOCK
    strict = later > lax.broadcasted_iota(jnp.int32, shape, 1)
    span = range(groups)
    at = [lanes_at(side, group, groups) for group in span]
    out = [pl.ds(group * LANES, LANES) for group in span]
    held = [pl.ds((side * groups + group) * LANES, LANES) for group in span]
    cumuls = [cumulate(w_ref[:, held[group]]) for group in span]
    for group in span:
        gate = g_ref[:, at[group]].astype(F32)
        out_ref[2, :, out[group]] = gate / (1.0 + jnp.exp(-gate))
    scores = []
    for group in span:
        r, k = r_ref[:, at[group]].astype(F32), k_ref[:, held[group]].astype(F32)
        cumul = cumuls[group]
        before = cumul - w_ref[:, held[group]].astype(F32)
        out_ref[1, :, out[group]] = r * jnp.exp(before)
        pieces = []
        for start in range(0, length, BLOCK):
            stop = start + BLOCK
            middle = start + BLOCK // 2 - 1
            reference = cumul[middle : middle + 1]
            r_high, r_low = split(r[start:stop] * jnp.exp(before[start:stop] - reference))
            k_high, k_low = split(k[:stop] * jnp.exp(reference - cumul[:stop]))
            if stop < length:
                rest = jnp.zeros((length - stop, LANES), BF16)
                k_high = jnp.concatenate([k_high, rest], axis=0)
                k_low = jnp.concatenate([k_low, rest], axis=0)
            r_high, r_low = spread_heads(r_high, masks), spread_heads(r_low, masks)
            pieces.append(dot_nt(r_high, k_high) + dot_nt(r_low, k_high) + dot_nt(r_high, k_low))
        scores.append(split(jnp.where(strict, jnp.concatenate(pieces, axis=0), F32(0.0))))
    mixes = []
    for group in span:
        v = v_ref[:, held[group]]
        wide = dot(jnp.concatenate(scores[group], axis=1), jnp.concatenate([v, v], axis=0))
        step = HEADS * BLOCK
        mixed = jnp.concatenate(
            [own_blocks(wide[i * step : (i + 1) * step], BLOCK) for i in range(length // BLOCK)],
            axis=0,
        )
        r, k = r_ref[:, at[group]].astype(F32), k_ref[:, held[group]].astype(F32)
        diagonal_high, diagonal_low = split(r * bonus_row(bonus_ref, side, group, groups) * k)
        diagonal = dot(diagonal_high, ones) + dot(diagonal_low, ones)
        mixes.append(mixed + diagonal * v.astype(F32))
    for group in span:
        m_high, m_low = split(mixes[group])
        out_ref[0, :, out[group]] = mixes[group] - (dot(m_high, share) + dot(m_low, share))


def finish_kernel(
    shrink, p0, p1, p2, p3, ends_mine, ends_other, in_mine, in_other, gain_ref, bias_ref, out_ref,
    state_ref, buf, sems,
):
    core = lax.axis_index("head")
    place = lax.axis_index("seq") % PLANE
    groups = ends_mine.shape[0]
    length = in_mine.shape[1]
    first = core == 0
    share = same_head(1.0 / CHANNELS)
    masks = half_masks(CHANNELS)
    for step, piece in enumerate((p0, p1, p2, p3)):
        source = lax.bitwise_xor(place, step) * ROWS
        for group in range(groups):
            at = pl.multiple_of(source + group * CHANNELS, ROWS)
            if step:
                state, _ = get_wire(piece, shrink, group)
            else:
                state = piece[group * ROWS : (group + 1) * ROWS, :]
            state_ref[pl.ds(at, ROWS), :] = state
    states = {}
    for group in range(groups):
        early = jnp.where(first, ends_mine[group], ends_other[group])
        near = state_ref[group * CHANNELS : (group + 1) * CHANNELS, :]
        far = jnp.exp(early[CHANNELS : CHANNELS + 1]) * near + early[:CHANNELS]
        near = split(near - jnp.mean(near, axis=0, keepdims=True))
        far = split(far - jnp.mean(far, axis=0, keepdims=True))
        for side in range(2):
            pick = first if side == 0 else jnp.logical_not(first)
            states[side, group] = [
                spread_heads(jnp.where(pick, one, two), masks) for one, two in zip(near, far)
            ]
    copies = []
    for side, local in enumerate((in_mine, in_other)):
        mixes, spreads = {}, {}
        for group in range(groups):
            out = pl.ds(group * LANES, LANES)
            s_high, s_low = states[side, group]
            r_high, r_low = split(local[1, :, out])
            mixes[group] = local[0, :, out] + (
                dot_nt(r_high, s_high) + dot_nt(r_low, s_high) + dot_nt(r_high, s_low)
            )
        for group in range(groups):
            q_high, q_low = split(mixes[group] * mixes[group])
            spreads[group] = dot(q_high, share) + dot(q_low, share)
        for group in range(groups):
            gain, bias = tile_row(gain_ref, group, groups), tile_row(bias_ref, group, groups)
            out = pl.ds(group * LANES, LANES)
            normed = mixes[group] * lax.rsqrt(spreads[group] + 1e-5)
            gated = (normed * gain + bias) * local[2, :, out]
            buf[side, :, out] = gated.astype(BF16)
        rows = pl.ds(pl.multiple_of((core if side == 0 else 1 - core) * length, length), length)
        copies.append(pltpu.make_async_copy(buf.at[side], out_ref.at[rows, :], sems.at[side]))
        copies[-1].start()
    for copy in copies:
        copy.wait()


def program(r, k, v, w, gate, bonus, gain, bias):
    length, width = r.shape
    cores, count = lax.axis_size("head"), lax.axis_size("seq")
    planes = count // PLANE
    assert cores == 2 and count == planes * PLANE
    assert planes > 1 and planes & (planes - 1) == 0
    half = width // cores
    groups = half // LANES
    swap = [(0, 1), (1, 0)]
    hbm = pl.BlockSpec(memory_space=pltpu.HBM)
    gain, bias = gain.reshape(-1, TILE), bias.reshape(-1, TILE)

    def call(kernel, outs, **options):
        return pl.pallas_call(
            kernel,
            out_shape=outs,
            compiler_params=pltpu.CompilerParams(vmem_limit_bytes=VMEM_LIMIT),
            **options,
        )

    ends_shape = jax.ShapeDtypeStruct((groups, CHANNELS + 8, LANES), F32)
    packed_rows = -(-groups * (ROWS + 1) // 8) * 8
    packed = jax.ShapeDtypeStruct((packed_rows, LANES), F32)
    wire = jax.ShapeDtypeStruct((wire_rows(groups), LANES), F32)
    piece = jax.ShapeDtypeStruct((groups * ROWS, LANES), F32)
    shrink = 1.0
    while STATE_STEP * length * cores * count * shrink > 2.0**15:
        shrink *= 0.5

    held = pltpu.VMEM((length, width), BF16)
    mine, theirs, k, v, w = call(
        ends_kernel,
        [pltpu.VMEM(ends_shape.shape, F32)] * 2 + [held] * 3,
        in_specs=[hbm] * 3,
        scratch_shapes=[pltpu.SemaphoreType.DMA((cores, 3))],
    )(*(pltpu.with_memory_space_constraint(x, pltpu.HBM) for x in (k, v, w)))
    other = lax.ppermute(theirs, "head", swap)

    def within(side):
        return call(
            functools.partial(within_kernel, side), jax.ShapeDtypeStruct((3, length, half), F32)
        )(r, k, v, w, gate, bonus)

    def over_seq(value, flip):
        pairs = [(i, i ^ flip) for i in range(count)]
        return lax.ppermute(value.astype(jnp.float16), "seq", pairs).astype(F32)

    def to_places(pieces):
        return [pieces[0]] + [over_seq(pieces[step], step) for step in range(1, PLANE)]

    def mirror(value, bit):
        return over_seq(value, (2 * bit - 1) * PLANE)

    quarters = call(
        functools.partial(combine_kernel, shrink),
        [packed] + [wire] * (PLANE - 1),
        scratch_shapes=[pltpu.VMEM((groups, CHANNELS, LANES), F32)],
    )(mine, other)
    in_other = lax.ppermute(within(1), "head", swap)
    total, sent, prefix = call(
        functools.partial(plane_kernel, groups, shrink),
        [packed, wire, jax.ShapeDtypeStruct((PLANE,) + packed.shape, F32)],
        scratch_shapes=[pltpu.VMEM((PLANE,) + packed.shape, F32)],
    )(*to_places(quarters))
    in_mine = within(0)
    before = total
    bit = 1
    while 2 * bit < planes:
        total, sent, before = call(
            functools.partial(round_kernel, groups, shrink, bit, bit == 1), [packed, wire, packed]
        )(total, mirror(sent, bit), before)
        bit *= 2
    states = call(
        functools.partial(back_kernel, groups, shrink, bit), [piece] + [wire] * (PLANE - 1)
    )(prefix, before, mirror(sent, bit))
    return call(
        functools.partial(finish_kernel, shrink),
        jax.ShapeDtypeStruct((cores * length, half), BF16),
        out_specs=hbm,
        scratch_shapes=[
            pltpu.VMEM((groups * CHANNELS, LANES), F32),
            pltpu.VMEM((cores, length, half), BF16),
            pltpu.SemaphoreType.DMA((cores,)),
        ],
    )(*to_places(states), mine, other, in_mine, in_other, gain, bias)


def solution(mesh):
    tokens = P(("seq", "head"), None)
    return jax.shard_map(
        program,
        mesh=mesh,
        in_specs=(tokens,) * 5 + (P(), P(), P()),
        out_specs=P("seq", "head"),
        check_vma=False,
    )
```

```python
import functools

import jax
import jax.numpy as jnp
from jax import lax
from jax.experimental import pallas as pl
from jax.experimental.pallas import tpu as pltpu
from jax.sharding import PartitionSpec as P


CHANNELS = 64
TILE = 128
LANES = 256
HEADS = LANES // CHANNELS
BLOCK = 64
PLANE = 4
ROWS = CHANNELS // PLANE
STATE_STEP = 0.75 * 6.0
SCALE_FLOOR = 2.0**-10
CODE_SPAN = 29.5
CODE_LOW = 14.0
VMEM_LIMIT = 12 * 2**20
F32 = jnp.float32
BF16 = jnp.bfloat16


def split(value):
    high = value.astype(BF16)
    return high, (value - high.astype(F32)).astype(BF16)


def dot(left, right):
    return lax.dot_general(left, right, (((1,), (0,)), ((), ())), preferred_element_type=F32)


def dot_nt(left, right):
    return lax.dot_general(left, right, (((1,), (1,)), ((), ())), preferred_element_type=F32)


def same_head(value):
    rows = lax.broadcasted_iota(jnp.int32, (LANES, LANES), 0) // CHANNELS
    columns = lax.broadcasted_iota(jnp.int32, (LANES, LANES), 1) // CHANNELS
    return jnp.where(rows == columns, F32(value), F32(0.0)).astype(BF16)


def half_masks(rows):
    left = lax.broadcasted_iota(jnp.int32, (rows, TILE), 1) < CHANNELS
    one, zero = F32(1.0), F32(0.0)
    return jnp.where(left, one, zero).astype(BF16), jnp.where(left, zero, one).astype(BF16)


def spread_heads(value, masks):
    zero = jnp.zeros((value.shape[0], TILE), value.dtype)
    pieces = []
    for head in range(HEADS):
        tile = head // 2
        kept = value[:, tile * TILE : (tile + 1) * TILE] * masks[head % 2]
        pieces.append(
            jnp.concatenate([kept if i == tile else zero for i in range(LANES // TILE)], axis=1)
        )
    return jnp.concatenate(pieces, axis=0)


def own_blocks(stacked, rows):
    left = lax.broadcasted_iota(jnp.int32, (rows, TILE), 1) < CHANNELS
    pieces = []
    for tile in range(LANES // TILE):
        part = stacked[:, tile * TILE : (tile + 1) * TILE]
        head = 2 * tile
        pieces.append(
            jnp.where(
                left,
                part[head * rows : (head + 1) * rows],
                part[(head + 1) * rows : (head + 2) * rows],
            )
        )
    return jnp.concatenate(pieces, axis=1)


def cumulate(decay):
    length = decay.shape[0]
    rows = lax.broadcasted_iota(jnp.int32, (length, length), 0)
    columns = lax.broadcasted_iota(jnp.int32, (length, length), 1)
    lower = jnp.where(rows >= columns, F32(1.0), F32(0.0)).astype(BF16)
    return dot(lower, decay)


def lanes_at(side, group, groups):
    core = lax.axis_index("head")
    core = core if side == 0 else 1 - core
    return pl.ds(pl.multiple_of((core * groups + group) * LANES, LANES), LANES)


def bonus_row(ref, side, group, groups):
    core = lax.axis_index("head")
    core = core if side == 0 else 1 - core
    first = (core * groups + group) * HEADS
    return jnp.concatenate([ref[pl.ds(first + head, 1), :] for head in range(HEADS)], axis=1)


def tile_row(ref, group, groups):
    tiles = LANES // TILE
    first = (lax.axis_index("head") * groups + group) * tiles
    return jnp.concatenate([ref[pl.ds(first + tile, 1), :] for tile in range(tiles)], axis=1)


def half_at(side, half):
    core = lax.axis_index("head")
    core = core if side == 0 else 1 - core
    return pl.ds(pl.multiple_of(core * half, LANES), half)


def ends_kernel(
    k_ref, v_ref, w_ref, r_ref, g_ref, mine_ref, theirs_ref, k_buf, v_buf, w_buf, r_buf, g_buf,
    sems, late_sems,
):
    groups = mine_ref.shape[0]
    half = groups * LANES
    copies = {}
    for side in (1, 0):
        at = half_at(side, half)
        for index, (ref, buf) in enumerate(((w_ref, w_buf), (k_ref, k_buf), (v_ref, v_buf))):
            copies[side, index] = pltpu.make_async_copy(
                ref.at[:, at], buf.at[:, pl.ds(side * half, half)], sems.at[side, index]
            )
            copies[side, index].start()
    late = []
    for index, (ref, buf) in enumerate(((r_ref, r_buf), (g_ref, g_buf))):
        late.append(pltpu.make_async_copy(ref, buf, late_sems.at[index]))
        late[-1].start()
    for side, out_ref in ((1, theirs_ref), (0, mine_ref)):
        for index in range(3):
            copies[side, index].wait()
        span = range(groups)
        at = [pl.ds(side * half + group * LANES, LANES) for group in span]
        cumuls = [cumulate(w_buf[:, at[group]]) for group in span]
        turned = [v_buf[:, at[group]].astype(F32).T.astype(BF16) for group in span]
        weighted = []
        for group in span:
            final = cumuls[group][-1:]
            out_ref[group, CHANNELS:, :] = jnp.broadcast_to(final, (8, LANES))
            weighted.append(split(k_buf[:, at[group]].astype(F32) * jnp.exp(final - cumuls[group])))
        for group in span:
            wide = dot(
                jnp.concatenate([turned[group]] * 2, axis=1),
                jnp.concatenate(weighted[group], axis=0),
            )
            out_ref[group, :CHANNELS, :] = own_blocks(wide, CHANNELS)
    for copy in late:
        copy.wait()


def log_row(groups, group):
    return slice(groups * ROWS + group, groups * ROWS + group + 1)


def wire_rows(groups):
    return -(-groups * (ROWS + 3) // 16) * 16


def put_wire(ref, shrink, group, state, log=None):
    groups = ref.shape[0] // (ROWS + 3)
    top = jnp.max(jnp.abs(state), axis=0, keepdims=True)
    scale = (top * 1.01 + SCALE_FLOOR).astype(BF16).astype(F32)
    code = jnp.exp2(jnp.abs(state) * (CODE_SPAN / scale) - CODE_LOW)
    ref[group * ROWS : (group + 1) * ROWS, :] = jnp.where(state < 0.0, -code, code)
    row = groups * ROWS + group
    ref[row : row + 1, :] = scale * F32(shrink)
    high = jnp.zeros((1, LANES), F32) if log is None else log.astype(BF16).astype(F32)
    ref[row + groups : row + groups + 1, :] = high
    low = high if log is None else log - high
    ref[row + 2 * groups : row + 2 * groups + 1, :] = low


def clear_rest(ref):
    groups = ref.shape[0] // (ROWS + 3)
    rest = ref.shape[0] - groups * (ROWS + 3)
    if rest:
        ref[groups * (ROWS + 3) :, :] = jnp.zeros((rest, LANES), F32)


def get_wire(ref, shrink, group):
    groups = ref.shape[0] // (ROWS + 3)
    row = groups * ROWS + group
    scale = ref[row : row + 1, :] * F32(1.0 / (shrink * CODE_SPAN))
    code = ref[group * ROWS : (group + 1) * ROWS, :]
    size = (jnp.log2(jnp.abs(code)) + CODE_LOW) * scale
    log = ref[row + groups : row + groups + 1, :] + ref[row + 2 * groups : row + 2 * groups + 1, :]
    return jnp.where(code < 0.0, -size, size), log


def combine_kernel(shrink, mine_ref, other_ref, q0, q1, q2, q3, state_ref):
    core = lax.axis_index("head")
    place = lax.axis_index("seq") % PLANE
    groups = mine_ref.shape[0]
    first = core == 0
    for out in (q1, q2, q3):
        clear_rest(out)
    for group in range(groups):
        mine, other = mine_ref[group], other_ref[group]
        early, late = jnp.where(first, mine, other), jnp.where(first, other, mine)
        late_log = late[CHANNELS : CHANNELS + 1]
        state_ref[group] = early[:CHANNELS] * jnp.exp(late_log) + late[:CHANNELS]
        both = early[CHANNELS : CHANNELS + 1] + late_log
        for step, out in enumerate((q0, q1, q2, q3)):
            at = pl.multiple_of(lax.bitwise_xor(place, step) * ROWS, ROWS)
            state = state_ref[group, pl.ds(at, ROWS), :]
            if step:
                put_wire(out, shrink, group, state, both)
            else:
                out[group * ROWS : (group + 1) * ROWS, :] = state
                out[log_row(groups, group), :] = both


def plane_kernel(groups, shrink, q0, q1, q2, q3, total_ref, wire_ref, prefix_ref, slab_ref):
    place = lax.axis_index("seq") % PLANE
    clear_rest(wire_ref)
    for group in range(groups):
        rows = slice(group * ROWS, (group + 1) * ROWS)
        row = log_row(groups, group)
        slab_ref[place, rows, :] = q0[rows, :]
        slab_ref[place, row, :] = q0[row, :]
        for step, piece in ((1, q1), (2, q2), (3, q3)):
            to = lax.bitwise_xor(place, step)
            state, log = get_wire(piece, shrink, group)
            slab_ref[to, rows, :] = state
            slab_ref[to, row, :] = log
    for group in range(groups):
        rows = slice(group * ROWS, (group + 1) * ROWS)
        row = log_row(groups, group)
        state = jnp.zeros((ROWS, LANES), F32)
        log = jnp.zeros((1, LANES), F32)
        for slab in range(PLANE):
            prefix_ref[slab, rows, :] = state
            prefix_ref[slab, row, :] = jnp.exp(log)
            step = slab_ref[slab, row, :]
            state = jnp.exp(step) * state + slab_ref[slab, rows, :]
            log = log + step
        total_ref[rows, :] = state
        total_ref[row, :] = log
        put_wire(wire_ref, shrink, group, state, log)


def round_kernel(
    groups, shrink, bit, first_round, total_ref, got_ref, before_ref, wire_out, before_out, *total_out
):
    plane = lax.axis_index("seq") // PLANE
    upper = lax.bitwise_and(plane, bit) != 0
    clear_rest(wire_out)
    for group in range(groups):
        rows = slice(group * ROWS, (group + 1) * ROWS)
        row = log_row(groups, group)
        total, total_log = total_ref[rows, :], total_ref[row, :]
        got, got_log = get_wire(got_ref, shrink, group)
        low, high = jnp.where(upper, got, total), jnp.where(upper, total, got)
        both = jnp.exp(jnp.where(upper, total_log, got_log)) * low + high
        for out in total_out:
            out[rows, :] = both
            out[row, :] = total_log + got_log
        put_wire(wire_out, shrink, group, both, total_log + got_log)
        if first_round:
            before = jnp.where(upper, got, F32(0.0))
            before_decay = jnp.where(upper, jnp.exp(got_log), F32(1.0))
        else:
            decay = before_ref[row, :]
            before = before_ref[rows, :]
            before = jnp.where(upper, decay * got + before, before)
            before_decay = jnp.where(upper, jnp.exp(got_log) * decay, decay)
        before_out[rows, :] = before
        before_out[row, :] = before_decay


def back_kernel(groups, shrink, bit, prefix_ref, before_ref, got_ref, p0, p1, p2, p3):
    seq = lax.axis_index("seq")
    place = seq % PLANE
    upper = lax.bitwise_and(seq // PLANE, bit) != 0
    for out in (p1, p2, p3):
        clear_rest(out)
    for group in range(groups):
        rows = slice(group * ROWS, (group + 1) * ROWS)
        row = log_row(groups, group)
        before = before_ref[rows, :]
        got, _ = get_wire(got_ref, shrink, group)
        before = jnp.where(upper, before_ref[row, :] * got + before, before)
        for step, out in enumerate((p0, p1, p2, p3)):
            to = lax.bitwise_xor(place, step)
            state = prefix_ref[to, row, :] * before + prefix_ref[to, rows, :]
            if step:
                put_wire(out, shrink, group, state)
            else:
                out[rows, :] = state


def within_kernel(side, r_ref, k_ref, v_ref, w_ref, g_ref, bonus_ref, out_ref):
    groups = out_ref.shape[2] // LANES
    length = w_ref.shape[0]
    ones = same_head(1.0)
    share = same_head(1.0 / CHANNELS)
    masks = half_masks(BLOCK)
    shape = (HEADS * length, length)
    row = lax.broadcasted_iota(jnp.int32, shape, 0)
    later = row // (HEADS * BLOCK) * BLOCK + row % BLOCK
    strict = later > lax.broadcasted_iota(jnp.int32, shape, 1)
    span = range(groups)
    at = [lanes_at(side, group, groups) for group in span]
    out = [pl.ds(group * LANES, LANES) for group in span]
    held = [pl.ds((side * groups + group) * LANES, LANES) for group in span]
    cumuls = [cumulate(w_ref[:, held[group]]) for group in span]
    for group in span:
        gate = g_ref[:, at[group]].astype(F32)
        out_ref[2, :, out[group]] = gate / (1.0 + jnp.exp(-gate))
    scores = []
    for group in span:
        r, k = r_ref[:, at[group]].astype(F32), k_ref[:, held[group]].astype(F32)
        cumul = cumuls[group]
        before = cumul - w_ref[:, held[group]].astype(F32)
        out_ref[1, :, out[group]] = r * jnp.exp(before)
        pieces = []
        for start in range(0, length, BLOCK):
            stop = start + BLOCK
            middle = start + BLOCK // 2 - 1
            reference = cumul[middle : middle + 1]
            r_high, r_low = split(r[start:stop] * jnp.exp(before[start:stop] - reference))
            k_high, k_low = split(k[:stop] * jnp.exp(reference - cumul[:stop]))
            if stop < length:
                rest = jnp.zeros((length - stop, LANES), BF16)
                k_high = jnp.concatenate([k_high, rest], axis=0)
                k_low = jnp.concatenate([k_low, rest], axis=0)
            r_high, r_low = spread_heads(r_high, masks), spread_heads(r_low, masks)
            pieces.append(dot_nt(r_high, k_high) + dot_nt(r_low, k_high) + dot_nt(r_high, k_low))
        scores.append(split(jnp.where(strict, jnp.concatenate(pieces, axis=0), F32(0.0))))
    mixes = []
    for group in span:
        v = v_ref[:, held[group]]
        wide = dot(jnp.concatenate(scores[group], axis=1), jnp.concatenate([v, v], axis=0))
        step = HEADS * BLOCK
        mixed = jnp.concatenate(
            [own_blocks(wide[i * step : (i + 1) * step], BLOCK) for i in range(length // BLOCK)],
            axis=0,
        )
        r, k = r_ref[:, at[group]].astype(F32), k_ref[:, held[group]].astype(F32)
        diagonal_high, diagonal_low = split(r * bonus_row(bonus_ref, side, group, groups) * k)
        diagonal = dot(diagonal_high, ones) + dot(diagonal_low, ones)
        mixes.append(mixed + diagonal * v.astype(F32))
    for group in span:
        m_high, m_low = split(mixes[group])
        out_ref[0, :, out[group]] = mixes[group] - (dot(m_high, share) + dot(m_low, share))


def finish_kernel(
    shrink, p0, p1, p2, p3, ends_mine, ends_other, in_mine, in_other, gain_ref, bias_ref, out_ref,
    state_ref, buf, sems,
):
    core = lax.axis_index("head")
    place = lax.axis_index("seq") % PLANE
    groups = ends_mine.shape[0]
    length = in_mine.shape[1]
    first = core == 0
    share = same_head(1.0 / CHANNELS)
    masks = half_masks(CHANNELS)
    for step, piece in enumerate((p0, p1, p2, p3)):
        source = lax.bitwise_xor(place, step) * ROWS
        for group in range(groups):
            at = pl.multiple_of(source + group * CHANNELS, ROWS)
            if step:
                state, _ = get_wire(piece, shrink, group)
            else:
                state = piece[group * ROWS : (group + 1) * ROWS, :]
            state_ref[pl.ds(at, ROWS), :] = state
    states = {}
    for group in range(groups):
        early = jnp.where(first, ends_mine[group], ends_other[group])
        near = state_ref[group * CHANNELS : (group + 1) * CHANNELS, :]
        far = jnp.exp(early[CHANNELS : CHANNELS + 1]) * near + early[:CHANNELS]
        near = split(near - jnp.mean(near, axis=0, keepdims=True))
        far = split(far - jnp.mean(far, axis=0, keepdims=True))
        for side in range(2):
            pick = first if side == 0 else jnp.logical_not(first)
            states[side, group] = [
                spread_heads(jnp.where(pick, one, two), masks) for one, two in zip(near, far)
            ]
    copies = []
    for side, local in enumerate((in_mine, in_other)):
        mixes, spreads = {}, {}
        for group in range(groups):
            out = pl.ds(group * LANES, LANES)
            s_high, s_low = states[side, group]
            r_high, r_low = split(local[1, :, out])
            mixes[group] = local[0, :, out] + (
                dot_nt(r_high, s_high) + dot_nt(r_low, s_high) + dot_nt(r_high, s_low)
            )
        for group in range(groups):
            q_high, q_low = split(mixes[group] * mixes[group])
            spreads[group] = dot(q_high, share) + dot(q_low, share)
        for group in range(groups):
            gain, bias = tile_row(gain_ref, group, groups), tile_row(bias_ref, group, groups)
            out = pl.ds(group * LANES, LANES)
            normed = mixes[group] * lax.rsqrt(spreads[group] + 1e-5)
            gated = (normed * gain + bias) * local[2, :, out]
            buf[side, :, out] = gated.astype(BF16)
        rows = pl.ds(pl.multiple_of((core if side == 0 else 1 - core) * length, length), length)
        copies.append(pltpu.make_async_copy(buf.at[side], out_ref.at[rows, :], sems.at[side]))
        copies[-1].start()
    for copy in copies:
        copy.wait()


def program(r, k, v, w, gate, bonus, gain, bias):
    length, width = r.shape
    cores, count = lax.axis_size("head"), lax.axis_size("seq")
    planes = count // PLANE
    assert cores == 2 and count == planes * PLANE
    assert planes > 1 and planes & (planes - 1) == 0
    half = width // cores
    groups = half // LANES
    swap = [(0, 1), (1, 0)]
    hbm = pl.BlockSpec(memory_space=pltpu.HBM)
    gain, bias = gain.reshape(-1, TILE), bias.reshape(-1, TILE)

    def call(kernel, outs, **options):
        return pl.pallas_call(
            kernel,
            out_shape=outs,
            compiler_params=pltpu.CompilerParams(vmem_limit_bytes=VMEM_LIMIT),
            **options,
        )

    ends_shape = jax.ShapeDtypeStruct((groups, CHANNELS + 8, LANES), F32)
    packed_rows = -(-groups * (ROWS + 1) // 8) * 8
    packed = jax.ShapeDtypeStruct((packed_rows, LANES), F32)
    wire = jax.ShapeDtypeStruct((wire_rows(groups), LANES), F32)
    piece = jax.ShapeDtypeStruct((groups * ROWS, LANES), F32)
    shrink = 1.0
    while STATE_STEP * length * cores * count * shrink > 2.0**15:
        shrink *= 0.5

    held = pltpu.VMEM((length, width), BF16)
    mine, theirs, k, v, w, r, gate = call(
        ends_kernel,
        [pltpu.VMEM(ends_shape.shape, F32)] * 2 + [held] * 5,
        in_specs=[hbm] * 5,
        scratch_shapes=[pltpu.SemaphoreType.DMA((cores, 3)), pltpu.SemaphoreType.DMA((2,))],
    )(*(pltpu.with_memory_space_constraint(x, pltpu.HBM) for x in (k, v, w, r, gate)))
    other = lax.ppermute(theirs, "head", swap)

    def within(side):
        return call(
            functools.partial(within_kernel, side), jax.ShapeDtypeStruct((3, length, half), F32)
        )(r, k, v, w, gate, bonus)

    def over_seq(value, flip):
        pairs = [(i, i ^ flip) for i in range(count)]
        return lax.ppermute(value.astype(jnp.float16), "seq", pairs).astype(F32)

    def to_places(pieces):
        return [pieces[0]] + [over_seq(pieces[step], step) for step in range(1, PLANE)]

    def mirror(value, bit):
        return over_seq(value, (2 * bit - 1) * PLANE)

    quarters = call(
        functools.partial(combine_kernel, shrink),
        [packed] + [wire] * (PLANE - 1),
        scratch_shapes=[pltpu.VMEM((groups, CHANNELS, LANES), F32)],
    )(mine, other)
    in_other = lax.ppermute(within(1), "head", swap)
    total, sent, prefix = call(
        functools.partial(plane_kernel, groups, shrink),
        [packed, wire, jax.ShapeDtypeStruct((PLANE,) + packed.shape, F32)],
        scratch_shapes=[pltpu.VMEM((PLANE,) + packed.shape, F32)],
    )(*to_places(quarters))
    in_mine = within(0)
    before = total
    bit = 1
    while 2 * bit < planes:
        more = 4 * bit < planes
        sent, before, *rest = call(
            functools.partial(round_kernel, groups, shrink, bit, bit == 1),
            [wire, packed] + [packed] * more,
        )(total, mirror(sent, bit), before)
        total = rest[0] if more else None
        bit *= 2
    states = call(
        functools.partial(back_kernel, groups, shrink, bit), [piece] + [wire] * (PLANE - 1)
    )(prefix, before, mirror(sent, bit))
    return call(
        functools.partial(finish_kernel, shrink),
        jax.ShapeDtypeStruct((cores * length, half), BF16),
        out_specs=hbm,
        scratch_shapes=[
            pltpu.VMEM((groups * CHANNELS, LANES), F32),
            pltpu.VMEM((cores, length, half), BF16),
            pltpu.SemaphoreType.DMA((cores,)),
        ],
    )(*to_places(states), mine, other, in_mine, in_other, gain, bias)


def solution(mesh):
    tokens = P(("seq", "head"), None)
    return jax.shard_map(
        program,
        mesh=mesh,
        in_specs=(tokens,) * 5 + (P(), P(), P()),
        out_specs=P("seq", "head"),
        check_vma=False,
    )
```

```python
import functools

import jax
import jax.numpy as jnp
from jax import lax
from jax.experimental import pallas as pl
from jax.experimental.pallas import tpu as pltpu
from jax.sharding import PartitionSpec as P


CHANNELS = 64
TILE = 128
LANES = 256
HEADS = LANES // CHANNELS
BLOCK = 64
PLANE = 4
ROWS = CHANNELS // PLANE
STATE_STEP = 0.75 * 6.0
SCALE_FLOOR = 2.0**-10
CODE_SPAN = 29.5
CODE_LOW = 14.0
VMEM_LIMIT = 12 * 2**20
F32 = jnp.float32
BF16 = jnp.bfloat16


def split(value):
    high = value.astype(BF16)
    return high, (value - high.astype(F32)).astype(BF16)


def dot(left, right):
    return lax.dot_general(left, right, (((1,), (0,)), ((), ())), preferred_element_type=F32)


def dot_nt(left, right):
    return lax.dot_general(left, right, (((1,), (1,)), ((), ())), preferred_element_type=F32)


def same_head(value):
    rows = lax.broadcasted_iota(jnp.int32, (LANES, LANES), 0) // CHANNELS
    columns = lax.broadcasted_iota(jnp.int32, (LANES, LANES), 1) // CHANNELS
    return jnp.where(rows == columns, F32(value), F32(0.0)).astype(BF16)


def half_masks(rows):
    left = lax.broadcasted_iota(jnp.int32, (rows, TILE), 1) < CHANNELS
    one, zero = F32(1.0), F32(0.0)
    return jnp.where(left, one, zero).astype(BF16), jnp.where(left, zero, one).astype(BF16)


def spread_heads(value, masks):
    zero = jnp.zeros((value.shape[0], TILE), value.dtype)
    pieces = []
    for head in range(HEADS):
        tile = head // 2
        kept = value[:, tile * TILE : (tile + 1) * TILE] * masks[head % 2]
        pieces.append(
            jnp.concatenate([kept if i == tile else zero for i in range(LANES // TILE)], axis=1)
        )
    return jnp.concatenate(pieces, axis=0)


def own_blocks(stacked, rows):
    left = lax.broadcasted_iota(jnp.int32, (rows, TILE), 1) < CHANNELS
    pieces = []
    for tile in range(LANES // TILE):
        part = stacked[:, tile * TILE : (tile + 1) * TILE]
        head = 2 * tile
        pieces.append(
            jnp.where(
                left,
                part[head * rows : (head + 1) * rows],
                part[(head + 1) * rows : (head + 2) * rows],
            )
        )
    return jnp.concatenate(pieces, axis=1)


def cumulate(decay):
    length = decay.shape[0]
    rows = lax.broadcasted_iota(jnp.int32, (length, length), 0)
    columns = lax.broadcasted_iota(jnp.int32, (length, length), 1)
    lower = jnp.where(rows >= columns, F32(1.0), F32(0.0)).astype(BF16)
    return dot(lower, decay)


def lanes_at(side, group, groups):
    core = lax.axis_index("head")
    core = core if side == 0 else 1 - core
    return pl.ds(pl.multiple_of((core * groups + group) * LANES, LANES), LANES)


def bonus_row(ref, side, group, groups):
    core = lax.axis_index("head")
    core = core if side == 0 else 1 - core
    first = (core * groups + group) * HEADS
    return jnp.concatenate([ref[pl.ds(first + head, 1), :] for head in range(HEADS)], axis=1)


def tile_row(ref, group, groups):
    tiles = LANES // TILE
    first = (lax.axis_index("head") * groups + group) * tiles
    return jnp.concatenate([ref[pl.ds(first + tile, 1), :] for tile in range(tiles)], axis=1)


def half_at(side, half):
    core = lax.axis_index("head")
    core = core if side == 0 else 1 - core
    return pl.ds(pl.multiple_of(core * half, LANES), half)


def ends_kernel(
    k_ref, v_ref, w_ref, r_ref, g_ref, mine_ref, theirs_ref, k_buf, v_buf, w_buf, r_buf, g_buf,
    sems, late_sems,
):
    groups = mine_ref.shape[0]
    half = groups * LANES
    copies = {}
    for side in (1, 0):
        at = half_at(side, half)
        for index, (ref, buf) in enumerate(((w_ref, w_buf), (k_ref, k_buf), (v_ref, v_buf))):
            copies[side, index] = pltpu.make_async_copy(
                ref.at[:, at], buf.at[:, pl.ds(side * half, half)], sems.at[side, index]
            )
            copies[side, index].start()
    late = []
    for index, (ref, buf) in enumerate(((r_ref, r_buf), (g_ref, g_buf))):
        late.append(pltpu.make_async_copy(ref, buf, late_sems.at[index]))
        late[-1].start()
    for side, out_ref in ((1, theirs_ref), (0, mine_ref)):
        for index in range(3):
            copies[side, index].wait()
        span = range(groups)
        at = [pl.ds(side * half + group * LANES, LANES) for group in span]
        cumuls = [cumulate(w_buf[:, at[group]]) for group in span]
        turned = [v_buf[:, at[group]].astype(F32).T.astype(BF16) for group in span]
        weighted = []
        for group in span:
            final = cumuls[group][-1:]
            out_ref[group, CHANNELS:, :] = jnp.broadcast_to(final, (8, LANES))
            weighted.append(split(k_buf[:, at[group]].astype(F32) * jnp.exp(final - cumuls[group])))
        for group in span:
            wide = dot(
                jnp.concatenate([turned[group]] * 2, axis=1),
                jnp.concatenate(weighted[group], axis=0),
            )
            out_ref[group, :CHANNELS, :] = own_blocks(wide, CHANNELS)
    for copy in late:
        copy.wait()


def log_row(groups, group):
    return slice(groups * ROWS + group, groups * ROWS + group + 1)


def wire_rows(groups):
    return -(-groups * (ROWS + 3) // 16) * 16


def put_wire(ref, shrink, group, state, log=None):
    groups = ref.shape[0] // (ROWS + 3)
    top = jnp.max(jnp.abs(state), axis=0, keepdims=True)
    scale = (top * 1.01 + SCALE_FLOOR).astype(BF16).astype(F32)
    code = jnp.exp2(jnp.abs(state) * (CODE_SPAN / scale) - CODE_LOW)
    ref[group * ROWS : (group + 1) * ROWS, :] = jnp.where(state < 0.0, -code, code)
    row = groups * ROWS + group
    ref[row : row + 1, :] = scale * F32(shrink)
    high = jnp.zeros((1, LANES), F32) if log is None else log.astype(BF16).astype(F32)
    ref[row + groups : row + groups + 1, :] = high
    low = high if log is None else log - high
    ref[row + 2 * groups : row + 2 * groups + 1, :] = low


def clear_rest(ref):
    groups = ref.shape[0] // (ROWS + 3)
    rest = ref.shape[0] - groups * (ROWS + 3)
    if rest:
        ref[groups * (ROWS + 3) :, :] = jnp.zeros((rest, LANES), F32)


def get_wire(ref, shrink, group):
    groups = ref.shape[0] // (ROWS + 3)
    row = groups * ROWS + group
    scale = ref[row : row + 1, :] * F32(1.0 / (shrink * CODE_SPAN))
    code = ref[group * ROWS : (group + 1) * ROWS, :]
    size = (jnp.log2(jnp.abs(code)) + CODE_LOW) * scale
    log = ref[row + groups : row + groups + 1, :] + ref[row + 2 * groups : row + 2 * groups + 1, :]
    return jnp.where(code < 0.0, -size, size), log


def combine_kernel(shrink, mine_ref, other_ref, q0, q1, q2, q3, state_ref):
    core = lax.axis_index("head")
    place = lax.axis_index("seq") % PLANE
    groups = mine_ref.shape[0]
    first = core == 0
    for out in (q1, q2, q3):
        clear_rest(out)
    for group in range(groups):
        mine, other = mine_ref[group], other_ref[group]
        early, late = jnp.where(first, mine, other), jnp.where(first, other, mine)
        late_log = late[CHANNELS : CHANNELS + 1]
        state_ref[group] = early[:CHANNELS] * jnp.exp(late_log) + late[:CHANNELS]
        both = early[CHANNELS : CHANNELS + 1] + late_log
        for step, out in enumerate((q0, q1, q2, q3)):
            at = pl.multiple_of(lax.bitwise_xor(place, step) * ROWS, ROWS)
            state = state_ref[group, pl.ds(at, ROWS), :]
            if step:
                put_wire(out, shrink, group, state, both)
            else:
                out[group * ROWS : (group + 1) * ROWS, :] = state
                out[log_row(groups, group), :] = both


def plane_kernel(groups, shrink, q0, q1, q2, q3, total_ref, wire_ref, prefix_ref, slab_ref):
    place = lax.axis_index("seq") % PLANE
    clear_rest(wire_ref)
    for group in range(groups):
        rows = slice(group * ROWS, (group + 1) * ROWS)
        row = log_row(groups, group)
        slab_ref[place, rows, :] = q0[rows, :]
        slab_ref[place, row, :] = q0[row, :]
        for step, piece in ((1, q1), (2, q2), (3, q3)):
            to = lax.bitwise_xor(place, step)
            state, log = get_wire(piece, shrink, group)
            slab_ref[to, rows, :] = state
            slab_ref[to, row, :] = log
    for group in range(groups):
        rows = slice(group * ROWS, (group + 1) * ROWS)
        row = log_row(groups, group)
        state = jnp.zeros((ROWS, LANES), F32)
        log = jnp.zeros((1, LANES), F32)
        for slab in range(PLANE):
            prefix_ref[slab, rows, :] = state
            prefix_ref[slab, row, :] = jnp.exp(log)
            step = slab_ref[slab, row, :]
            state = jnp.exp(step) * state + slab_ref[slab, rows, :]
            log = log + step
        total_ref[rows, :] = state
        total_ref[row, :] = log
        put_wire(wire_ref, shrink, group, state, log)


def group_prefix(groups, shrink, bit, radix, total_ref, got_refs, slab_ref):
    mine = lax.axis_index("seq") // PLANE // bit % radix
    for group in range(groups):
        rows = slice(group * ROWS, (group + 1) * ROWS)
        row = log_row(groups, group)
        slab_ref[mine, rows, :] = total_ref[rows, :]
        slab_ref[mine, row, :] = total_ref[row, :]
        for step, got in enumerate(got_refs, 1):
            to = lax.bitwise_xor(mine, step)
            state, log = get_wire(got, shrink, group)
            slab_ref[to, rows, :] = state
            slab_ref[to, row, :] = log
    found = []
    for group in range(groups):
        rows = slice(group * ROWS, (group + 1) * ROWS)
        row = log_row(groups, group)
        state, log = jnp.zeros((ROWS, LANES), F32), jnp.zeros((1, LANES), F32)
        before, before_log = state, log
        for slab in range(radix):
            step = slab_ref[slab, row, :]
            state = jnp.exp(step) * state + slab_ref[slab, rows, :]
            log = log + step
            before = jnp.where(slab < mine, state, before)
            before_log = jnp.where(slab < mine, log, before_log)
        found.append((before, before_log, state, log))
    return found


def round_kernel(groups, shrink, bit, radix, first, *refs):
    total_ref, before_ref, *got_refs = refs[: 2 + radix - 1]
    total_out, wire_out, before_out, slab_ref = refs[2 + radix - 1 :]
    clear_rest(wire_out)
    found = group_prefix(groups, shrink, bit, radix, total_ref, got_refs, slab_ref)
    for group, (state, log, total, total_log) in enumerate(found):
        rows = slice(group * ROWS, (group + 1) * ROWS)
        row = log_row(groups, group)
        if not first:
            state = jnp.exp(before_ref[row, :]) * state + before_ref[rows, :]
            log = log + before_ref[row, :]
        before_out[rows, :] = state
        before_out[row, :] = log
        total_out[rows, :] = total
        total_out[row, :] = total_log
        put_wire(wire_out, shrink, group, total, total_log)


def back_kernel(groups, shrink, bit, radix, first, *refs):
    prefix_ref, total_ref, before_ref, *got_refs = refs[: 3 + radix - 1]
    *outs, slab_ref = refs[3 + radix - 1 :]
    place = lax.axis_index("seq") % PLANE
    for out in outs[1:]:
        clear_rest(out)
    found = group_prefix(groups, shrink, bit, radix, total_ref, got_refs, slab_ref)
    for group, (before, _, _, _) in enumerate(found):
        rows = slice(group * ROWS, (group + 1) * ROWS)
        row = log_row(groups, group)
        if not first:
            before = jnp.exp(before_ref[row, :]) * before + before_ref[rows, :]
        for step, out in enumerate(outs):
            to = lax.bitwise_xor(place, step)
            state = prefix_ref[to, row, :] * before + prefix_ref[to, rows, :]
            if step:
                put_wire(out, shrink, group, state)
            else:
                out[rows, :] = state


def within_kernel(side, r_ref, k_ref, v_ref, w_ref, g_ref, bonus_ref, out_ref):
    groups = out_ref.shape[2] // LANES
    length = w_ref.shape[0]
    ones = same_head(1.0)
    share = same_head(1.0 / CHANNELS)
    masks = half_masks(BLOCK)
    shape = (HEADS * length, length)
    row = lax.broadcasted_iota(jnp.int32, shape, 0)
    later = row // (HEADS * BLOCK) * BLOCK + row % BLOCK
    strict = later > lax.broadcasted_iota(jnp.int32, shape, 1)
    span = range(groups)
    at = [lanes_at(side, group, groups) for group in span]
    out = [pl.ds(group * LANES, LANES) for group in span]
    held = [pl.ds((side * groups + group) * LANES, LANES) for group in span]
    cumuls = [cumulate(w_ref[:, held[group]]) for group in span]
    for group in span:
        gate = g_ref[:, at[group]].astype(F32)
        out_ref[2, :, out[group]] = gate / (1.0 + jnp.exp(-gate))
    scores = []
    for group in span:
        r, k = r_ref[:, at[group]].astype(F32), k_ref[:, held[group]].astype(F32)
        cumul = cumuls[group]
        before = cumul - w_ref[:, held[group]].astype(F32)
        out_ref[1, :, out[group]] = r * jnp.exp(before)
        pieces = []
        for start in range(0, length, BLOCK):
            stop = start + BLOCK
            middle = start + BLOCK // 2 - 1
            reference = cumul[middle : middle + 1]
            r_high, r_low = split(r[start:stop] * jnp.exp(before[start:stop] - reference))
            k_high, k_low = split(k[:stop] * jnp.exp(reference - cumul[:stop]))
            if stop < length:
                rest = jnp.zeros((length - stop, LANES), BF16)
                k_high = jnp.concatenate([k_high, rest], axis=0)
                k_low = jnp.concatenate([k_low, rest], axis=0)
            r_high, r_low = spread_heads(r_high, masks), spread_heads(r_low, masks)
            pieces.append(dot_nt(r_high, k_high) + dot_nt(r_low, k_high) + dot_nt(r_high, k_low))
        scores.append(split(jnp.where(strict, jnp.concatenate(pieces, axis=0), F32(0.0))))
    mixes = []
    for group in span:
        v = v_ref[:, held[group]]
        wide = dot(jnp.concatenate(scores[group], axis=1), jnp.concatenate([v, v], axis=0))
        step = HEADS * BLOCK
        mixed = jnp.concatenate(
            [own_blocks(wide[i * step : (i + 1) * step], BLOCK) for i in range(length // BLOCK)],
            axis=0,
        )
        r, k = r_ref[:, at[group]].astype(F32), k_ref[:, held[group]].astype(F32)
        diagonal_high, diagonal_low = split(r * bonus_row(bonus_ref, side, group, groups) * k)
        diagonal = dot(diagonal_high, ones) + dot(diagonal_low, ones)
        mixes.append(mixed + diagonal * v.astype(F32))
    for group in span:
        m_high, m_low = split(mixes[group])
        out_ref[0, :, out[group]] = mixes[group] - (dot(m_high, share) + dot(m_low, share))


def finish_kernel(
    shrink, p0, p1, p2, p3, ends_mine, ends_other, in_mine, in_other, gain_ref, bias_ref, out_ref,
    state_ref, buf, sems,
):
    core = lax.axis_index("head")
    place = lax.axis_index("seq") % PLANE
    groups = ends_mine.shape[0]
    length = in_mine.shape[1]
    first = core == 0
    share = same_head(1.0 / CHANNELS)
    masks = half_masks(CHANNELS)
    for step, piece in enumerate((p0, p1, p2, p3)):
        source = lax.bitwise_xor(place, step) * ROWS
        for group in range(groups):
            at = pl.multiple_of(source + group * CHANNELS, ROWS)
            if step:
                state, _ = get_wire(piece, shrink, group)
            else:
                state = piece[group * ROWS : (group + 1) * ROWS, :]
            state_ref[pl.ds(at, ROWS), :] = state
    states = {}
    for group in range(groups):
        early = jnp.where(first, ends_mine[group], ends_other[group])
        near = state_ref[group * CHANNELS : (group + 1) * CHANNELS, :]
        far = jnp.exp(early[CHANNELS : CHANNELS + 1]) * near + early[:CHANNELS]
        near = split(near - jnp.mean(near, axis=0, keepdims=True))
        far = split(far - jnp.mean(far, axis=0, keepdims=True))
        for side in range(2):
            pick = first if side == 0 else jnp.logical_not(first)
            states[side, group] = [
                spread_heads(jnp.where(pick, one, two), masks) for one, two in zip(near, far)
            ]
    copies = []
    for side, local in enumerate((in_mine, in_other)):
        mixes, spreads = {}, {}
        for group in range(groups):
            out = pl.ds(group * LANES, LANES)
            s_high, s_low = states[side, group]
            r_high, r_low = split(local[1, :, out])
            mixes[group] = local[0, :, out] + (
                dot_nt(r_high, s_high) + dot_nt(r_low, s_high) + dot_nt(r_high, s_low)
            )
        for group in range(groups):
            q_high, q_low = split(mixes[group] * mixes[group])
            spreads[group] = dot(q_high, share) + dot(q_low, share)
        for group in range(groups):
            gain, bias = tile_row(gain_ref, group, groups), tile_row(bias_ref, group, groups)
            out = pl.ds(group * LANES, LANES)
            normed = mixes[group] * lax.rsqrt(spreads[group] + 1e-5)
            gated = (normed * gain + bias) * local[2, :, out]
            buf[side, :, out] = gated.astype(BF16)
        rows = pl.ds(pl.multiple_of((core if side == 0 else 1 - core) * length, length), length)
        copies.append(pltpu.make_async_copy(buf.at[side], out_ref.at[rows, :], sems.at[side]))
        copies[-1].start()
    for copy in copies:
        copy.wait()


def program(r, k, v, w, gate, bonus, gain, bias):
    length, width = r.shape
    cores, count = lax.axis_size("head"), lax.axis_size("seq")
    planes = count // PLANE
    assert cores == 2 and count == planes * PLANE
    assert planes > 1 and planes & (planes - 1) == 0
    half = width // cores
    groups = half // LANES
    swap = [(0, 1), (1, 0)]
    hbm = pl.BlockSpec(memory_space=pltpu.HBM)
    gain, bias = gain.reshape(-1, TILE), bias.reshape(-1, TILE)

    def call(kernel, outs, **options):
        return pl.pallas_call(
            kernel,
            out_shape=outs,
            compiler_params=pltpu.CompilerParams(vmem_limit_bytes=VMEM_LIMIT),
            **options,
        )

    ends_shape = jax.ShapeDtypeStruct((groups, CHANNELS + 8, LANES), F32)
    packed_rows = -(-groups * (ROWS + 1) // 8) * 8
    packed = jax.ShapeDtypeStruct((packed_rows, LANES), F32)
    wire = jax.ShapeDtypeStruct((wire_rows(groups), LANES), F32)
    piece = jax.ShapeDtypeStruct((groups * ROWS, LANES), F32)
    shrink = 1.0
    while STATE_STEP * length * cores * count * shrink > 2.0**15:
        shrink *= 0.5

    held = pltpu.VMEM((length, width), BF16)
    mine, theirs, k, v, w, r, gate = call(
        ends_kernel,
        [pltpu.VMEM(ends_shape.shape, F32)] * 2 + [held] * 5,
        in_specs=[hbm] * 5,
        scratch_shapes=[pltpu.SemaphoreType.DMA((cores, 3)), pltpu.SemaphoreType.DMA((2,))],
    )(*(pltpu.with_memory_space_constraint(x, pltpu.HBM) for x in (k, v, w, r, gate)))
    other = lax.ppermute(theirs, "head", swap)

    def within(side):
        return call(
            functools.partial(within_kernel, side), jax.ShapeDtypeStruct((3, length, half), F32)
        )(r, k, v, w, gate, bonus)

    def over_seq(value, flip):
        pairs = [(i, i ^ flip) for i in range(count)]
        return lax.ppermute(value.astype(jnp.float16), "seq", pairs).astype(F32)

    def to_places(pieces):
        return [pieces[0]] + [over_seq(pieces[step], step) for step in range(1, PLANE)]

    def across(value, bit, step):
        return over_seq(value, step * bit * PLANE)

    quarters = call(
        functools.partial(combine_kernel, shrink),
        [packed] + [wire] * (PLANE - 1),
        scratch_shapes=[pltpu.VMEM((groups, CHANNELS, LANES), F32)],
    )(mine, other)
    in_other = lax.ppermute(within(1), "head", swap)
    total, sent, prefix = call(
        functools.partial(plane_kernel, groups, shrink),
        [packed, wire, jax.ShapeDtypeStruct((PLANE,) + packed.shape, F32)],
        scratch_shapes=[pltpu.VMEM((PLANE,) + packed.shape, F32)],
    )(*to_places(quarters))
    in_mine = within(0)
    before, bit = total, 1
    while True:
        radix = min(4, planes // bit)
        last = bit * radix == planes
        slabs = [pltpu.VMEM((radix,) + packed.shape, F32)]
        options = (groups, shrink, bit, radix, bit == 1)
        got = [across(sent, bit, step) for step in range(1, radix)]
        if last:
            break
        total, sent, before = call(
            functools.partial(round_kernel, *options), [packed, wire, packed], scratch_shapes=slabs
        )(total, before, *got)
        bit *= radix
    states = call(
        functools.partial(back_kernel, *options),
        [piece] + [wire] * (PLANE - 1),
        scratch_shapes=slabs,
    )(prefix, total, before, *got)
    return call(
        functools.partial(finish_kernel, shrink),
        jax.ShapeDtypeStruct((cores * length, half), BF16),
        out_specs=hbm,
        scratch_shapes=[
            pltpu.VMEM((groups * CHANNELS, LANES), F32),
            pltpu.VMEM((cores, length, half), BF16),
            pltpu.SemaphoreType.DMA((cores,)),
        ],
    )(*to_places(states), mine, other, in_mine, in_other, gain, bias)


def solution(mesh):
    tokens = P(("seq", "head"), None)
    return jax.shard_map(
        program,
        mesh=mesh,
        in_specs=(tokens,) * 5 + (P(), P(), P()),
        out_specs=P("seq", "head"),
        check_vma=False,
    )
```

```python
import functools

import jax
import jax.numpy as jnp
from jax import lax
from jax.experimental import pallas as pl
from jax.experimental.pallas import tpu as pltpu
from jax.sharding import PartitionSpec as P


CHANNELS = 64
TILE = 128
LANES = 256
HEADS = LANES // CHANNELS
BLOCK = 64
PLANE = 4
ROWS = CHANNELS // PLANE
STATE_STEP = 0.75 * 6.0
SCALE_FLOOR = 2.0**-10
CODE_SPAN = 29.5
CODE_LOW = 14.0
VMEM_LIMIT = 12 * 2**20
F32 = jnp.float32
BF16 = jnp.bfloat16


def split(value):
    high = value.astype(BF16)
    return high, (value - high.astype(F32)).astype(BF16)


def dot(left, right):
    return lax.dot_general(left, right, (((1,), (0,)), ((), ())), preferred_element_type=F32)


def dot_nt(left, right):
    return lax.dot_general(left, right, (((1,), (1,)), ((), ())), preferred_element_type=F32)


def same_head(value):
    rows = lax.broadcasted_iota(jnp.int32, (LANES, LANES), 0) // CHANNELS
    columns = lax.broadcasted_iota(jnp.int32, (LANES, LANES), 1) // CHANNELS
    return jnp.where(rows == columns, F32(value), F32(0.0)).astype(BF16)


def half_masks(rows):
    left = lax.broadcasted_iota(jnp.int32, (rows, TILE), 1) < CHANNELS
    one, zero = F32(1.0), F32(0.0)
    return jnp.where(left, one, zero).astype(BF16), jnp.where(left, zero, one).astype(BF16)


def spread_heads(value, masks):
    zero = jnp.zeros((value.shape[0], TILE), value.dtype)
    pieces = []
    for head in range(HEADS):
        tile = head // 2
        kept = value[:, tile * TILE : (tile + 1) * TILE] * masks[head % 2]
        pieces.append(
            jnp.concatenate([kept if i == tile else zero for i in range(LANES // TILE)], axis=1)
        )
    return jnp.concatenate(pieces, axis=0)


def own_blocks(stacked, rows):
    left = lax.broadcasted_iota(jnp.int32, (rows, TILE), 1) < CHANNELS
    pieces = []
    for tile in range(LANES // TILE):
        part = stacked[:, tile * TILE : (tile + 1) * TILE]
        head = 2 * tile
        pieces.append(
            jnp.where(
                left,
                part[head * rows : (head + 1) * rows],
                part[(head + 1) * rows : (head + 2) * rows],
            )
        )
    return jnp.concatenate(pieces, axis=1)


def cumulate(decay):
    length = decay.shape[0]
    rows = lax.broadcasted_iota(jnp.int32, (length, length), 0)
    columns = lax.broadcasted_iota(jnp.int32, (length, length), 1)
    lower = jnp.where(rows >= columns, F32(1.0), F32(0.0)).astype(BF16)
    return dot(lower, decay)


def lanes_at(side, group, groups):
    core = lax.axis_index("head")
    core = core if side == 0 else 1 - core
    return pl.ds(pl.multiple_of((core * groups + group) * LANES, LANES), LANES)


def bonus_row(ref, side, group, groups):
    core = lax.axis_index("head")
    core = core if side == 0 else 1 - core
    first = (core * groups + group) * HEADS
    return jnp.concatenate([ref[pl.ds(first + head, 1), :] for head in range(HEADS)], axis=1)


def tile_row(ref, group, groups):
    tiles = LANES // TILE
    first = (lax.axis_index("head") * groups + group) * tiles
    return jnp.concatenate([ref[pl.ds(first + tile, 1), :] for tile in range(tiles)], axis=1)


def half_at(side, half):
    core = lax.axis_index("head")
    core = core if side == 0 else 1 - core
    return pl.ds(pl.multiple_of(core * half, LANES), half)


def ends_of(side, k_ref, v_ref, w_ref, out_ref):
    span = range(out_ref.shape[0])
    at = [pl.ds((side * len(span) + group) * LANES, LANES) for group in span]
    cumuls = [cumulate(w_ref[:, at[group]]) for group in span]
    turned = [v_ref[:, at[group]].astype(F32).T.astype(BF16) for group in span]
    weighted = []
    for group in span:
        final = cumuls[group][-1:]
        out_ref[group, CHANNELS:, :] = jnp.broadcast_to(final, (8, LANES))
        weighted.append(split(k_ref[:, at[group]].astype(F32) * jnp.exp(final - cumuls[group])))
    for group in span:
        wide = dot(
            jnp.concatenate([turned[group]] * 2, axis=1),
            jnp.concatenate(weighted[group], axis=0),
        )
        out_ref[group, :CHANNELS, :] = own_blocks(wide, CHANNELS)


def load_kernel(
    k_ref, v_ref, w_ref, r_ref, g_ref, theirs_ref, k_buf, v_buf, w_buf, r_buf, g_buf,
    sems, late_sems,
):
    half = theirs_ref.shape[0] * LANES
    copies = {}
    for side in (1, 0):
        at = half_at(side, half)
        for index, (ref, buf) in enumerate(((w_ref, w_buf), (k_ref, k_buf), (v_ref, v_buf))):
            copies[side, index] = pltpu.make_async_copy(
                ref.at[:, at], buf.at[:, pl.ds(side * half, half)], sems.at[side, index]
            )
            copies[side, index].start()
    for index, (ref, buf) in enumerate(((r_ref, r_buf), (g_ref, g_buf))):
        copies[2, index] = pltpu.make_async_copy(ref, buf, late_sems.at[index])
        copies[2, index].start()
    for index in range(3):
        copies[1, index].wait()
    ends_of(1, k_buf, v_buf, w_buf, theirs_ref)
    for (side, _), copy in copies.items():
        if side != 1:
            copy.wait()


def ends_kernel(k_ref, v_ref, w_ref, mine_ref):
    ends_of(0, k_ref, v_ref, w_ref, mine_ref)


def log_row(groups, group):
    return slice(groups * ROWS + group, groups * ROWS + group + 1)


def wire_rows(groups):
    return -(-groups * (ROWS + 3) // 16) * 16


def put_wire(ref, shrink, group, state, log=None):
    groups = ref.shape[0] // (ROWS + 3)
    top = jnp.max(jnp.abs(state), axis=0, keepdims=True)
    scale = (top * 1.01 + SCALE_FLOOR).astype(BF16).astype(F32)
    code = jnp.exp2(jnp.abs(state) * (CODE_SPAN / scale) - CODE_LOW)
    ref[group * ROWS : (group + 1) * ROWS, :] = jnp.where(state < 0.0, -code, code)
    row = groups * ROWS + group
    ref[row : row + 1, :] = scale * F32(shrink)
    high = jnp.zeros((1, LANES), F32) if log is None else log.astype(BF16).astype(F32)
    ref[row + groups : row + groups + 1, :] = high
    low = high if log is None else log - high
    ref[row + 2 * groups : row + 2 * groups + 1, :] = low


def clear_rest(ref):
    groups = ref.shape[0] // (ROWS + 3)
    rest = ref.shape[0] - groups * (ROWS + 3)
    if rest:
        ref[groups * (ROWS + 3) :, :] = jnp.zeros((rest, LANES), F32)


def get_wire(ref, shrink, group):
    groups = ref.shape[0] // (ROWS + 3)
    row = groups * ROWS + group
    scale = ref[row : row + 1, :] * F32(1.0 / (shrink * CODE_SPAN))
    code = ref[group * ROWS : (group + 1) * ROWS, :]
    size = (jnp.log2(jnp.abs(code)) + CODE_LOW) * scale
    log = ref[row + groups : row + groups + 1, :] + ref[row + 2 * groups : row + 2 * groups + 1, :]
    return jnp.where(code < 0.0, -size, size), log


def combine_kernel(shrink, mine_ref, other_ref, q0, q1, q2, q3, state_ref):
    core = lax.axis_index("head")
    place = lax.axis_index("seq") % PLANE
    groups = mine_ref.shape[0]
    first = core == 0
    for out in (q1, q2, q3):
        clear_rest(out)
    for group in range(groups):
        mine, other = mine_ref[group], other_ref[group]
        early, late = jnp.where(first, mine, other), jnp.where(first, other, mine)
        late_log = late[CHANNELS : CHANNELS + 1]
        state_ref[group] = early[:CHANNELS] * jnp.exp(late_log) + late[:CHANNELS]
        both = early[CHANNELS : CHANNELS + 1] + late_log
        for step, out in enumerate((q0, q1, q2, q3)):
            at = pl.multiple_of(lax.bitwise_xor(place, step) * ROWS, ROWS)
            state = state_ref[group, pl.ds(at, ROWS), :]
            if step:
                put_wire(out, shrink, group, state, both)
            else:
                out[group * ROWS : (group + 1) * ROWS, :] = state
                out[log_row(groups, group), :] = both


def plane_kernel(groups, shrink, q0, q1, q2, q3, total_ref, wire_ref, prefix_ref, slab_ref):
    place = lax.axis_index("seq") % PLANE
    clear_rest(wire_ref)
    for group in range(groups):
        rows = slice(group * ROWS, (group + 1) * ROWS)
        row = log_row(groups, group)
        slab_ref[place, rows, :] = q0[rows, :]
        slab_ref[place, row, :] = q0[row, :]
        for step, piece in ((1, q1), (2, q2), (3, q3)):
            to = lax.bitwise_xor(place, step)
            state, log = get_wire(piece, shrink, group)
            slab_ref[to, rows, :] = state
            slab_ref[to, row, :] = log
    for group in range(groups):
        rows = slice(group * ROWS, (group + 1) * ROWS)
        row = log_row(groups, group)
        state = jnp.zeros((ROWS, LANES), F32)
        log = jnp.zeros((1, LANES), F32)
        for slab in range(PLANE):
            prefix_ref[slab, rows, :] = state
            prefix_ref[slab, row, :] = jnp.exp(log)
            step = slab_ref[slab, row, :]
            state = jnp.exp(step) * state + slab_ref[slab, rows, :]
            log = log + step
        total_ref[rows, :] = state
        total_ref[row, :] = log
        put_wire(wire_ref, shrink, group, state, log)


def group_prefix(groups, shrink, bit, radix, total_ref, got_refs, slab_ref):
    mine = lax.axis_index("seq") // PLANE // bit % radix
    for group in range(groups):
        rows = slice(group * ROWS, (group + 1) * ROWS)
        row = log_row(groups, group)
        slab_ref[mine, rows, :] = total_ref[rows, :]
        slab_ref[mine, row, :] = total_ref[row, :]
        for step, got in enumerate(got_refs, 1):
            to = lax.bitwise_xor(mine, step)
            state, log = get_wire(got, shrink, group)
            slab_ref[to, rows, :] = state
            slab_ref[to, row, :] = log
    found = []
    for group in range(groups):
        rows = slice(group * ROWS, (group + 1) * ROWS)
        row = log_row(groups, group)
        state, log = jnp.zeros((ROWS, LANES), F32), jnp.zeros((1, LANES), F32)
        before, before_log = state, log
        for slab in range(radix):
            step = slab_ref[slab, row, :]
            state = jnp.exp(step) * state + slab_ref[slab, rows, :]
            log = log + step
            before = jnp.where(slab < mine, state, before)
            before_log = jnp.where(slab < mine, log, before_log)
        found.append((before, before_log, state, log))
    return found


def round_kernel(groups, shrink, bit, radix, first, *refs):
    total_ref, before_ref, *got_refs = refs[: 2 + radix - 1]
    total_out, wire_out, before_out, slab_ref = refs[2 + radix - 1 :]
    clear_rest(wire_out)
    found = group_prefix(groups, shrink, bit, radix, total_ref, got_refs, slab_ref)
    for group, (state, log, total, total_log) in enumerate(found):
        rows = slice(group * ROWS, (group + 1) * ROWS)
        row = log_row(groups, group)
        if not first:
            state = jnp.exp(before_ref[row, :]) * state + before_ref[rows, :]
            log = log + before_ref[row, :]
        before_out[rows, :] = state
        before_out[row, :] = log
        total_out[rows, :] = total
        total_out[row, :] = total_log
        put_wire(wire_out, shrink, group, total, total_log)


def back_kernel(groups, shrink, bit, radix, first, *refs):
    prefix_ref, total_ref, before_ref, *got_refs = refs[: 3 + radix - 1]
    *outs, slab_ref = refs[3 + radix - 1 :]
    place = lax.axis_index("seq") % PLANE
    for out in outs[1:]:
        clear_rest(out)
    found = group_prefix(groups, shrink, bit, radix, total_ref, got_refs, slab_ref)
    for group, (before, _, _, _) in enumerate(found):
        rows = slice(group * ROWS, (group + 1) * ROWS)
        row = log_row(groups, group)
        if not first:
            before = jnp.exp(before_ref[row, :]) * before + before_ref[rows, :]
        for step, out in enumerate(outs):
            to = lax.bitwise_xor(place, step)
            state = prefix_ref[to, row, :] * before + prefix_ref[to, rows, :]
            if step:
                put_wire(out, shrink, group, state)
            else:
                out[rows, :] = state


def within_kernel(side, r_ref, k_ref, v_ref, w_ref, g_ref, bonus_ref, out_ref):
    groups = out_ref.shape[2] // LANES
    length = w_ref.shape[0]
    ones = same_head(1.0)
    share = same_head(1.0 / CHANNELS)
    masks = half_masks(BLOCK)
    shape = (HEADS * length, length)
    row = lax.broadcasted_iota(jnp.int32, shape, 0)
    later = row // (HEADS * BLOCK) * BLOCK + row % BLOCK
    strict = later > lax.broadcasted_iota(jnp.int32, shape, 1)
    span = range(groups)
    at = [lanes_at(side, group, groups) for group in span]
    out = [pl.ds(group * LANES, LANES) for group in span]
    held = [pl.ds((side * groups + group) * LANES, LANES) for group in span]
    cumuls = [cumulate(w_ref[:, held[group]]) for group in span]
    for group in span:
        gate = g_ref[:, at[group]].astype(F32)
        out_ref[2, :, out[group]] = gate / (1.0 + jnp.exp(-gate))
    scores = []
    for group in span:
        r, k = r_ref[:, at[group]].astype(F32), k_ref[:, held[group]].astype(F32)
        cumul = cumuls[group]
        before = cumul - w_ref[:, held[group]].astype(F32)
        out_ref[1, :, out[group]] = r * jnp.exp(before)
        pieces = []
        for start in range(0, length, BLOCK):
            stop = start + BLOCK
            middle = start + BLOCK // 2 - 1
            reference = cumul[middle : middle + 1]
            r_high, r_low = split(r[start:stop] * jnp.exp(before[start:stop] - reference))
            k_high, k_low = split(k[:stop] * jnp.exp(reference - cumul[:stop]))
            if stop < length:
                rest = jnp.zeros((length - stop, LANES), BF16)
                k_high = jnp.concatenate([k_high, rest], axis=0)
                k_low = jnp.concatenate([k_low, rest], axis=0)
            r_high, r_low = spread_heads(r_high, masks), spread_heads(r_low, masks)
            pieces.append(dot_nt(r_high, k_high) + dot_nt(r_low, k_high) + dot_nt(r_high, k_low))
        scores.append(split(jnp.where(strict, jnp.concatenate(pieces, axis=0), F32(0.0))))
    mixes = []
    for group in span:
        v = v_ref[:, held[group]]
        wide = dot(jnp.concatenate(scores[group], axis=1), jnp.concatenate([v, v], axis=0))
        step = HEADS * BLOCK
        mixed = jnp.concatenate(
            [own_blocks(wide[i * step : (i + 1) * step], BLOCK) for i in range(length // BLOCK)],
            axis=0,
        )
        r, k = r_ref[:, at[group]].astype(F32), k_ref[:, held[group]].astype(F32)
        diagonal_high, diagonal_low = split(r * bonus_row(bonus_ref, side, group, groups) * k)
        diagonal = dot(diagonal_high, ones) + dot(diagonal_low, ones)
        mixes.append(mixed + diagonal * v.astype(F32))
    for group in span:
        m_high, m_low = split(mixes[group])
        out_ref[0, :, out[group]] = mixes[group] - (dot(m_high, share) + dot(m_low, share))


def finish_kernel(
    shrink, p0, p1, p2, p3, ends_mine, ends_other, in_mine, in_other, gain_ref, bias_ref, out_ref,
    state_ref, buf, sems,
):
    core = lax.axis_index("head")
    place = lax.axis_index("seq") % PLANE
    groups = ends_mine.shape[0]
    length = in_mine.shape[1]
    first = core == 0
    share = same_head(1.0 / CHANNELS)
    masks = half_masks(CHANNELS)
    for step, piece in enumerate((p0, p1, p2, p3)):
        source = lax.bitwise_xor(place, step) * ROWS
        for group in range(groups):
            at = pl.multiple_of(source + group * CHANNELS, ROWS)
            if step:
                state, _ = get_wire(piece, shrink, group)
            else:
                state = piece[group * ROWS : (group + 1) * ROWS, :]
            state_ref[pl.ds(at, ROWS), :] = state
    states = {}
    for group in range(groups):
        early = jnp.where(first, ends_mine[group], ends_other[group])
        near = state_ref[group * CHANNELS : (group + 1) * CHANNELS, :]
        far = jnp.exp(early[CHANNELS : CHANNELS + 1]) * near + early[:CHANNELS]
        near = split(near - jnp.mean(near, axis=0, keepdims=True))
        far = split(far - jnp.mean(far, axis=0, keepdims=True))
        for side in range(2):
            pick = first if side == 0 else jnp.logical_not(first)
            states[side, group] = [
                spread_heads(jnp.where(pick, one, two), masks) for one, two in zip(near, far)
            ]
    copies = []
    for side, local in enumerate((in_mine, in_other)):
        mixes, spreads = {}, {}
        for group in range(groups):
            out = pl.ds(group * LANES, LANES)
            s_high, s_low = states[side, group]
            r_high, r_low = split(local[1, :, out])
            mixes[group] = local[0, :, out] + (
                dot_nt(r_high, s_high) + dot_nt(r_low, s_high) + dot_nt(r_high, s_low)
            )
        for group in range(groups):
            q_high, q_low = split(mixes[group] * mixes[group])
            spreads[group] = dot(q_high, share) + dot(q_low, share)
        for group in range(groups):
            gain, bias = tile_row(gain_ref, group, groups), tile_row(bias_ref, group, groups)
            out = pl.ds(group * LANES, LANES)
            normed = mixes[group] * lax.rsqrt(spreads[group] + 1e-5)
            gated = (normed * gain + bias) * local[2, :, out]
            buf[side, :, out] = gated.astype(BF16)
        rows = pl.ds(pl.multiple_of((core if side == 0 else 1 - core) * length, length), length)
        copies.append(pltpu.make_async_copy(buf.at[side], out_ref.at[rows, :], sems.at[side]))
        copies[-1].start()
    for copy in copies:
        copy.wait()


def program(r, k, v, w, gate, bonus, gain, bias):
    length, width = r.shape
    cores, count = lax.axis_size("head"), lax.axis_size("seq")
    planes = count // PLANE
    assert cores == 2 and count == planes * PLANE
    assert planes > 1 and planes & (planes - 1) == 0
    half = width // cores
    groups = half // LANES
    swap = [(0, 1), (1, 0)]
    hbm = pl.BlockSpec(memory_space=pltpu.HBM)
    gain, bias = gain.reshape(-1, TILE), bias.reshape(-1, TILE)

    def call(kernel, outs, **options):
        return pl.pallas_call(
            kernel,
            out_shape=outs,
            compiler_params=pltpu.CompilerParams(vmem_limit_bytes=VMEM_LIMIT),
            **options,
        )

    ends_shape = jax.ShapeDtypeStruct((groups, CHANNELS + 8, LANES), F32)
    packed_rows = -(-groups * (ROWS + 1) // 8) * 8
    packed = jax.ShapeDtypeStruct((packed_rows, LANES), F32)
    wire = jax.ShapeDtypeStruct((wire_rows(groups), LANES), F32)
    piece = jax.ShapeDtypeStruct((groups * ROWS, LANES), F32)
    shrink = 1.0
    while STATE_STEP * length * cores * count * shrink > 2.0**15:
        shrink *= 0.5

    held = pltpu.VMEM((length, width), BF16)
    theirs, k, v, w, r, gate = call(
        load_kernel,
        [pltpu.VMEM(ends_shape.shape, F32)] + [held] * 5,
        in_specs=[hbm] * 5,
        scratch_shapes=[pltpu.SemaphoreType.DMA((cores, 3)), pltpu.SemaphoreType.DMA((2,))],
    )(*(pltpu.with_memory_space_constraint(x, pltpu.HBM) for x in (k, v, w, r, gate)))
    other = lax.ppermute(theirs, "head", swap)
    mine = call(ends_kernel, ends_shape)(k, v, w)

    def within(side):
        return call(
            functools.partial(within_kernel, side), jax.ShapeDtypeStruct((3, length, half), F32)
        )(r, k, v, w, gate, bonus)

    def over_seq(value, flip):
        pairs = [(i, i ^ flip) for i in range(count)]
        return lax.ppermute(value.astype(jnp.float16), "seq", pairs).astype(F32)

    def to_places(pieces):
        return [pieces[0]] + [over_seq(pieces[step], step) for step in range(1, PLANE)]

    def across(value, bit, step):
        return over_seq(value, step * bit * PLANE)

    quarters = call(
        functools.partial(combine_kernel, shrink),
        [packed] + [wire] * (PLANE - 1),
        scratch_shapes=[pltpu.VMEM((groups, CHANNELS, LANES), F32)],
    )(mine, other)
    in_other = lax.ppermute(within(1), "head", swap)
    total, sent, prefix = call(
        functools.partial(plane_kernel, groups, shrink),
        [packed, wire, jax.ShapeDtypeStruct((PLANE,) + packed.shape, F32)],
        scratch_shapes=[pltpu.VMEM((PLANE,) + packed.shape, F32)],
    )(*to_places(quarters))
    in_mine = within(0)
    before, bit = total, 1
    while True:
        radix = min(4, planes // bit)
        last = bit * radix == planes
        slabs = [pltpu.VMEM((radix,) + packed.shape, F32)]
        options = (groups, shrink, bit, radix, bit == 1)
        got = [across(sent, bit, step) for step in range(1, radix)]
        if last:
            break
        total, sent, before = call(
            functools.partial(round_kernel, *options), [packed, wire, packed], scratch_shapes=slabs
        )(total, before, *got)
        bit *= radix
    states = call(
        functools.partial(back_kernel, *options),
        [piece] + [wire] * (PLANE - 1),
        scratch_shapes=slabs,
    )(prefix, total, before, *got)
    return call(
        functools.partial(finish_kernel, shrink),
        jax.ShapeDtypeStruct((cores * length, half), BF16),
        out_specs=hbm,
        scratch_shapes=[
            pltpu.VMEM((groups * CHANNELS, LANES), F32),
            pltpu.VMEM((cores, length, half), BF16),
            pltpu.SemaphoreType.DMA((cores,)),
        ],
    )(*to_places(states), mine, other, in_mine, in_other, gain, bias)


def solution(mesh):
    tokens = P(("seq", "head"), None)
    return jax.shard_map(
        program,
        mesh=mesh,
        in_specs=(tokens,) * 5 + (P(), P(), P()),
        out_specs=P("seq", "head"),
        check_vma=False,
    )
```

```python
import functools

import jax
import jax.numpy as jnp
from jax import lax
from jax.experimental import pallas as pl
from jax.experimental.pallas import tpu as pltpu
from jax.sharding import PartitionSpec as P


CHANNELS = 64
TILE = 128
LANES = 256
HEADS = LANES // CHANNELS
BLOCK = 64
PLANE = 4
ROWS = CHANNELS // PLANE
STATE_STEP = 0.75 * 6.0
SCALE_FLOOR = 2.0**-10
CODE_SPAN = 29.5
CODE_LOW = 14.0
VMEM_LIMIT = 12 * 2**20
F32 = jnp.float32
BF16 = jnp.bfloat16


def split(value):
    high = value.astype(BF16)
    return high, (value - high.astype(F32)).astype(BF16)


def dot(left, right):
    return lax.dot_general(left, right, (((1,), (0,)), ((), ())), preferred_element_type=F32)


def dot_nt(left, right):
    return lax.dot_general(left, right, (((1,), (1,)), ((), ())), preferred_element_type=F32)


def same_head(value):
    rows = lax.broadcasted_iota(jnp.int32, (LANES, LANES), 0) // CHANNELS
    columns = lax.broadcasted_iota(jnp.int32, (LANES, LANES), 1) // CHANNELS
    return jnp.where(rows == columns, F32(value), F32(0.0)).astype(BF16)


def half_masks(rows):
    left = lax.broadcasted_iota(jnp.int32, (rows, TILE), 1) < CHANNELS
    one, zero = F32(1.0), F32(0.0)
    return jnp.where(left, one, zero).astype(BF16), jnp.where(left, zero, one).astype(BF16)


def spread_heads(value, masks):
    zero = jnp.zeros((value.shape[0], TILE), value.dtype)
    pieces = []
    for head in range(HEADS):
        tile = head // 2
        kept = value[:, tile * TILE : (tile + 1) * TILE] * masks[head % 2]
        pieces.append(
            jnp.concatenate([kept if i == tile else zero for i in range(LANES // TILE)], axis=1)
        )
    return jnp.concatenate(pieces, axis=0)


def own_blocks(stacked, rows):
    left = lax.broadcasted_iota(jnp.int32, (rows, TILE), 1) < CHANNELS
    pieces = []
    for tile in range(LANES // TILE):
        part = stacked[:, tile * TILE : (tile + 1) * TILE]
        head = 2 * tile
        pieces.append(
            jnp.where(
                left,
                part[head * rows : (head + 1) * rows],
                part[(head + 1) * rows : (head + 2) * rows],
            )
        )
    return jnp.concatenate(pieces, axis=1)


def cumulate(decay):
    length = decay.shape[0]
    rows = lax.broadcasted_iota(jnp.int32, (length, length), 0)
    columns = lax.broadcasted_iota(jnp.int32, (length, length), 1)
    lower = jnp.where(rows >= columns, F32(1.0), F32(0.0)).astype(BF16)
    return dot(lower, decay)


def lanes_at(side, group, groups):
    core = lax.axis_index("head")
    core = core if side == 0 else 1 - core
    return pl.ds(pl.multiple_of((core * groups + group) * LANES, LANES), LANES)


def bonus_row(ref, side, group, groups):
    core = lax.axis_index("head")
    core = core if side == 0 else 1 - core
    first = (core * groups + group) * HEADS
    return jnp.concatenate([ref[pl.ds(first + head, 1), :] for head in range(HEADS)], axis=1)


def tile_row(ref, group, groups):
    tiles = LANES // TILE
    first = (lax.axis_index("head") * groups + group) * tiles
    return jnp.concatenate([ref[pl.ds(first + tile, 1), :] for tile in range(tiles)], axis=1)


def half_at(side, half):
    core = lax.axis_index("head")
    core = core if side == 0 else 1 - core
    return pl.ds(pl.multiple_of(core * half, LANES), half)


def ends_of(side, k_ref, v_ref, w_ref, out_ref):
    span = range(out_ref.shape[0])
    at = [pl.ds((side * len(span) + group) * LANES, LANES) for group in span]
    cumuls = [cumulate(w_ref[:, at[group]]) for group in span]
    turned = [v_ref[:, at[group]].astype(F32).T.astype(BF16) for group in span]
    weighted = []
    for group in span:
        final = cumuls[group][-1:]
        out_ref[group, CHANNELS:, :] = jnp.broadcast_to(final, (8, LANES))
        weighted.append(split(k_ref[:, at[group]].astype(F32) * jnp.exp(final - cumuls[group])))
    for group in span:
        wide = dot(
            jnp.concatenate([turned[group]] * 2, axis=1),
            jnp.concatenate(weighted[group], axis=0),
        )
        out_ref[group, :CHANNELS, :] = own_blocks(wide, CHANNELS)


def load_kernel(k_ref, v_ref, w_ref, theirs_ref, k_buf, v_buf, w_buf, sems):
    half = theirs_ref.shape[0] * LANES
    copies = {}
    for side in (1, 0):
        at = half_at(side, half)
        for index, (ref, buf) in enumerate(((w_ref, w_buf), (k_ref, k_buf), (v_ref, v_buf))):
            copies[side, index] = pltpu.make_async_copy(
                ref.at[:, at], buf.at[:, pl.ds(side * half, half)], sems.at[side, index]
            )
            copies[side, index].start()
    for index in range(3):
        copies[1, index].wait()
    ends_of(1, k_buf, v_buf, w_buf, theirs_ref)
    for index in range(3):
        copies[0, index].wait()


def ends_kernel(k_ref, v_ref, w_ref, r_ref, g_ref, mine_ref, r_buf, g_buf, sems):
    copies = []
    for index, (ref, buf) in enumerate(((r_ref, r_buf), (g_ref, g_buf))):
        copies.append(pltpu.make_async_copy(ref, buf, sems.at[index]))
        copies[-1].start()
    ends_of(0, k_ref, v_ref, w_ref, mine_ref)
    for copy in copies:
        copy.wait()


def log_row(groups, group):
    return slice(groups * ROWS + group, groups * ROWS + group + 1)


def wire_rows(groups):
    return -(-groups * (ROWS + 3) // 16) * 16


def put_wire(ref, shrink, group, state, log=None):
    groups = ref.shape[0] // (ROWS + 3)
    top = jnp.max(jnp.abs(state), axis=0, keepdims=True)
    scale = (top * 1.01 + SCALE_FLOOR).astype(BF16).astype(F32)
    code = jnp.exp2(jnp.abs(state) * (CODE_SPAN / scale) - CODE_LOW)
    ref[group * ROWS : (group + 1) * ROWS, :] = jnp.where(state < 0.0, -code, code)
    row = groups * ROWS + group
    ref[row : row + 1, :] = scale * F32(shrink)
    high = jnp.zeros((1, LANES), F32) if log is None else log.astype(BF16).astype(F32)
    ref[row + groups : row + groups + 1, :] = high
    low = high if log is None else log - high
    ref[row + 2 * groups : row + 2 * groups + 1, :] = low


def clear_rest(ref):
    groups = ref.shape[0] // (ROWS + 3)
    rest = ref.shape[0] - groups * (ROWS + 3)
    if rest:
        ref[groups * (ROWS + 3) :, :] = jnp.zeros((rest, LANES), F32)


def get_wire(ref, shrink, group):
    groups = ref.shape[0] // (ROWS + 3)
    row = groups * ROWS + group
    scale = ref[row : row + 1, :] * F32(1.0 / (shrink * CODE_SPAN))
    code = ref[group * ROWS : (group + 1) * ROWS, :]
    size = (jnp.log2(jnp.abs(code)) + CODE_LOW) * scale
    log = ref[row + groups : row + groups + 1, :] + ref[row + 2 * groups : row + 2 * groups + 1, :]
    return jnp.where(code < 0.0, -size, size), log


def combine_kernel(shrink, mine_ref, other_ref, q0, q1, q2, q3, state_ref):
    core = lax.axis_index("head")
    place = lax.axis_index("seq") % PLANE
    groups = mine_ref.shape[0]
    first = core == 0
    for out in (q1, q2, q3):
        clear_rest(out)
    for group in range(groups):
        mine, other = mine_ref[group], other_ref[group]
        early, late = jnp.where(first, mine, other), jnp.where(first, other, mine)
        late_log = late[CHANNELS : CHANNELS + 1]
        state_ref[group] = early[:CHANNELS] * jnp.exp(late_log) + late[:CHANNELS]
        both = early[CHANNELS : CHANNELS + 1] + late_log
        for step, out in enumerate((q0, q1, q2, q3)):
            at = pl.multiple_of(lax.bitwise_xor(place, step) * ROWS, ROWS)
            state = state_ref[group, pl.ds(at, ROWS), :]
            if step:
                put_wire(out, shrink, group, state, both)
            else:
                out[group * ROWS : (group + 1) * ROWS, :] = state
                out[log_row(groups, group), :] = both


def plane_kernel(groups, shrink, q0, q1, q2, q3, total_ref, wire_ref, prefix_ref, slab_ref):
    place = lax.axis_index("seq") % PLANE
    clear_rest(wire_ref)
    for group in range(groups):
        rows = slice(group * ROWS, (group + 1) * ROWS)
        row = log_row(groups, group)
        slab_ref[place, rows, :] = q0[rows, :]
        slab_ref[place, row, :] = q0[row, :]
        for step, piece in ((1, q1), (2, q2), (3, q3)):
            to = lax.bitwise_xor(place, step)
            state, log = get_wire(piece, shrink, group)
            slab_ref[to, rows, :] = state
            slab_ref[to, row, :] = log
    for group in range(groups):
        rows = slice(group * ROWS, (group + 1) * ROWS)
        row = log_row(groups, group)
        state = jnp.zeros((ROWS, LANES), F32)
        log = jnp.zeros((1, LANES), F32)
        for slab in range(PLANE):
            prefix_ref[slab, rows, :] = state
            prefix_ref[slab, row, :] = jnp.exp(log)
            step = slab_ref[slab, row, :]
            state = jnp.exp(step) * state + slab_ref[slab, rows, :]
            log = log + step
        total_ref[rows, :] = state
        total_ref[row, :] = log
        put_wire(wire_ref, shrink, group, state, log)


def group_prefix(groups, shrink, bit, radix, total_ref, got_refs, slab_ref):
    mine = lax.axis_index("seq") // PLANE // bit % radix
    for group in range(groups):
        rows = slice(group * ROWS, (group + 1) * ROWS)
        row = log_row(groups, group)
        slab_ref[mine, rows, :] = total_ref[rows, :]
        slab_ref[mine, row, :] = total_ref[row, :]
        for step, got in enumerate(got_refs, 1):
            to = lax.bitwise_xor(mine, step)
            state, log = get_wire(got, shrink, group)
            slab_ref[to, rows, :] = state
            slab_ref[to, row, :] = log
    found = []
    for group in range(groups):
        rows = slice(group * ROWS, (group + 1) * ROWS)
        row = log_row(groups, group)
        state, log = jnp.zeros((ROWS, LANES), F32), jnp.zeros((1, LANES), F32)
        before, before_log = state, log
        for slab in range(radix):
            step = slab_ref[slab, row, :]
            state = jnp.exp(step) * state + slab_ref[slab, rows, :]
            log = log + step
            before = jnp.where(slab < mine, state, before)
            before_log = jnp.where(slab < mine, log, before_log)
        found.append((before, before_log, state, log))
    return found


def round_kernel(groups, shrink, bit, radix, first, *refs):
    total_ref, before_ref, *got_refs = refs[: 2 + radix - 1]
    total_out, wire_out, before_out, slab_ref = refs[2 + radix - 1 :]
    clear_rest(wire_out)
    found = group_prefix(groups, shrink, bit, radix, total_ref, got_refs, slab_ref)
    for group, (state, log, total, total_log) in enumerate(found):
        rows = slice(group * ROWS, (group + 1) * ROWS)
        row = log_row(groups, group)
        if not first:
            state = jnp.exp(before_ref[row, :]) * state + before_ref[rows, :]
            log = log + before_ref[row, :]
        before_out[rows, :] = state
        before_out[row, :] = log
        total_out[rows, :] = total
        total_out[row, :] = total_log
        put_wire(wire_out, shrink, group, total, total_log)


def back_kernel(groups, shrink, bit, radix, first, *refs):
    prefix_ref, total_ref, before_ref, *got_refs = refs[: 3 + radix - 1]
    *outs, slab_ref = refs[3 + radix - 1 :]
    place = lax.axis_index("seq") % PLANE
    for out in outs[1:]:
        clear_rest(out)
    found = group_prefix(groups, shrink, bit, radix, total_ref, got_refs, slab_ref)
    for group, (before, _, _, _) in enumerate(found):
        rows = slice(group * ROWS, (group + 1) * ROWS)
        row = log_row(groups, group)
        if not first:
            before = jnp.exp(before_ref[row, :]) * before + before_ref[rows, :]
        for step, out in enumerate(outs):
            to = lax.bitwise_xor(place, step)
            state = prefix_ref[to, row, :] * before + prefix_ref[to, rows, :]
            if step:
                put_wire(out, shrink, group, state)
            else:
                out[rows, :] = state


def within_kernel(side, r_ref, k_ref, v_ref, w_ref, g_ref, bonus_ref, out_ref):
    groups = out_ref.shape[2] // LANES
    length = w_ref.shape[0]
    ones = same_head(1.0)
    share = same_head(1.0 / CHANNELS)
    masks = half_masks(BLOCK)
    shape = (HEADS * length, length)
    row = lax.broadcasted_iota(jnp.int32, shape, 0)
    later = row // (HEADS * BLOCK) * BLOCK + row % BLOCK
    strict = later > lax.broadcasted_iota(jnp.int32, shape, 1)
    span = range(groups)
    at = [lanes_at(side, group, groups) for group in span]
    out = [pl.ds(group * LANES, LANES) for group in span]
    held = [pl.ds((side * groups + group) * LANES, LANES) for group in span]
    cumuls = [cumulate(w_ref[:, held[group]]) for group in span]
    for group in span:
        gate = g_ref[:, at[group]].astype(F32)
        out_ref[2, :, out[group]] = gate / (1.0 + jnp.exp(-gate))
    scores = []
    for group in span:
        r, k = r_ref[:, at[group]].astype(F32), k_ref[:, held[group]].astype(F32)
        cumul = cumuls[group]
        before = cumul - w_ref[:, held[group]].astype(F32)
        out_ref[1, :, out[group]] = r * jnp.exp(before)
        pieces = []
        for start in range(0, length, BLOCK):
            stop = start + BLOCK
            middle = start + BLOCK // 2 - 1
            reference = cumul[middle : middle + 1]
            r_high, r_low = split(r[start:stop] * jnp.exp(before[start:stop] - reference))
            k_high, k_low = split(k[:stop] * jnp.exp(reference - cumul[:stop]))
            if stop < length:
                rest = jnp.zeros((length - stop, LANES), BF16)
                k_high = jnp.concatenate([k_high, rest], axis=0)
                k_low = jnp.concatenate([k_low, rest], axis=0)
            r_high, r_low = spread_heads(r_high, masks), spread_heads(r_low, masks)
            pieces.append(dot_nt(r_high, k_high) + dot_nt(r_low, k_high) + dot_nt(r_high, k_low))
        scores.append(split(jnp.where(strict, jnp.concatenate(pieces, axis=0), F32(0.0))))
    mixes = []
    for group in span:
        v = v_ref[:, held[group]]
        wide = dot(jnp.concatenate(scores[group], axis=1), jnp.concatenate([v, v], axis=0))
        step = HEADS * BLOCK
        mixed = jnp.concatenate(
            [own_blocks(wide[i * step : (i + 1) * step], BLOCK) for i in range(length // BLOCK)],
            axis=0,
        )
        r, k = r_ref[:, at[group]].astype(F32), k_ref[:, held[group]].astype(F32)
        diagonal_high, diagonal_low = split(r * bonus_row(bonus_ref, side, group, groups) * k)
        diagonal = dot(diagonal_high, ones) + dot(diagonal_low, ones)
        mixes.append(mixed + diagonal * v.astype(F32))
    for group in span:
        m_high, m_low = split(mixes[group])
        out_ref[0, :, out[group]] = mixes[group] - (dot(m_high, share) + dot(m_low, share))


def prep_kernel(ends_mine, ends_other, in_mine, in_other, flow_ref, high_ref, low_ref):
    core = lax.axis_index("head")
    groups = ends_mine.shape[0]
    length = in_mine.shape[1]
    first = core == 0
    masks = half_masks(CHANNELS)
    for group in range(groups):
        out = pl.ds(group * LANES, LANES)
        early = jnp.where(first, ends_mine[group], ends_other[group])
        state = early[:CHANNELS]
        s_high, s_low = split(state - jnp.mean(state, axis=0, keepdims=True))
        s_high, s_low = spread_heads(s_high, masks), spread_heads(s_low, masks)
        near = [jnp.where(first, in_mine[i, :, out], in_other[i, :, out]) for i in range(3)]
        far = [jnp.where(first, in_other[i, :, out], in_mine[i, :, out]) for i in range(3)]
        r_high, r_low = split(far[1])
        flow_ref[0, :length, out] = near[0]
        flow_ref[0, length:, out] = far[0] + (
            dot_nt(r_high, s_high) + dot_nt(r_low, s_high) + dot_nt(r_high, s_low)
        )
        flow_ref[1, :length, out] = near[2]
        flow_ref[1, length:, out] = far[2]
        high_ref[:length, out], low_ref[:length, out] = split(near[1])
        decay = jnp.exp(early[CHANNELS : CHANNELS + 1])
        high_ref[length:, out], low_ref[length:, out] = split(far[1] * decay)


def finish_kernel(
    shrink, p0, p1, p2, p3, flow_ref, high_ref, low_ref, gain_ref, bias_ref, out_ref,
    state_ref, buf, sems,
):
    place = lax.axis_index("seq") % PLANE
    groups = p0.shape[0] // ROWS
    share = same_head(1.0 / CHANNELS)
    masks = half_masks(CHANNELS)
    for step, piece in enumerate((p0, p1, p2, p3)):
        source = lax.bitwise_xor(place, step) * ROWS
        for group in range(groups):
            at = pl.multiple_of(source + group * CHANNELS, ROWS)
            if step:
                state, _ = get_wire(piece, shrink, group)
            else:
                state = piece[group * ROWS : (group + 1) * ROWS, :]
            state_ref[pl.ds(at, ROWS), :] = state
    states = []
    for group in range(groups):
        state = state_ref[group * CHANNELS : (group + 1) * CHANNELS, :]
        pair = split(state - jnp.mean(state, axis=0, keepdims=True))
        states.append([spread_heads(part, masks) for part in pair])
    copies = []
    for part in (range(groups - groups // 2), range(groups - groups // 2, groups)):
        if not len(part):
            continue
        mixes, spreads = {}, {}
        for group in part:
            out = pl.ds(group * LANES, LANES)
            s_high, s_low = states[group]
            r_high, r_low = high_ref[:, out], low_ref[:, out]
            mixes[group] = flow_ref[0, :, out] + (
                dot_nt(r_high, s_high) + dot_nt(r_low, s_high) + dot_nt(r_high, s_low)
            )
        for group in part:
            q_high, q_low = split(mixes[group] * mixes[group])
            spreads[group] = dot(q_high, share) + dot(q_low, share)
        for group in part:
            gain, bias = tile_row(gain_ref, group, groups), tile_row(bias_ref, group, groups)
            out = pl.ds(group * LANES, LANES)
            normed = mixes[group] * lax.rsqrt(spreads[group] + 1e-5)
            buf[:, out] = ((normed * gain + bias) * flow_ref[1, :, out]).astype(BF16)
        at = pl.ds(part[0] * LANES, len(part) * LANES)
        copies.append(
            pltpu.make_async_copy(buf.at[:, at], out_ref.at[:, at], sems.at[len(copies)])
        )
        copies[-1].start()
    for copy in copies:
        copy.wait()


def program(r, k, v, w, gate, bonus, gain, bias):
    length, width = r.shape
    cores, count = lax.axis_size("head"), lax.axis_size("seq")
    planes = count // PLANE
    assert cores == 2 and count == planes * PLANE
    assert planes > 1 and planes & (planes - 1) == 0
    half = width // cores
    groups = half // LANES
    swap = [(0, 1), (1, 0)]
    hbm = pl.BlockSpec(memory_space=pltpu.HBM)
    gain, bias = gain.reshape(-1, TILE), bias.reshape(-1, TILE)

    def call(kernel, outs, **options):
        return pl.pallas_call(
            kernel,
            out_shape=outs,
            compiler_params=pltpu.CompilerParams(vmem_limit_bytes=VMEM_LIMIT),
            **options,
        )

    ends_shape = jax.ShapeDtypeStruct((groups, CHANNELS + 8, LANES), F32)
    packed_rows = -(-groups * (ROWS + 1) // 8) * 8
    packed = jax.ShapeDtypeStruct((packed_rows, LANES), F32)
    wire = jax.ShapeDtypeStruct((wire_rows(groups), LANES), F32)
    piece = jax.ShapeDtypeStruct((groups * ROWS, LANES), F32)
    shrink = 1.0
    while STATE_STEP * length * cores * count * shrink > 2.0**15:
        shrink *= 0.5

    held = pltpu.VMEM((length, width), BF16)
    k, v, w, r, gate = (pltpu.with_memory_space_constraint(x, pltpu.HBM) for x in (k, v, w, r, gate))
    theirs, k, v, w = call(
        load_kernel,
        [pltpu.VMEM(ends_shape.shape, F32)] + [held] * 3,
        in_specs=[hbm] * 3,
        scratch_shapes=[pltpu.SemaphoreType.DMA((cores, 3))],
    )(k, v, w)
    other = lax.ppermute(theirs, "head", swap)
    mine, r, gate = call(
        ends_kernel,
        [ends_shape] + [held] * 2,
        in_specs=[pl.BlockSpec()] * 3 + [hbm] * 2,
        scratch_shapes=[pltpu.SemaphoreType.DMA((2,))],
    )(k, v, w, r, gate)

    def within(side):
        return call(
            functools.partial(within_kernel, side), jax.ShapeDtypeStruct((3, length, half), F32)
        )(r, k, v, w, gate, bonus)

    def over_seq(value, flip):
        pairs = [(i, i ^ flip) for i in range(count)]
        return lax.ppermute(value.astype(jnp.float16), "seq", pairs).astype(F32)

    def to_places(pieces):
        return [pieces[0]] + [over_seq(pieces[step], step) for step in range(1, PLANE)]

    def across(value, bit, step):
        return over_seq(value, step * bit * PLANE)

    quarters = call(
        functools.partial(combine_kernel, shrink),
        [packed] + [wire] * (PLANE - 1),
        scratch_shapes=[pltpu.VMEM((groups, CHANNELS, LANES), F32)],
    )(mine, other)
    in_other = lax.ppermute(within(1), "head", swap)
    total, sent, prefix = call(
        functools.partial(plane_kernel, groups, shrink),
        [packed, wire, jax.ShapeDtypeStruct((PLANE,) + packed.shape, F32)],
        scratch_shapes=[pltpu.VMEM((PLANE,) + packed.shape, F32)],
    )(*to_places(quarters))
    in_mine = within(0)
    before, bit = total, 1
    while True:
        radix = min(4, planes // bit)
        last = bit * radix == planes
        slabs = [pltpu.VMEM((radix,) + packed.shape, F32)]
        options = (groups, shrink, bit, radix, bit == 1)
        got = [across(sent, bit, step) for step in range(1, radix)]
        if last:
            break
        total, sent, before = call(
            functools.partial(round_kernel, *options), [packed, wire, packed], scratch_shapes=slabs
        )(total, before, *got)
        bit *= radix
    states = call(
        functools.partial(back_kernel, *options),
        [piece] + [wire] * (PLANE - 1),
        scratch_shapes=slabs,
    )(prefix, total, before, *got)
    pieces = to_places(states)
    tokens = cores * length
    parts = call(
        prep_kernel,
        [jax.ShapeDtypeStruct((2, tokens, half), F32)]
        + [jax.ShapeDtypeStruct((tokens, half), BF16)] * 2,
    )(mine, other, in_mine, in_other)
    return call(
        functools.partial(finish_kernel, shrink),
        jax.ShapeDtypeStruct((tokens, half), BF16),
        out_specs=hbm,
        scratch_shapes=[
            pltpu.VMEM((groups * CHANNELS, LANES), F32),
            pltpu.VMEM((tokens, half), BF16),
            pltpu.SemaphoreType.DMA((2,)),
        ],
    )(*pieces, *parts, gain, bias)


def solution(mesh):
    tokens = P(("seq", "head"), None)
    return jax.shard_map(
        program,
        mesh=mesh,
        in_specs=(tokens,) * 5 + (P(), P(), P()),
        out_specs=P("seq", "head"),
        check_vma=False,
    )
```

```python
import functools

import jax
import jax.numpy as jnp
from jax import lax
from jax.experimental import pallas as pl
from jax.experimental.pallas import tpu as pltpu
from jax.sharding import PartitionSpec as P


CHANNELS = 64
TILE = 128
LANES = 256
HEADS = LANES // CHANNELS
BLOCK = 64
PLANE = 4
ROWS = CHANNELS // PLANE
STATE_STEP = 0.75 * 6.0
SCALE_FLOOR = 2.0**-10
CODE_SPAN = 14.7
CODE_MIDDLE = 0.75
VMEM_LIMIT = 12 * 2**20
F32 = jnp.float32
BF16 = jnp.bfloat16


def split(value):
    high = value.astype(BF16)
    return high, (value - high.astype(F32)).astype(BF16)


def dot(left, right):
    return lax.dot_general(left, right, (((1,), (0,)), ((), ())), preferred_element_type=F32)


def dot_nt(left, right):
    return lax.dot_general(left, right, (((1,), (1,)), ((), ())), preferred_element_type=F32)


def same_head(value):
    rows = lax.broadcasted_iota(jnp.int32, (LANES, LANES), 0) // CHANNELS
    columns = lax.broadcasted_iota(jnp.int32, (LANES, LANES), 1) // CHANNELS
    return jnp.where(rows == columns, F32(value), F32(0.0)).astype(BF16)


def half_masks(rows):
    left = lax.broadcasted_iota(jnp.int32, (rows, TILE), 1) < CHANNELS
    one, zero = F32(1.0), F32(0.0)
    return jnp.where(left, one, zero).astype(BF16), jnp.where(left, zero, one).astype(BF16)


def spread_heads(value, masks):
    zero = jnp.zeros((value.shape[0], TILE), value.dtype)
    pieces = []
    for head in range(HEADS):
        tile = head // 2
        kept = value[:, tile * TILE : (tile + 1) * TILE] * masks[head % 2]
        pieces.append(
            jnp.concatenate([kept if i == tile else zero for i in range(LANES // TILE)], axis=1)
        )
    return jnp.concatenate(pieces, axis=0)


def own_blocks(stacked, rows):
    left = lax.broadcasted_iota(jnp.int32, (rows, TILE), 1) < CHANNELS
    pieces = []
    for tile in range(LANES // TILE):
        part = stacked[:, tile * TILE : (tile + 1) * TILE]
        head = 2 * tile
        pieces.append(
            jnp.where(
                left,
                part[head * rows : (head + 1) * rows],
                part[(head + 1) * rows : (head + 2) * rows],
            )
        )
    return jnp.concatenate(pieces, axis=1)


def cumulate(decay):
    length = decay.shape[0]
    rows = lax.broadcasted_iota(jnp.int32, (length, length), 0)
    columns = lax.broadcasted_iota(jnp.int32, (length, length), 1)
    lower = jnp.where(rows >= columns, F32(1.0), F32(0.0)).astype(BF16)
    return dot(lower, decay)


def sum_after(decay):
    length = decay.shape[0]
    rows = lax.broadcasted_iota(jnp.int32, (length, length), 0)
    columns = lax.broadcasted_iota(jnp.int32, (length, length), 1)
    return dot(jnp.where(rows < columns, F32(1.0), F32(0.0)).astype(BF16), decay)


def lanes_at(side, group, groups):
    core = lax.axis_index("head")
    core = core if side == 0 else 1 - core
    return pl.ds(pl.multiple_of((core * groups + group) * LANES, LANES), LANES)


def bonus_row(ref, side, group, groups):
    core = lax.axis_index("head")
    core = core if side == 0 else 1 - core
    first = (core * groups + group) * HEADS
    return jnp.concatenate([ref[pl.ds(first + head, 1), :] for head in range(HEADS)], axis=1)


def tile_row(ref, group, groups):
    tiles = LANES // TILE
    first = (lax.axis_index("head") * groups + group) * tiles
    return jnp.concatenate([ref[pl.ds(first + tile, 1), :] for tile in range(tiles)], axis=1)


def half_at(side, half):
    core = lax.axis_index("head")
    core = core if side == 0 else 1 - core
    return pl.ds(pl.multiple_of(core * half, LANES), half)


def ends_of(side, k_ref, v_ref, w_ref, out_ref):
    span = range(out_ref.shape[0])
    at = [pl.ds((side * len(span) + group) * LANES, LANES) for group in span]
    afters = [sum_after(w_ref[:, at[group]]) for group in span]
    turned = [v_ref[:, at[group]].astype(F32).T.astype(BF16) for group in span]
    weighted = []
    for group in span:
        after = afters[group]
        final = after[:1] + w_ref[:, at[group]][:1].astype(F32)
        out_ref[group, CHANNELS:, :] = jnp.broadcast_to(final, (8, LANES))
        weighted.append(split(k_ref[:, at[group]].astype(F32) * jnp.exp(after)))
    for group in span:
        wide = dot(
            jnp.concatenate([turned[group]] * 2, axis=1),
            jnp.concatenate(weighted[group], axis=0),
        )
        out_ref[group, :CHANNELS, :] = own_blocks(wide, CHANNELS)


def load_kernel(k_ref, v_ref, w_ref, theirs_ref, k_buf, v_buf, w_buf, sems):
    half = theirs_ref.shape[0] * LANES
    copies = {}
    for side in (1, 0):
        at = half_at(side, half)
        for index, (ref, buf) in enumerate(((w_ref, w_buf), (k_ref, k_buf), (v_ref, v_buf))):
            copies[side, index] = pltpu.make_async_copy(
                ref.at[:, at], buf.at[:, pl.ds(side * half, half)], sems.at[side, index]
            )
            copies[side, index].start()
    for index in range(3):
        copies[1, index].wait()
    ends_of(1, k_buf, v_buf, w_buf, theirs_ref)
    for index in range(3):
        copies[0, index].wait()


def ends_kernel(k_ref, v_ref, w_ref, r_ref, g_ref, mine_ref, r_buf, g_buf, sems):
    copies = []
    for index, (ref, buf) in enumerate(((r_ref, r_buf), (g_ref, g_buf))):
        copies.append(pltpu.make_async_copy(ref, buf, sems.at[index]))
        copies[-1].start()
    ends_of(0, k_ref, v_ref, w_ref, mine_ref)
    for copy in copies:
        copy.wait()


def log_row(groups, group):
    return slice(groups * ROWS + group, groups * ROWS + group + 1)


def wire_rows(groups):
    return -(-groups * (ROWS + 3) // 16) * 16


def put_wire(ref, shrink, group, state, log=None):
    groups = ref.shape[0] // (ROWS + 3)
    top = jnp.max(jnp.abs(state), axis=0, keepdims=True)
    scale = (top * 1.01 + SCALE_FLOOR).astype(BF16).astype(F32)
    code = jnp.exp2(state * (CODE_SPAN / scale) + CODE_MIDDLE)
    ref[group * ROWS : (group + 1) * ROWS, :] = code
    row = groups * ROWS + group
    ref[row : row + 1, :] = scale * F32(shrink)
    high = jnp.zeros((1, LANES), F32) if log is None else log.astype(BF16).astype(F32)
    ref[row + groups : row + groups + 1, :] = high
    low = high if log is None else log - high
    ref[row + 2 * groups : row + 2 * groups + 1, :] = low


def clear_rest(ref):
    groups = ref.shape[0] // (ROWS + 3)
    rest = ref.shape[0] - groups * (ROWS + 3)
    if rest:
        ref[groups * (ROWS + 3) :, :] = jnp.zeros((rest, LANES), F32)


def get_wire(ref, shrink, group):
    groups = ref.shape[0] // (ROWS + 3)
    row = groups * ROWS + group
    scale = ref[row : row + 1, :] * F32(1.0 / (shrink * CODE_SPAN))
    code = ref[group * ROWS : (group + 1) * ROWS, :]
    state = (jnp.log2(code) - CODE_MIDDLE) * scale
    log = ref[row + groups : row + groups + 1, :] + ref[row + 2 * groups : row + 2 * groups + 1, :]
    return state, log


def combine_kernel(shrink, mine_ref, other_ref, q0, q1, q2, q3, state_ref):
    core = lax.axis_index("head")
    place = lax.axis_index("seq") % PLANE
    groups = mine_ref.shape[0]
    first = core == 0
    for out in (q1, q2, q3):
        clear_rest(out)
    for group in range(groups):
        mine, other = mine_ref[group], other_ref[group]
        early, late = jnp.where(first, mine, other), jnp.where(first, other, mine)
        late_log = late[CHANNELS : CHANNELS + 1]
        state_ref[group] = early[:CHANNELS] * jnp.exp(late_log) + late[:CHANNELS]
        both = early[CHANNELS : CHANNELS + 1] + late_log
        for step, out in enumerate((q0, q1, q2, q3)):
            at = pl.multiple_of(lax.bitwise_xor(place, step) * ROWS, ROWS)
            state = state_ref[group, pl.ds(at, ROWS), :]
            if step:
                put_wire(out, shrink, group, state, both)
            else:
                out[group * ROWS : (group + 1) * ROWS, :] = state
                out[log_row(groups, group), :] = both


def plane_kernel(groups, shrink, q0, q1, q2, q3, total_ref, wire_ref, prefix_ref, slab_ref):
    place = lax.axis_index("seq") % PLANE
    clear_rest(wire_ref)
    for group in range(groups):
        rows = slice(group * ROWS, (group + 1) * ROWS)
        row = log_row(groups, group)
        slab_ref[place, rows, :] = q0[rows, :]
        slab_ref[place, row, :] = q0[row, :]
        for step, piece in ((1, q1), (2, q2), (3, q3)):
            to = lax.bitwise_xor(place, step)
            state, log = get_wire(piece, shrink, group)
            slab_ref[to, rows, :] = state
            slab_ref[to, row, :] = log
    for group in range(groups):
        rows = slice(group * ROWS, (group + 1) * ROWS)
        row = log_row(groups, group)
        state = jnp.zeros((ROWS, LANES), F32)
        log = jnp.zeros((1, LANES), F32)
        for slab in range(PLANE):
            prefix_ref[slab, rows, :] = state
            prefix_ref[slab, row, :] = jnp.exp(log)
            step = slab_ref[slab, row, :]
            state = jnp.exp(step) * state + slab_ref[slab, rows, :]
            log = log + step
        total_ref[rows, :] = state
        total_ref[row, :] = log
        put_wire(wire_ref, shrink, group, state, log)


def group_prefix(groups, shrink, bit, radix, total_ref, got_refs, slab_ref):
    mine = lax.axis_index("seq") // PLANE // bit % radix
    for group in range(groups):
        rows = slice(group * ROWS, (group + 1) * ROWS)
        row = log_row(groups, group)
        slab_ref[mine, rows, :] = total_ref[rows, :]
        slab_ref[mine, row, :] = total_ref[row, :]
        for step, got in enumerate(got_refs, 1):
            to = lax.bitwise_xor(mine, step)
            state, log = get_wire(got, shrink, group)
            slab_ref[to, rows, :] = state
            slab_ref[to, row, :] = log
    found = []
    for group in range(groups):
        rows = slice(group * ROWS, (group + 1) * ROWS)
        row = log_row(groups, group)
        state, log = jnp.zeros((ROWS, LANES), F32), jnp.zeros((1, LANES), F32)
        before, before_log = state, log
        for slab in range(radix):
            step = slab_ref[slab, row, :]
            state = jnp.exp(step) * state + slab_ref[slab, rows, :]
            log = log + step
            before = jnp.where(slab < mine, state, before)
            before_log = jnp.where(slab < mine, log, before_log)
        found.append((before, before_log, state, log))
    return found


def round_kernel(groups, shrink, bit, radix, first, *refs):
    total_ref, before_ref, *got_refs = refs[: 2 + radix - 1]
    total_out, wire_out, before_out, slab_ref = refs[2 + radix - 1 :]
    clear_rest(wire_out)
    found = group_prefix(groups, shrink, bit, radix, total_ref, got_refs, slab_ref)
    for group, (state, log, total, total_log) in enumerate(found):
        rows = slice(group * ROWS, (group + 1) * ROWS)
        row = log_row(groups, group)
        if not first:
            state = jnp.exp(before_ref[row, :]) * state + before_ref[rows, :]
            log = log + before_ref[row, :]
        before_out[rows, :] = state
        before_out[row, :] = log
        total_out[rows, :] = total
        total_out[row, :] = total_log
        put_wire(wire_out, shrink, group, total, total_log)


def back_kernel(groups, shrink, bit, radix, first, *refs):
    prefix_ref, total_ref, before_ref, *got_refs = refs[: 3 + radix - 1]
    *outs, slab_ref = refs[3 + radix - 1 :]
    place = lax.axis_index("seq") % PLANE
    for out in outs[1:]:
        clear_rest(out)
    found = group_prefix(groups, shrink, bit, radix, total_ref, got_refs, slab_ref)
    for group, (before, _, _, _) in enumerate(found):
        rows = slice(group * ROWS, (group + 1) * ROWS)
        row = log_row(groups, group)
        if not first:
            before = jnp.exp(before_ref[row, :]) * before + before_ref[rows, :]
        for step, out in enumerate(outs):
            to = lax.bitwise_xor(place, step)
            state = prefix_ref[to, row, :] * before + prefix_ref[to, rows, :]
            if step:
                put_wire(out, shrink, group, state)
            else:
                out[rows, :] = state


def within_kernel(side, r_ref, k_ref, v_ref, w_ref, g_ref, bonus_ref, out_ref):
    groups = out_ref.shape[2] // LANES
    length = w_ref.shape[0]
    ones = same_head(1.0)
    share = same_head(1.0 / CHANNELS)
    masks = half_masks(BLOCK)
    shape = (HEADS * length, length)
    row = lax.broadcasted_iota(jnp.int32, shape, 0)
    later = row // (HEADS * BLOCK) * BLOCK + row % BLOCK
    strict = later > lax.broadcasted_iota(jnp.int32, shape, 1)
    span = range(groups)
    at = [lanes_at(side, group, groups) for group in span]
    out = [pl.ds(group * LANES, LANES) for group in span]
    held = [pl.ds((side * groups + group) * LANES, LANES) for group in span]
    cumuls = [cumulate(w_ref[:, held[group]]) for group in span]
    for group in span:
        gate = g_ref[:, at[group]].astype(F32)
        out_ref[2, :, out[group]] = gate / (1.0 + jnp.exp(-gate))
    scores = []
    for group in span:
        r, k = r_ref[:, at[group]].astype(F32), k_ref[:, held[group]].astype(F32)
        cumul = cumuls[group]
        before = cumul - w_ref[:, held[group]].astype(F32)
        out_ref[1, :, out[group]] = r * jnp.exp(before)
        pieces = []
        for start in range(0, length, BLOCK):
            stop = start + BLOCK
            middle = start + BLOCK // 2 - 1
            reference = cumul[middle : middle + 1]
            r_high, r_low = split(r[start:stop] * jnp.exp(before[start:stop] - reference))
            k_high, k_low = split(k[:stop] * jnp.exp(reference - cumul[:stop]))
            if stop < length:
                rest = jnp.zeros((length - stop, LANES), BF16)
                k_high = jnp.concatenate([k_high, rest], axis=0)
                k_low = jnp.concatenate([k_low, rest], axis=0)
            r_high, r_low = spread_heads(r_high, masks), spread_heads(r_low, masks)
            pieces.append(dot_nt(r_high, k_high) + dot_nt(r_low, k_high) + dot_nt(r_high, k_low))
        scores.append(split(jnp.where(strict, jnp.concatenate(pieces, axis=0), F32(0.0))))
    mixes = []
    for group in span:
        v = v_ref[:, held[group]]
        wide = dot(jnp.concatenate(scores[group], axis=1), jnp.concatenate([v, v], axis=0))
        step = HEADS * BLOCK
        mixed = jnp.concatenate(
            [own_blocks(wide[i * step : (i + 1) * step], BLOCK) for i in range(length // BLOCK)],
            axis=0,
        )
        r, k = r_ref[:, at[group]].astype(F32), k_ref[:, held[group]].astype(F32)
        diagonal_high, diagonal_low = split(r * bonus_row(bonus_ref, side, group, groups) * k)
        diagonal = dot(diagonal_high, ones) + dot(diagonal_low, ones)
        mixes.append(mixed + diagonal * v.astype(F32))
    for group in span:
        m_high, m_low = split(mixes[group])
        out_ref[0, :, out[group]] = mixes[group] - (dot(m_high, share) + dot(m_low, share))


def prep_kernel(ends_mine, ends_other, in_mine, in_other, flow_ref, high_ref, low_ref):
    core = lax.axis_index("head")
    groups = ends_mine.shape[0]
    length = in_mine.shape[1]
    first = core == 0
    masks = half_masks(CHANNELS)
    for group in range(groups):
        out = pl.ds(group * LANES, LANES)
        early = jnp.where(first, ends_mine[group], ends_other[group])
        state = early[:CHANNELS]
        s_high, s_low = split(state - jnp.mean(state, axis=0, keepdims=True))
        s_high, s_low = spread_heads(s_high, masks), spread_heads(s_low, masks)
        near = [jnp.where(first, in_mine[i, :, out], in_other[i, :, out]) for i in range(3)]
        far = [jnp.where(first, in_other[i, :, out], in_mine[i, :, out]) for i in range(3)]
        r_high, r_low = split(far[1])
        flow_ref[0, :length, out] = near[0]
        flow_ref[0, length:, out] = far[0] + (
            dot_nt(r_high, s_high) + dot_nt(r_low, s_high) + dot_nt(r_high, s_low)
        )
        flow_ref[1, :length, out] = near[2]
        flow_ref[1, length:, out] = far[2]
        high_ref[:length, out], low_ref[:length, out] = split(near[1])
        decay = jnp.exp(early[CHANNELS : CHANNELS + 1])
        high_ref[length:, out], low_ref[length:, out] = split(far[1] * decay)


def finish_kernel(
    shrink, p0, p1, p2, p3, flow_ref, high_ref, low_ref, gain_ref, bias_ref, out_ref,
    state_ref, buf, sems,
):
    place = lax.axis_index("seq") % PLANE
    groups = p0.shape[0] // ROWS
    share = same_head(1.0 / CHANNELS)
    masks = half_masks(CHANNELS)
    for step, piece in enumerate((p0, p1, p2, p3)):
        source = lax.bitwise_xor(place, step) * ROWS
        for group in range(groups):
            at = pl.multiple_of(source + group * CHANNELS, ROWS)
            if step:
                state, _ = get_wire(piece, shrink, group)
            else:
                state = piece[group * ROWS : (group + 1) * ROWS, :]
            state_ref[pl.ds(at, ROWS), :] = state
    states = []
    for group in range(groups):
        state = state_ref[group * CHANNELS : (group + 1) * CHANNELS, :]
        pair = split(state - jnp.mean(state, axis=0, keepdims=True))
        states.append([spread_heads(part, masks) for part in pair])
    copies = []
    for part in (range(groups - groups // 2), range(groups - groups // 2, groups)):
        if not len(part):
            continue
        mixes, spreads = {}, {}
        for group in part:
            out = pl.ds(group * LANES, LANES)
            s_high, s_low = states[group]
            r_high, r_low = high_ref[:, out], low_ref[:, out]
            mixes[group] = flow_ref[0, :, out] + (
                dot_nt(r_high, s_high) + dot_nt(r_low, s_high) + dot_nt(r_high, s_low)
            )
        for group in part:
            q_high, q_low = split(mixes[group] * mixes[group])
            spreads[group] = dot(q_high, share) + dot(q_low, share)
        for group in part:
            gain, bias = tile_row(gain_ref, group, groups), tile_row(bias_ref, group, groups)
            out = pl.ds(group * LANES, LANES)
            normed = mixes[group] * lax.rsqrt(spreads[group] + 1e-5)
            buf[:, out] = ((normed * gain + bias) * flow_ref[1, :, out]).astype(BF16)
        at = pl.ds(part[0] * LANES, len(part) * LANES)
        copies.append(
            pltpu.make_async_copy(buf.at[:, at], out_ref.at[:, at], sems.at[len(copies)])
        )
        copies[-1].start()
    for copy in copies:
        copy.wait()


def program(r, k, v, w, gate, bonus, gain, bias):
    length, width = r.shape
    cores, count = lax.axis_size("head"), lax.axis_size("seq")
    planes = count // PLANE
    assert cores == 2 and count == planes * PLANE
    assert planes > 1 and planes & (planes - 1) == 0
    half = width // cores
    groups = half // LANES
    swap = [(0, 1), (1, 0)]
    hbm = pl.BlockSpec(memory_space=pltpu.HBM)
    gain, bias = gain.reshape(-1, TILE), bias.reshape(-1, TILE)

    def call(kernel, outs, **options):
        return pl.pallas_call(
            kernel,
            out_shape=outs,
            compiler_params=pltpu.CompilerParams(vmem_limit_bytes=VMEM_LIMIT),
            **options,
        )

    ends_shape = jax.ShapeDtypeStruct((groups, CHANNELS + 8, LANES), F32)
    packed_rows = -(-groups * (ROWS + 1) // 8) * 8
    packed = jax.ShapeDtypeStruct((packed_rows, LANES), F32)
    wire = jax.ShapeDtypeStruct((wire_rows(groups), LANES), F32)
    piece = jax.ShapeDtypeStruct((groups * ROWS, LANES), F32)
    shrink = 1.0
    while STATE_STEP * length * cores * count * shrink > 2.0**15:
        shrink *= 0.5

    held = pltpu.VMEM((length, width), BF16)
    k, v, w, r, gate = (pltpu.with_memory_space_constraint(x, pltpu.HBM) for x in (k, v, w, r, gate))
    theirs, k, v, w = call(
        load_kernel,
        [pltpu.VMEM(ends_shape.shape, F32)] + [held] * 3,
        in_specs=[hbm] * 3,
        scratch_shapes=[pltpu.SemaphoreType.DMA((cores, 3))],
    )(k, v, w)
    other = lax.ppermute(theirs, "head", swap)
    mine, r, gate = call(
        ends_kernel,
        [ends_shape] + [held] * 2,
        in_specs=[pl.BlockSpec()] * 3 + [hbm] * 2,
        scratch_shapes=[pltpu.SemaphoreType.DMA((2,))],
    )(k, v, w, r, gate)

    def within(side):
        return call(
            functools.partial(within_kernel, side), jax.ShapeDtypeStruct((3, length, half), F32)
        )(r, k, v, w, gate, bonus)

    def over_seq(value, flip):
        pairs = [(i, i ^ flip) for i in range(count)]
        return lax.ppermute(value.astype(jnp.float16), "seq", pairs).astype(F32)

    def to_places(pieces):
        return [pieces[0]] + [over_seq(pieces[step], step) for step in range(1, PLANE)]

    def across(value, bit, step):
        return over_seq(value, step * bit * PLANE)

    quarters = call(
        functools.partial(combine_kernel, shrink),
        [packed] + [wire] * (PLANE - 1),
        scratch_shapes=[pltpu.VMEM((groups, CHANNELS, LANES), F32)],
    )(mine, other)
    in_other = lax.ppermute(within(1), "head", swap)
    total, sent, prefix = call(
        functools.partial(plane_kernel, groups, shrink),
        [packed, wire, jax.ShapeDtypeStruct((PLANE,) + packed.shape, F32)],
        scratch_shapes=[pltpu.VMEM((PLANE,) + packed.shape, F32)],
    )(*to_places(quarters))
    in_mine = within(0)
    before, bit = total, 1
    while True:
        radix = min(4, planes // bit)
        last = bit * radix == planes
        slabs = [pltpu.VMEM((radix,) + packed.shape, F32)]
        options = (groups, shrink, bit, radix, bit == 1)
        got = [across(sent, bit, step) for step in range(1, radix)]
        if last:
            break
        total, sent, before = call(
            functools.partial(round_kernel, *options), [packed, wire, packed], scratch_shapes=slabs
        )(total, before, *got)
        bit *= radix
    states = call(
        functools.partial(back_kernel, *options),
        [piece] + [wire] * (PLANE - 1),
        scratch_shapes=slabs,
    )(prefix, total, before, *got)
    pieces = to_places(states)
    tokens = cores * length
    parts = call(
        prep_kernel,
        [jax.ShapeDtypeStruct((2, tokens, half), F32)]
        + [jax.ShapeDtypeStruct((tokens, half), BF16)] * 2,
    )(mine, other, in_mine, in_other)
    return call(
        functools.partial(finish_kernel, shrink),
        jax.ShapeDtypeStruct((tokens, half), BF16),
        out_specs=hbm,
        scratch_shapes=[
            pltpu.VMEM((groups * CHANNELS, LANES), F32),
            pltpu.VMEM((tokens, half), BF16),
            pltpu.SemaphoreType.DMA((2,)),
        ],
    )(*pieces, *parts, gain, bias)


def solution(mesh):
    tokens = P(("seq", "head"), None)
    return jax.shard_map(
        program,
        mesh=mesh,
        in_specs=(tokens,) * 5 + (P(), P(), P()),
        out_specs=P("seq", "head"),
        check_vma=False,
    )
```
